8 devices in a mesh: dp: 1 (over z), etp: 2 (over y), ep: 4 (over x, core).
Axes of the slice: x: 2, y: 2, z: 1, core: 2. Of those that a mesh axis runs over, the one named last changes fastest.
Arguments:
- x_in: bfloat16 [512, 1024], P(('dp', 'ep'))
- y_grad: bfloat16 [512, 1024], P(('dp', 'ep'))
- prim_exp: int32 [512], P(('dp', 'ep'))
- alt_exp: int32 [512], P(('dp', 'ep'))
- w_router: bfloat16 [1024, 32], replicated
- exp_gate: bfloat16 [32, 1024, 512], P('ep', None, 'etp')
- exp_up: bfloat16 [32, 1024, 512], P('ep', None, 'etp')
- exp_down: bfloat16 [32, 512, 1024], P('ep', 'etp')
- sh_gate: bfloat16 [1024, 512], P(None, 'etp')
- sh_up: bfloat16 [1024, 512], P(None, 'etp')
- sh_down: bfloat16 [512, 1024], P('etp')
Outputs:
- output 1: bfloat16 [512, 1024], P(('dp', 'ep'))
- output 2: bfloat16 [512, 1024], P(('dp', 'ep'))
- output 3: float32 [32, 1024, 512], P(('dp', 'ep'), None, 'etp')
- output 4: float32 [32, 1024, 512], P(('dp', 'ep'), None, 'etp')
- output 5: float32 [32, 512, 1024], P(('dp', 'ep'), 'etp')
- output 6: float32 [1024, 512], P('dp', 'etp')
- output 7: float32 [1024, 512], P('dp', 'etp')
- output 8: float32 [512, 1024], P(('dp', 'etp'))
- output 9: float32 [1024, 32], P('dp')
All inputs are finite; a program needn't handle non-finite values.
Results may differ from the reference program's by a relative error of at most 0.001.
Values are sent between devices in bfloat16 or wider.
A program may use at most 1 GiB of HBM per device.

```python
import jax
import jax.numpy as jnp
from jax import lax

D = 1024
FF = 512
EXPERTS = 32
TOKENS = 512
CAP = 20
EPS = 1e-5


def draw_routes(route_key):
    key_hot, key_pick, key_coin, key_flat, key_alt = jax.random.split(route_key, 5)
    hot_ids = jax.random.permutation(key_hot, EXPERTS)[:3]
    hot_pick = jax.random.randint(key_pick, (TOKENS,), 0, 3)
    hot_coin = jax.random.randint(key_coin, (TOKENS,), 0, 4)
    flat_ids = jax.random.randint(key_flat, (TOKENS,), 0, EXPERTS)
    prim_exp = jnp.where(hot_coin == 0, hot_ids[hot_pick], flat_ids).astype(jnp.int32)
    alt_shift = jax.random.randint(key_alt, (TOKENS,), 1, EXPERTS)
    alt_exp = ((prim_exp + alt_shift) % EXPERTS).astype(jnp.int32)
    return prim_exp, alt_exp


def normal_mat(rand_key, arr_shape, mult_scale):
    return (jax.random.normal(rand_key, arr_shape, jnp.float32) * mult_scale).astype(jnp.bfloat16)


def setup_inputs(seed: int = 0, part: int = 0) -> dict:
    base_key = jax.random.key(seed)
    part_keys = jax.random.split(jax.random.fold_in(base_key, part), 3)
    weight_keys = jax.random.split(base_key, 7)
    prim_exp, alt_exp = draw_routes(part_keys[2])
    return dict(
        x_in=normal_mat(part_keys[0], (TOKENS, D), 1.0),
        y_grad=normal_mat(part_keys[1], (TOKENS, D), 1.0),
        prim_exp=prim_exp,
        alt_exp=alt_exp,
        w_router=normal_mat(weight_keys[0], (D, EXPERTS), D ** -0.5),
        exp_gate=normal_mat(weight_keys[1], (EXPERTS, D, FF), D ** -0.5),
        exp_up=normal_mat(weight_keys[2], (EXPERTS, D, FF), D ** -0.5),
        exp_down=normal_mat(weight_keys[3], (EXPERTS, FF, D), 0.5 * EXPERTS * FF ** -0.5),
        sh_gate=normal_mat(weight_keys[4], (D, FF), D ** -0.5),
        sh_up=normal_mat(weight_keys[5], (D, FF), D ** -0.5),
        sh_down=normal_mat(weight_keys[6], (FF, D), FF ** -0.5),
    )


def exclusive_rank(onehot):
    return jnp.sum((jnp.cumsum(onehot, axis=0) - onehot) * onehot, axis=1)


def route_tokens(prim_exp, alt_exp):
    expert_ids = jnp.arange(EXPERTS)
    one_prim = (prim_exp[:, None] == expert_ids[None, :]).astype(jnp.int32)
    rank_prim = exclusive_rank(one_prim)
    keep_prim = rank_prim < CAP
    kept_count = jnp.minimum(jnp.sum(one_prim, axis=0), CAP)
    overflow = jnp.logical_not(keep_prim).astype(jnp.int32)
    one_alt = (alt_exp[:, None] == expert_ids[None, :]).astype(jnp.int32) * overflow[:, None]
    slot_alt = exclusive_rank(one_alt) + jnp.sum(one_alt * kept_count[None, :], axis=1)
    keep_alt = (overflow == 1) & (slot_alt < CAP)
    assign = jnp.where(keep_prim, prim_exp, jnp.where(keep_alt, alt_exp, -1))
    slot_idx = jnp.where(keep_prim, rank_prim, slot_alt)
    return assign, slot_idx


def glu_forward(tok_rows, w_gate, w_up):
    act_gate = jnp.dot(tok_rows, w_gate, preferred_element_type=jnp.float32)
    act_up = jnp.dot(tok_rows, w_up, preferred_element_type=jnp.float32)
    hidden = (jax.nn.silu(act_gate) * act_up).astype(jnp.bfloat16)
    return hidden, act_gate, act_up


def glu_backward(d_hidden, act_gate, act_up):
    sig_gate = jax.nn.sigmoid(act_gate)
    d_gate = (d_hidden * act_up * sig_gate * (1.0 + act_gate * (1.0 - sig_gate))).astype(jnp.bfloat16)
    d_up = (d_hidden * act_gate * sig_gate).astype(jnp.bfloat16)
    return d_gate, d_up


def expert_forward(packed):
    tok_rows, w_gate, w_up, w_down = packed
    hidden, act_gate, act_up = glu_forward(tok_rows, w_gate, w_up)
    out_rows = jnp.dot(hidden, w_down, preferred_element_type=jnp.float32).astype(jnp.bfloat16)
    return hidden, act_gate, act_up, out_rows


def expert_backward(packed):
    tok_rows, d_rows, hidden, act_gate, act_up, w_gate, w_up, w_down = packed
    d_hidden = jnp.dot(d_rows, w_down.T, preferred_element_type=jnp.float32)
    g_down = jnp.dot(hidden.T, d_rows, preferred_element_type=jnp.float32)
    d_gate, d_up = glu_backward(d_hidden, act_gate, act_up)
    g_gate = jnp.dot(tok_rows.T, d_gate, preferred_element_type=jnp.float32)
    g_up = jnp.dot(tok_rows.T, d_up, preferred_element_type=jnp.float32)
    d_rows_in = (jnp.dot(d_gate, w_gate.T, preferred_element_type=jnp.float32) + jnp.dot(d_up, w_up.T, preferred_element_type=jnp.float32)).astype(jnp.bfloat16)
    return g_gate, g_up, g_down, d_rows_in


def reference(x_in, y_grad, prim_exp, alt_exp, w_router, exp_gate, exp_up, exp_down, sh_gate, sh_up, sh_down):
    x_wide = x_in.astype(jnp.float32)
    inv_rms = lax.rsqrt(jnp.mean(x_wide * x_wide, axis=1, keepdims=True) + EPS)
    normed = (x_wide * inv_rms).astype(jnp.bfloat16)
    gate_probs = jax.nn.softmax(jnp.dot(normed, w_router, preferred_element_type=jnp.float32), axis=1)
    assign, slot_idx = route_tokens(prim_exp, alt_exp)
    flat_pos = jnp.where(assign >= 0, assign * CAP + slot_idx, EXPERTS * CAP)
    slot_table = jnp.full((EXPERTS * CAP + 1,), TOKENS, jnp.int32).at[flat_pos].set(jnp.arange(TOKENS, dtype=jnp.int32))[: EXPERTS * CAP]
    expert_rows = jnp.take(normed, slot_table, axis=0, mode="fill", fill_value=0).reshape(EXPERTS, CAP, D)
    hidden, act_gate, act_up, out_rows = lax.map(expert_forward, (expert_rows, exp_gate, exp_up, exp_down))
    tok_out = jnp.take(out_rows.reshape(EXPERTS * CAP, D), flat_pos, axis=0, mode="fill", fill_value=0).astype(jnp.float32)
    one_assign = (assign[:, None] == jnp.arange(EXPERTS)[None, :]).astype(jnp.float32)
    gate_val = jnp.sum(gate_probs * one_assign, axis=1, keepdims=True)
    sh_hidden, sh_act_gate, sh_act_up = glu_forward(normed, sh_gate, sh_up)
    sh_out = jnp.dot(sh_hidden, sh_down, preferred_element_type=jnp.float32)
    y_out = (x_wide + sh_out + gate_val * tok_out).astype(jnp.bfloat16)
    dy_wide = y_grad.astype(jnp.float32)
    d_route = (gate_val * dy_wide).astype(jnp.bfloat16)
    d_gate_val = jnp.sum(dy_wide * tok_out, axis=1, keepdims=True)
    d_logits = (d_gate_val * gate_val * (one_assign - gate_probs)).astype(jnp.bfloat16)
    g_router = jnp.dot(normed.T, d_logits, preferred_element_type=jnp.float32)
    dn_router = jnp.dot(d_logits, w_router.T, preferred_element_type=jnp.float32)
    sh_d_hidden = jnp.dot(y_grad, sh_down.T, preferred_element_type=jnp.float32)
    g_sh_down = jnp.dot(sh_hidden.T, y_grad, preferred_element_type=jnp.float32)
    sh_d_gate, sh_d_up = glu_backward(sh_d_hidden, sh_act_gate, sh_act_up)
    g_sh_gate = jnp.dot(normed.T, sh_d_gate, preferred_element_type=jnp.float32)
    g_sh_up = jnp.dot(normed.T, sh_d_up, preferred_element_type=jnp.float32)
    dn_shared = jnp.dot(sh_d_gate, sh_gate.T, preferred_element_type=jnp.float32) + jnp.dot(sh_d_up, sh_up.T, preferred_element_type=jnp.float32)
    d_rows = jnp.take(d_route, slot_table, axis=0, mode="fill", fill_value=0).reshape(EXPERTS, CAP, D)
    g_exp_gate, g_exp_up, g_exp_down, d_rows_in = lax.map(expert_backward, (expert_rows, d_rows, hidden, act_gate, act_up, exp_gate, exp_up, exp_down))
    dn_routed = jnp.take(d_rows_in.reshape(EXPERTS * CAP, D), flat_pos, axis=0, mode="fill", fill_value=0).astype(jnp.float32)
    d_normed = dn_shared + dn_router + dn_routed
    norm_proj = jnp.mean(d_normed * x_wide, axis=1, keepdims=True)
    x_grad = (dy_wide + inv_rms * d_normed - x_wide * inv_rms ** 3 * norm_proj).astype(jnp.bfloat16)
    return (y_out, x_grad, g_exp_gate, g_exp_up, g_exp_down, g_sh_gate, g_sh_up, g_sh_down, g_router)
```

```python
import functools

import jax
import jax.numpy as jnp
from jax import lax
from jax.experimental import pallas as pl
from jax.experimental.pallas import tpu as pltpu
from jax.sharding import PartitionSpec as P

EPS = 1e-5
F32 = jnp.float32
BF16 = jnp.bfloat16
MESH = pl.DeviceIdType.MESH
ANY = pl.BlockSpec(memory_space=pl.ANY)
VMEM = pl.BlockSpec(memory_space=pltpu.VMEM)
NN = (((1,), (0,)), ((), ()))
NT = (((1,), (1,)), ((), ()))
TN = (((0,), (0,)), ((), ()))

SHARDS = 4
TOK = 128
DIM = 1024
HALF = 512
EXPERTS = 32
OWN = 8
CAP = 20
PAD = 32
SLOTS = OWN * CAP


def mm(a, b, dims=NN):
    return lax.dot_general(a, b, dims, preferred_element_type=F32)


def inv_rms_of(x_wide):
    return lax.rsqrt(jnp.mean(x_wide * x_wide, axis=1, keepdims=True) + EPS)


def glu_grads(d_hidden, act_gate, act_up):
    sig_gate = jax.nn.sigmoid(act_gate)
    d_gate = (d_hidden * act_up * sig_gate * (1.0 + act_gate * (1.0 - sig_gate))).astype(BF16)
    d_up = (d_hidden * act_gate * sig_gate).astype(BF16)
    return d_gate, d_up


def to_row(col):
    return jnp.transpose(jnp.broadcast_to(col, (TOK, TOK)))[:8]


def to_col(row):
    return jnp.transpose(jnp.broadcast_to(row, (TOK, TOK)))[:, :1]


def barrier(peers):
    sem = pltpu.get_barrier_semaphore()
    for peer in peers:
        pl.semaphore_signal(sem, inc=1, device_id=peer, device_id_type=MESH)
    pl.semaphore_wait(sem, len(peers))


def gather_kernel(x_ref, dy_ref, ids_ref, wg_hbm, wu_hbm, wd_hbm, x_all, dy_all, ids_all, s_out, dns_out, wg, wu, wd, s_send, s_recv, d_send, d_recv, w_sem, send_sem, recv_sem, y_send_sem, y_recv_sem):
    me = lax.axis_index("ep")
    side = lax.axis_index("etp")
    mate = jnp.bitwise_xor(me, 1)
    across = jnp.bitwise_xor(me, 2)
    to_mate, to_across, to_twin = {"ep": mate}, {"ep": across}, {"etp": 1 - side}
    loads = [pltpu.make_async_copy(src, dst, w_sem.at[k]) for k, (src, dst) in enumerate(((wg_hbm, wg), (wu_hbm, wu), (wd_hbm, wd)))]
    for load in loads:
        load.start()
    barrier((to_mate, to_across, to_twin))
    half_rows = TOK // 2

    def pieces(shard):
        return [
            (ids_ref, ids_all.at[shard]),
            (x_ref.at[:half_rows], x_all.at[shard, :half_rows]),
            (x_ref.at[half_rows:], x_all.at[shard, half_rows:]),
            (dy_ref.at[:half_rows], dy_all.at[shard, :half_rows]),
            (dy_ref.at[half_rows:], dy_all.at[shard, half_rows:]),
        ]

    def remote(src, dst, lane, k, target):
        return pltpu.make_async_remote_copy(src_ref=src, dst_ref=dst, send_sem=send_sem.at[lane, k], recv_sem=recv_sem.at[lane, k], device_id=target, device_id_type=MESH)

    out_across = [remote(src, dst, 0, k, to_across) for k, (src, dst) in enumerate(pieces(me))]
    out_mate = [remote(src, dst, 1, k, to_mate) for k, (src, dst) in enumerate(pieces(me))]
    for copy in out_across:
        copy.start()
    for copy in out_mate:
        copy.start()
    x_all[me] = x_ref[...]
    dy_all[me] = dy_ref[...]
    ids_all[me] = ids_ref[...]

    x_wide = x_ref[...].astype(F32)
    normed = (x_wide * inv_rms_of(x_wide)).astype(BF16)
    for load in loads:
        load.wait()
    act_gate = mm(normed, wg[...])
    act_up = mm(normed, wu[...])
    hidden = (jax.nn.silu(act_gate) * act_up).astype(BF16)
    theirs = pl.ds(pl.multiple_of((1 - side) * HALF, HALF), HALF)
    mine = pl.ds(pl.multiple_of(side * HALF, HALF), HALF)
    s_send[...] = mm(hidden, wd[:, theirs])
    s_copy = pltpu.make_async_remote_copy(src_ref=s_send, dst_ref=s_recv, send_sem=y_send_sem.at[0], recv_sem=y_recv_sem.at[0], device_id=to_twin, device_id_type=MESH)
    s_copy.start()
    d_gate, d_up = glu_grads(mm(dy_ref[...], wd[...], NT), act_gate, act_up)
    d_send[...] = mm(d_gate, wg[theirs, :], NT) + mm(d_up, wu[theirs, :], NT)
    d_copy = pltpu.make_async_remote_copy(src_ref=d_send, dst_ref=d_recv, send_sem=y_send_sem.at[1], recv_sem=y_recv_sem.at[1], device_id=to_twin, device_id_type=MESH)
    d_copy.start()
    s_out[...] = mm(hidden, wd[:, mine])
    dns_out[...] = mm(d_gate, wg[mine, :], NT) + mm(d_up, wu[mine, :], NT)

    forwards = []
    for k, (_, dst) in enumerate(pieces(across)):
        out_across[k].wait_recv()
        forward = remote(dst, dst, 2, k, to_mate)
        forward.start()
        forwards.append(forward)
    s_copy.wait_recv()
    s_out[...] += s_recv[...]
    d_copy.wait_recv()
    dns_out[...] += d_recv[...]
    for copy in out_mate + forwards:
        copy.wait_recv()
    for copy in out_across + out_mate + forwards + [s_copy, d_copy]:
        copy.wait_send()


def gather_call(x_in, y_grad, ids, sh_gate, sh_up, sh_down):
    width = sh_gate.shape[1]
    return pl.pallas_call(
        gather_kernel,
        out_shape=(
            jax.ShapeDtypeStruct((SHARDS, TOK, DIM), BF16),
            jax.ShapeDtypeStruct((SHARDS, TOK, DIM), BF16),
            jax.ShapeDtypeStruct((SHARDS, 8, TOK), jnp.int32),
            jax.ShapeDtypeStruct((TOK, HALF), F32),
            jax.ShapeDtypeStruct((TOK, HALF), F32),
        ),
        in_specs=[VMEM, VMEM, VMEM, ANY, ANY, ANY],
        out_specs=(VMEM,) * 5,
        scratch_shapes=[
            pltpu.VMEM((DIM, width), BF16),
            pltpu.VMEM((DIM, width), BF16),
            pltpu.VMEM((width, DIM), BF16),
            pltpu.VMEM((TOK, HALF), F32),
            pltpu.VMEM((TOK, HALF), F32),
            pltpu.VMEM((TOK, HALF), F32),
            pltpu.VMEM((TOK, HALF), F32),
            pltpu.SemaphoreType.DMA((3,)),
            pltpu.SemaphoreType.DMA((3, 5)),
            pltpu.SemaphoreType.DMA((3, 5)),
            pltpu.SemaphoreType.DMA((2,)),
            pltpu.SemaphoreType.DMA((2,)),
        ],
        compiler_params=pltpu.CompilerParams(collective_id=0, has_side_effects=True),
        name="gather_tokens",
    )(x_in, y_grad, ids, sh_gate, sh_up, sh_down)


def forward_kernel(x_ref, dy_ref, ids_ref, wr_ref, wg, wu, wd, o_send, o_keep, xs, us, a_out, b_out, h_out, n_out, meta, p_out):
    me = lax.axis_index("ep")
    side = lax.axis_index("etp")
    total = SHARDS * TOK

    @pl.when(pl.program_id(0) == 0)
    def route():
        x_wide = x_ref[...].reshape(total, DIM).astype(F32)
        normed = (x_wide * inv_rms_of(x_wide)).astype(BF16)
        n_out[...] = normed
        logits = mm(normed, wr_ref[...])
        top = jnp.max(logits, axis=1, keepdims=True)
        expo = jnp.exp(logits - top)
        probs = expo / jnp.sum(expo, axis=1, keepdims=True)
        wide = jnp.concatenate([probs, jnp.zeros((total, TOK - EXPERTS), F32)], axis=1)
        probs_t = jnp.concatenate([jnp.transpose(wide[s * TOK : (s + 1) * TOK])[:EXPERTS] for s in range(SHARDS)], axis=1)
        p_out[...] = probs_t

        prim = jnp.concatenate([ids_ref[s, 0:1, :] for s in range(SHARDS)], axis=1)
        alt = jnp.concatenate([ids_ref[s, 1:2, :] for s in range(SHARDS)], axis=1)
        expert = lax.broadcasted_iota(jnp.int32, (EXPERTS, total), 0)
        before = (lax.broadcasted_iota(jnp.int32, (total, total), 0) < lax.broadcasted_iota(jnp.int32, (total, total), 1)).astype(F32).astype(BF16)
        one_prim = (expert == prim).astype(F32)
        rank_prim = jnp.sum(one_prim * mm(one_prim.astype(BF16), before), axis=0, keepdims=True)
        keep_prim = rank_prim < CAP
        kept = jnp.minimum(jnp.sum(one_prim, axis=1, keepdims=True), float(CAP))
        one_alt = jnp.where(keep_prim, 0.0, (expert == alt).astype(F32))
        slot_alt = jnp.sum(one_alt * (mm(one_alt.astype(BF16), before) + kept), axis=0, keepdims=True)
        keep_alt = jnp.logical_and(jnp.logical_not(keep_prim), slot_alt < CAP)
        assign = jnp.where(keep_prim, prim, jnp.where(keep_alt, alt, -1))
        slot = jnp.where(keep_prim, rank_prim, slot_alt).astype(jnp.int32)
        gate = jnp.sum(jnp.where(expert == assign, probs_t, 0.0), axis=0, keepdims=True)
        flat = jnp.where(assign >= 0, assign * CAP + slot, -1)
        meta[0:1] = assign.astype(F32)
        meta[1:2] = flat.astype(F32)
        meta[2:3] = gate
        meta[3:8] = jnp.zeros((5, total), F32)

        local = assign - me * OWN
        owned = jnp.logical_and(local >= 0, local < OWN)
        target = jnp.where(owned, local * PAD + slot, -1)
        picked = lax.broadcasted_iota(jnp.int32, (OWN * PAD, total), 0) == target
        pick = picked.astype(F32).astype(BF16)
        xs[...] = mm(pick, normed).astype(BF16)
        gate_slot = jnp.sum(jnp.where(picked, gate, 0.0), axis=1, keepdims=True)
        us[...] = (gate_slot * mm(pick, dy_ref[...].reshape(total, DIM))).astype(BF16)

    theirs = pl.ds(pl.multiple_of((1 - side) * HALF, HALF), HALF)
    mine = pl.ds(pl.multiple_of(side * HALF, HALF), HALF)
    for j in range(2):
        row = pl.multiple_of((pl.program_id(0) * 2 + j) * PAD, PAD)
        rows = xs[pl.ds(row, PAD), :]
        act_gate = mm(rows, wg[j])
        act_up = mm(rows, wu[j])
        hidden = (jax.nn.silu(act_gate) * act_up).astype(BF16)
        a_out[j] = act_gate
        b_out[j] = act_up
        h_out[j] = hidden
        o_send[0, j * CAP : (j + 1) * CAP, :] = mm(hidden, wd[j, :, theirs])[:CAP]
        o_keep[0, j * CAP : (j + 1) * CAP, :] = mm(hidden, wd[j, :, mine])[:CAP]


def whole(shape):
    return pl.BlockSpec(shape, lambda i: (0,) * len(shape))


def forward_call(x_all, dy_all, ids_all, w_router, exp_gate, exp_up, exp_down):
    width = exp_gate.shape[2]
    total = SHARDS * TOK
    pair = lambda *shape: pl.BlockSpec((2,) + shape, lambda i: (i, 0, 0))
    part = pl.BlockSpec((1, 2 * CAP, HALF), lambda i: (i, 0, 0))
    return pl.pallas_call(
        forward_kernel,
        grid=(OWN // 2,),
        out_shape=(
            jax.ShapeDtypeStruct((OWN // 2, 2 * CAP, HALF), F32),
            jax.ShapeDtypeStruct((OWN // 2, 2 * CAP, HALF), F32),
            jax.ShapeDtypeStruct((OWN * PAD, DIM), BF16),
            jax.ShapeDtypeStruct((OWN * PAD, DIM), BF16),
            jax.ShapeDtypeStruct((OWN, PAD, width), F32),
            jax.ShapeDtypeStruct((OWN, PAD, width), F32),
            jax.ShapeDtypeStruct((OWN, PAD, width), BF16),
            jax.ShapeDtypeStruct((total, DIM), BF16),
            jax.ShapeDtypeStruct((8, total), F32),
            jax.ShapeDtypeStruct((EXPERTS, total), F32),
        ),
        in_specs=[whole((SHARDS, TOK, DIM)), whole((SHARDS, TOK, DIM)), whole((SHARDS, 8, TOK)), whole((DIM, EXPERTS)), pair(DIM, width), pair(DIM, width), pair(width, DIM)],
        out_specs=(part, part, whole((OWN * PAD, DIM)), whole((OWN * PAD, DIM)), pair(PAD, width), pair(PAD, width), pair(PAD, width), whole((total, DIM)), whole((8, total)), whole((EXPERTS, total))),
        compiler_params=pltpu.CompilerParams(dimension_semantics=("arbitrary",), vmem_limit_bytes=48 << 20),
        cost_estimate=pl.CostEstimate(flops=2 * 3 * OWN * PAD * DIM * width, bytes_accessed=16 << 20, transcendentals=0),
        name="expert_forward",
    )(x_all, dy_all, ids_all, w_router, exp_gate, exp_up, exp_down)


def backward_kernel(us, a_in, b_in, wg, wu, wd, d_send, d_keep, da_out, db_out):
    side = lax.axis_index("etp")
    theirs = pl.ds(pl.multiple_of((1 - side) * HALF, HALF), HALF)
    mine = pl.ds(pl.multiple_of(side * HALF, HALF), HALF)
    for j in range(2):
        row = pl.multiple_of((pl.program_id(0) * 2 + j) * PAD, PAD)
        d_gate, d_up = glu_grads(mm(us[pl.ds(row, PAD), :], wd[j], NT), a_in[j], b_in[j])
        da_out[j] = d_gate
        db_out[j] = d_up
        d_send[0, j * CAP : (j + 1) * CAP, :] = (mm(d_gate, wg[j, theirs, :], NT) + mm(d_up, wu[j, theirs, :], NT))[:CAP]
        d_keep[0, j * CAP : (j + 1) * CAP, :] = (mm(d_gate, wg[j, mine, :], NT) + mm(d_up, wu[j, mine, :], NT))[:CAP]


def backward_call(us, act_gate, act_up, exp_gate, exp_up, exp_down):
    width = exp_gate.shape[2]
    pair = lambda *shape: pl.BlockSpec((2,) + shape, lambda i: (i, 0, 0))
    part = pl.BlockSpec((1, 2 * CAP, HALF), lambda i: (i, 0, 0))
    return pl.pallas_call(
        backward_kernel,
        grid=(OWN // 2,),
        out_shape=(
            jax.ShapeDtypeStruct((OWN // 2, 2 * CAP, HALF), F32),
            jax.ShapeDtypeStruct((OWN // 2, 2 * CAP, HALF), F32),
            jax.ShapeDtypeStruct((OWN, PAD, width), BF16),
            jax.ShapeDtypeStruct((OWN, PAD, width), BF16),
        ),
        in_specs=[whole((OWN * PAD, DIM)), pair(PAD, width), pair(PAD, width), pair(DIM, width), pair(DIM, width), pair(width, DIM)],
        out_specs=(part, part, pair(PAD, width), pair(PAD, width)),
        compiler_params=pltpu.CompilerParams(dimension_semantics=("arbitrary",), vmem_limit_bytes=40 << 20),
        cost_estimate=pl.CostEstimate(flops=2 * 3 * OWN * PAD * DIM * width, bytes_accessed=16 << 20, transcendentals=0),
        name="expert_backward",
    )(us, act_gate, act_up, exp_gate, exp_up, exp_down)


def grads_kernel(xs, us, h_in, da_in, db_in, n_ref, dy_ref, sg, su, sd, g_gate, g_up, g_down, gs_gate, gs_up, gs_down):
    @pl.when(pl.program_id(0) == 0)
    def shared():
        normed = n_ref[...]
        d_rows = dy_ref[...].reshape(SHARDS * TOK, DIM)
        act_gate = mm(normed, sg[...])
        act_up = mm(normed, su[...])
        hidden = (jax.nn.silu(act_gate) * act_up).astype(BF16)
        d_gate, d_up = glu_grads(mm(d_rows, sd[...], NT), act_gate, act_up)
        gs_down[...] = mm(hidden, d_rows, TN)
        gs_gate[...] = mm(normed, d_gate, TN)
        gs_up[...] = mm(normed, d_up, TN)

    row = pl.multiple_of(pl.program_id(0) * PAD, PAD)
    rows = xs[pl.ds(row, PAD), :]
    g_down[0] = mm(h_in[0], us[pl.ds(row, PAD), :], TN)
    g_gate[0] = mm(rows, da_in[0], TN)
    g_up[0] = mm(rows, db_in[0], TN)


def grads_call(xs, us, hidden, d_gate, d_up, normed, dy_all, sh_gate, sh_up, sh_down):
    width = sh_gate.shape[1]
    total = SHARDS * TOK
    one = lambda *shape: pl.BlockSpec((1,) + shape, lambda i: (i, 0, 0))
    return pl.pallas_call(
        grads_kernel,
        grid=(OWN,),
        out_shape=(
            jax.ShapeDtypeStruct((OWN, DIM, width), F32),
            jax.ShapeDtypeStruct((OWN, DIM, width), F32),
            jax.ShapeDtypeStruct((OWN, width, DIM), F32),
            jax.ShapeDtypeStruct((DIM, width), F32),
            jax.ShapeDtypeStruct((DIM, width), F32),
            jax.ShapeDtypeStruct((width, DIM), F32),
        ),
        in_specs=[whole((OWN * PAD, DIM)), whole((OWN * PAD, DIM)), one(PAD, width), one(PAD, width), one(PAD, width), whole((total, DIM)), whole((SHARDS, TOK, DIM)), whole((DIM, width)), whole((DIM, width)), whole((width, DIM))],
        out_specs=(one(DIM, width), one(DIM, width), one(width, DIM), whole((DIM, width)), whole((DIM, width)), whole((width, DIM))),
        compiler_params=pltpu.CompilerParams(dimension_semantics=("arbitrary",), vmem_limit_bytes=48 << 20),
        cost_estimate=pl.CostEstimate(flops=8 << 30, bytes_accessed=32 << 20, transcendentals=0),
        name="weight_grads",
    )(xs, us, hidden, d_gate, d_up, normed, dy_all, sh_gate, sh_up, sh_down)


def finish_kernel(o_keep, o_recv, d_keep, d_recv, x_ref, dy_ref, s_ref, dns_ref, meta, p_ref, n_ref, wr_ref, y_out, dx_out, gr_out, o_all, d_all, dg_mine, dg_all, np_mine, np_recv, y_half, dx_half, send_sem, recv_sem, y_send_sem, y_recv_sem, g_send_sem, g_recv_sem):
    me = lax.axis_index("ep")
    side = lax.axis_index("etp")
    mate = jnp.bitwise_xor(me, 1)
    across = jnp.bitwise_xor(me, 2)
    to_mate, to_across, to_twin = {"ep": mate}, {"ep": across}, {"etp": 1 - side}
    others = [{"etp": jnp.bitwise_xor(side, k // SHARDS), "ep": jnp.bitwise_xor(me, k % SHARDS)} for k in range(1, 2 * SHARDS)]
    barrier(others)

    def remote(buf, shard, lane, k, target):
        view = buf.at[shard]
        return pltpu.make_async_remote_copy(src_ref=view, dst_ref=view, send_sem=send_sem.at[lane, k], recv_sem=recv_sem.at[lane, k], device_id=target, device_id_type=MESH)

    def twin(src, dst, k):
        return pltpu.make_async_remote_copy(src_ref=src, dst_ref=dst, send_sem=y_send_sem.at[k], recv_sem=y_recv_sem.at[k], device_id=to_twin, device_id_type=MESH)

    o_all[me] = (o_keep[...].reshape(SLOTS, HALF) + o_recv[...].reshape(SLOTS, HALF)).astype(BF16)
    o_copies = [remote(o_all, me, 0, 0, to_across), remote(o_all, me, 1, 0, to_mate)]
    for copy in o_copies:
        copy.start()
    d_all[me] = (d_keep[...].reshape(SLOTS, HALF) + d_recv[...].reshape(SLOTS, HALF)).astype(BF16)
    d_copies = [remote(d_all, me, 0, 1, to_across), remote(d_all, me, 1, 1, to_mate)]
    for copy in d_copies:
        copy.start()

    mine = pl.ds(pl.multiple_of(side * HALF, HALF), HALF)
    theirs = pl.ds(pl.multiple_of((1 - side) * HALF, HALF), HALF)
    home = pl.ds(pl.multiple_of(me * TOK, TOK), TOK)
    x_wide = x_ref[...].astype(F32)
    inv_rms = inv_rms_of(x_wide)
    x_half = x_ref[:, mine].astype(F32)
    dy_half = dy_ref[:, mine].astype(F32)
    gate = to_col(meta[2:3, home])
    flat = to_col(meta[1:2, home]).astype(jnp.int32)
    pick = (lax.broadcasted_iota(jnp.int32, (TOK, SHARDS * SLOTS), 1) == flat).astype(F32).astype(BF16)

    o_copies[0].wait_recv()
    o_forward = remote(o_all, across, 2, 0, to_mate)
    o_forward.start()
    o_copies[1].wait_recv()
    o_forward.wait_recv()
    tok_out = mm(pick, o_all[...].reshape(SHARDS * SLOTS, HALF))
    dg_mine[...] = to_row(jnp.sum(dy_half * tok_out, axis=1, keepdims=True))
    slot = side * SHARDS + me
    dg_copies = [pltpu.make_async_remote_copy(src_ref=dg_mine, dst_ref=dg_all.at[slot], send_sem=g_send_sem.at[k], recv_sem=g_recv_sem.at[k], device_id=other, device_id_type=MESH) for k, other in enumerate(others)]
    for copy in dg_copies:
        copy.start()
    dg_all[slot] = dg_mine[...]
    y_half[...] = (x_half + s_ref[...] + gate * tok_out).astype(BF16)
    y_copy = twin(y_half, y_out.at[:, mine], 0)
    y_copy.start()
    y_out[:, mine] = y_half[...]

    d_copies[0].wait_recv()
    d_forward = remote(d_all, across, 2, 1, to_mate)
    d_forward.start()
    d_copies[1].wait_recv()
    d_forward.wait_recv()
    dn_routed = mm(pick, d_all[...].reshape(SHARDS * SLOTS, HALF))
    for copy in dg_copies:
        copy.wait_recv()
    dg = jnp.concatenate([dg_all[s, 0:1, :] + dg_all[SHARDS + s, 0:1, :] for s in range(SHARDS)], axis=1)
    expert = lax.broadcasted_iota(jnp.int32, (EXPERTS, SHARDS * TOK), 0)
    one_assign = (expert == meta[0:1, :].astype(jnp.int32)).astype(F32)
    d_logits = (dg * meta[2:3, :] * (one_assign - p_ref[...])).astype(BF16)
    home_one = (lax.broadcasted_iota(jnp.int32, (EXPERTS, TOK), 0) == meta[0:1, home].astype(jnp.int32)).astype(F32)
    dg_home = dg_all[me, 0:1, :] + dg_all[SHARDS + me, 0:1, :]
    d_logits_home = (dg_home * meta[2:3, home] * (home_one - p_ref[:, home])).astype(BF16)
    dn_router = mm(d_logits_home.T, wr_ref[mine, :], NT)
    d_normed = dns_ref[...] + dn_router + dn_routed
    np_part = jnp.sum(d_normed * x_half, axis=1, keepdims=True)
    np_mine[...] = to_row(np_part)
    np_copy = twin(np_mine, np_recv, 1)
    np_copy.start()
    gr_out[...] = mm(d_logits, n_ref[...])
    np_copy.wait_recv()
    norm_proj = (np_part + to_col(np_recv[0:1, :])) / DIM
    dx_half[...] = (dy_half + inv_rms * d_normed - x_half * inv_rms**3 * norm_proj).astype(BF16)
    dx_copy = twin(dx_half, dx_out.at[:, mine], 2)
    dx_copy.start()
    dx_out[:, mine] = dx_half[...]
    y_copy.wait_recv()
    dx_copy.wait_recv()
    for copy in o_copies + d_copies + [o_forward, d_forward] + dg_copies + [y_copy, np_copy, dx_copy]:
        copy.wait_send()


def finish_call(*args):
    return pl.pallas_call(
        finish_kernel,
        out_shape=(
            jax.ShapeDtypeStruct((TOK, DIM), BF16),
            jax.ShapeDtypeStruct((TOK, DIM), BF16),
            jax.ShapeDtypeStruct((EXPERTS, DIM), F32),
        ),
        in_specs=[VMEM] * 12,
        out_specs=(VMEM,) * 3,
        scratch_shapes=[
            pltpu.VMEM((SHARDS, SLOTS, HALF), BF16),
            pltpu.VMEM((SHARDS, SLOTS, HALF), BF16),
            pltpu.VMEM((8, TOK), F32),
            pltpu.VMEM((2 * SHARDS, 8, TOK), F32),
            pltpu.VMEM((8, TOK), F32),
            pltpu.VMEM((8, TOK), F32),
            pltpu.VMEM((TOK, HALF), BF16),
            pltpu.VMEM((TOK, HALF), BF16),
            pltpu.SemaphoreType.DMA((3, 2)),
            pltpu.SemaphoreType.DMA((3, 2)),
            pltpu.SemaphoreType.DMA((3,)),
            pltpu.SemaphoreType.DMA((3,)),
            pltpu.SemaphoreType.DMA((7,)),
            pltpu.SemaphoreType.DMA((7,)),
        ],
        compiler_params=pltpu.CompilerParams(collective_id=1, has_side_effects=True),
        name="finish_tokens",
    )(*args)


def solution(mesh):
    tok_spec = P(("dp", "ep"), None)
    id_spec = P(("dp", "ep"))
    in_specs = (tok_spec, tok_spec, id_spec, id_spec, P(None, None), P("ep", None, "etp"), P("ep", None, "etp"), P("ep", "etp", None), P(None, "etp"), P(None, "etp"), P("etp", None))
    out_specs = (tok_spec, tok_spec, P(("dp", "ep"), None, "etp"), P(("dp", "ep"), None, "etp"), P(("dp", "ep"), "etp", None), P("dp", "etp"), P("dp", "etp"), P(("dp", "etp"), None), P("dp", None))

    def local_step(x_in, y_grad, prim_exp, alt_exp, w_router, exp_gate, exp_up, exp_down, sh_gate, sh_up, sh_down):
        ids = jnp.concatenate([prim_exp[None], alt_exp[None], jnp.zeros((6, TOK), jnp.int32)], axis=0)
        x_all, dy_all, ids_all, s_half, dns_half = gather_call(x_in, y_grad, ids, sh_gate, sh_up, sh_down)
        o_send, o_keep, xs, us, act_gate, act_up, hidden, normed, meta, probs = forward_call(x_all, dy_all, ids_all, w_router, exp_gate, exp_up, exp_down)
        swap = [(0, 1), (1, 0)]
        o_recv = lax.ppermute(o_send, "etp", swap)
        d_send, d_keep, d_gate, d_up = backward_call(us, act_gate, act_up, exp_gate, exp_up, exp_down)
        d_recv = lax.ppermute(d_send, "etp", swap)
        g_gate, g_up, g_down, gs_gate, gs_up, gs_down = grads_call(xs, us, hidden, d_gate, d_up, normed, dy_all, sh_gate, sh_up, sh_down)
        y_out, x_grad, g_router = finish_call(o_keep, o_recv, d_keep, d_recv, x_in, y_grad, s_half, dns_half, meta, probs, normed, w_router)
        return (y_out, x_grad, g_gate, g_up, g_down, gs_gate, gs_up, gs_down, g_router.T)

    return jax.shard_map(local_step, mesh=mesh, in_specs=in_specs, out_specs=out_specs, check_vma=False)
```

```python
import functools

import jax
import jax.numpy as jnp
from jax import lax
from jax.experimental import pallas as pl
from jax.experimental.pallas import tpu as pltpu
from jax.sharding import PartitionSpec as P

EPS = 1e-5
F32 = jnp.float32
BF16 = jnp.bfloat16
MESH = pl.DeviceIdType.MESH
ANY = pl.BlockSpec(memory_space=pl.ANY)
VMEM = pl.BlockSpec(memory_space=pltpu.VMEM)
NN = (((1,), (0,)), ((), ()))
NT = (((1,), (1,)), ((), ()))
TN = (((0,), (0,)), ((), ()))

SHARDS = 4
TOK = 128
DIM = 1024
HALF = 512
EXPERTS = 32
OWN = 8
CAP = 20
PAD = 32
SLOTS = OWN * CAP


def mm(a, b, dims=NN):
    return lax.dot_general(a, b, dims, preferred_element_type=F32)


def inv_rms_of(x_wide):
    return lax.rsqrt(jnp.mean(x_wide * x_wide, axis=1, keepdims=True) + EPS)


def glu_grads(d_hidden, act_gate, act_up):
    sig_gate = jax.nn.sigmoid(act_gate)
    d_gate = (d_hidden * act_up * sig_gate * (1.0 + act_gate * (1.0 - sig_gate))).astype(BF16)
    d_up = (d_hidden * act_gate * sig_gate).astype(BF16)
    return d_gate, d_up


def to_row(col):
    return jnp.transpose(jnp.broadcast_to(col, (TOK, TOK)))[:8]


def to_col(row):
    return jnp.transpose(jnp.broadcast_to(row, (TOK, TOK)))[:, :1]


def barrier(peers):
    sem = pltpu.get_barrier_semaphore()
    for peer in peers:
        pl.semaphore_signal(sem, inc=1, device_id=peer, device_id_type=MESH)
    pl.semaphore_wait(sem, len(peers))


def layer_kernel(x_hbm, dy_hbm, prim_hbm, alt_hbm, wr_hbm, wg_hbm, wu_hbm, wd_hbm, sg_hbm, su_hbm, sd_hbm,
                 y_out, dx_out, gr_out, xs_hbm, us_hbm, h_hbm, da_hbm, db_hbm, n_hbm, dy_all_hbm, sh_hbm, sda_hbm, sdb_hbm,
                 x_all, dy_all, ids_all, wr, wg, wu, wd, sg, su, sd, n_all, xs, us, acts, acts_up, hid, da, db, hid_s, da_s, db_s,
                 probs, meta, s_send, s_recv, s_keep, n_send, n_recv, n_keep, o_send, o_recv, o_keep, d_send, d_recv, d_keep,
                 o_all, d_all, dg_mine, dg_all, np_mine, np_recv, y_half, dx_half,
                 in_sem, w_sem, out_sem, send_sem, recv_sem, r_send_sem, r_recv_sem, y_send_sem, y_recv_sem, g_send_sem, g_recv_sem):
    me = lax.axis_index("ep")
    side = lax.axis_index("etp")
    total = SHARDS * TOK
    mate = jnp.bitwise_xor(me, 1)
    across = jnp.bitwise_xor(me, 2)
    to_mate, to_across, to_twin = {"ep": mate}, {"ep": across}, {"etp": 1 - side}
    others = [{"etp": jnp.bitwise_xor(side, k // SHARDS), "ep": jnp.bitwise_xor(me, k % SHARDS)} for k in range(1, 2 * SHARDS)]
    theirs = pl.ds(pl.multiple_of((1 - side) * HALF, HALF), HALF)
    mine = pl.ds(pl.multiple_of(side * HALF, HALF), HALF)
    home = pl.ds(pl.multiple_of(me * TOK, TOK), TOK)

    loads = [pltpu.make_async_copy(src, dst, in_sem.at[k]) for k, (src, dst) in enumerate((
        (x_hbm, x_all.at[me]), (prim_hbm, ids_all.at[me, 0:1]), (alt_hbm, ids_all.at[me, 1:2]), (dy_hbm, dy_all.at[me]),
        (sg_hbm, sg), (su_hbm, su), (sd_hbm, sd), (wr_hbm, wr)))]
    for load in loads:
        load.start()
    w_loads = [[pltpu.make_async_copy(src.at[e], dst.at[e], w_sem.at[k, e]) for k, (src, dst) in enumerate(((wg_hbm, wg), (wu_hbm, wu), (wd_hbm, wd)))] for e in range(OWN)]
    for group in w_loads:
        for load in group:
            load.start()
    barrier(others)

    def remote(view, lane, k, target):
        return pltpu.make_async_remote_copy(src_ref=view, dst_ref=view, send_sem=send_sem.at[lane, k], recv_sem=recv_sem.at[lane, k], device_id=target, device_id_type=MESH)

    def ret(buf, shard, chunk, lane, k, target):
        view = buf.at[shard, chunk * (SLOTS // 2) : (chunk + 1) * (SLOTS // 2)]
        return pltpu.make_async_remote_copy(src_ref=view, dst_ref=view, send_sem=r_send_sem.at[lane, k], recv_sem=r_recv_sem.at[lane, k], device_id=target, device_id_type=MESH)

    def twin(src, dst, k):
        return pltpu.make_async_remote_copy(src_ref=src, dst_ref=dst, send_sem=y_send_sem.at[k], recv_sem=y_recv_sem.at[k], device_id=to_twin, device_id_type=MESH)

    def pieces(shard):
        rows = TOK // 2
        return [ids_all.at[shard], x_all.at[shard, :rows], x_all.at[shard, rows:], dy_all.at[shard, :rows], dy_all.at[shard, rows:]]

    out_across = [remote(view, 0, k, to_across) for k, view in enumerate(pieces(me))]
    out_mate = [remote(view, 1, k, to_mate) for k, view in enumerate(pieces(me))]
    forwards = [remote(view, 2, k, to_mate) for k, view in enumerate(pieces(across))]
    for load in loads[:3]:
        load.wait()
    for k in range(3):
        out_across[k].start()
        out_mate[k].start()
    loads[3].wait()
    for k in range(3, 5):
        out_across[k].start()
        out_mate[k].start()

    x_wide = x_all[me].astype(F32)
    inv_rms = inv_rms_of(x_wide)
    normed = (x_wide * inv_rms).astype(BF16)
    for load in loads[4:7]:
        load.wait()
    act_gate = mm(normed, sg[...])
    act_up = mm(normed, su[...])
    hidden = (jax.nn.silu(act_gate) * act_up).astype(BF16)
    d_gate, d_up = glu_grads(mm(dy_all[me], sd[...], NT), act_gate, act_up)
    n_send[...] = mm(d_gate, sg[theirs, :], NT) + mm(d_up, su[theirs, :], NT)
    n_copy = twin(n_send, n_recv, 0)
    n_copy.start()
    s_send[...] = mm(hidden, sd[:, theirs])
    s_copy = twin(s_send, s_recv, 1)
    s_copy.start()
    n_keep[...] = mm(d_gate, sg[mine, :], NT) + mm(d_up, su[mine, :], NT)
    s_keep[...] = mm(hidden, sd[:, mine])

    for k in range(3):
        out_across[k].wait_recv()
        forwards[k].start()
    for k in range(3):
        out_mate[k].wait_recv()
        forwards[k].wait_recv()

    x_wide = x_all[...].reshape(total, DIM).astype(F32)
    n_all[...] = (x_wide * inv_rms_of(x_wide)).astype(BF16)
    loads[7].wait()
    logits = mm(n_all[...], wr[...], NT)
    top = jnp.max(logits, axis=1, keepdims=True)
    expo = jnp.exp(logits - top)
    share = expo / jnp.sum(expo, axis=1, keepdims=True)
    wide = jnp.concatenate([share, jnp.zeros((total, TOK - EXPERTS), F32)], axis=1)
    probs_t = jnp.concatenate([jnp.transpose(wide[s * TOK : (s + 1) * TOK])[:EXPERTS] for s in range(SHARDS)], axis=1)
    probs[...] = probs_t
    prim = jnp.concatenate([ids_all[s, 0:1, :] for s in range(SHARDS)], axis=1)
    alt = jnp.concatenate([ids_all[s, 1:2, :] for s in range(SHARDS)], axis=1)
    expert = lax.broadcasted_iota(jnp.int32, (EXPERTS, total), 0)
    before = (lax.broadcasted_iota(jnp.int32, (total, total), 0) < lax.broadcasted_iota(jnp.int32, (total, total), 1)).astype(F32).astype(BF16)
    one_prim = (expert == prim).astype(F32)
    rank_prim = jnp.sum(one_prim * mm(one_prim.astype(BF16), before), axis=0, keepdims=True)
    keep_prim = rank_prim < CAP
    kept = jnp.minimum(jnp.sum(one_prim, axis=1, keepdims=True), float(CAP))
    one_alt = jnp.where(keep_prim, 0.0, (expert == alt).astype(F32))
    slot_alt = jnp.sum(one_alt * (mm(one_alt.astype(BF16), before) + kept), axis=0, keepdims=True)
    keep_alt = jnp.logical_and(jnp.logical_not(keep_prim), slot_alt < CAP)
    assign = jnp.where(keep_prim, prim, jnp.where(keep_alt, alt, -1))
    slot = jnp.where(keep_prim, rank_prim, slot_alt).astype(jnp.int32)
    gate = jnp.sum(jnp.where(expert == assign, probs_t, 0.0), axis=0, keepdims=True)
    flat = jnp.where(assign >= 0, assign * CAP + slot, -1)
    meta[0:1] = assign.astype(F32)
    meta[1:2] = flat.astype(F32)
    meta[2:3] = gate
    local = assign - me * OWN
    owned = jnp.logical_and(local >= 0, local < OWN)
    target = jnp.where(owned, local * PAD + slot, -1)
    picked = lax.broadcasted_iota(jnp.int32, (OWN * PAD, total), 0) == target
    pick_own = picked.astype(F32).astype(BF16)
    gate_slot = jnp.sum(jnp.where(picked, gate, 0.0), axis=1, keepdims=True)
    xs[...] = mm(pick_own, n_all[...]).astype(BF16)

    o_copies, d_copies = [], []
    for e in range(OWN):
        for load in w_loads[e]:
            load.wait()
        rows = slice(e * PAD, (e + 1) * PAD)
        act_gate = mm(xs[rows, :], wg[e])
        act_up = mm(xs[rows, :], wu[e])
        hidden = (jax.nn.silu(act_gate) * act_up).astype(BF16)
        acts[rows, :] = act_gate
        acts_up[rows, :] = act_up
        hid[rows, :] = hidden
        part = slice(e * CAP, (e + 1) * CAP)
        o_send[part, :] = mm(hidden, wd[e, :, theirs])[:CAP]
        o_keep[part, :] = mm(hidden, wd[e, :, mine])[:CAP]
        if e % 2:
            chunk = slice((e - 1) * CAP, (e + 1) * CAP)
            o_copies.append(twin(o_send.at[chunk], o_recv.at[chunk], 2 + e // 2))
            o_copies[-1].start()
        if e in (1, 4):
            k = 3 if e == 1 else 4
            out_across[k].wait_recv()
            forwards[k].start()
    for k in range(3, 5):
        out_mate[k].wait_recv()
        forwards[k].wait_recv()
    us[...] = (gate_slot * mm(pick_own, dy_all[...].reshape(total, DIM))).astype(BF16)

    returns = []

    def give_back(buf, keep, recv, copies, chunk, base):
        for copy in copies[2 * chunk : 2 * chunk + 2]:
            copy.wait_recv()
        rows = slice(chunk * (SLOTS // 2), (chunk + 1) * (SLOTS // 2))
        buf[me, rows] = (keep[rows, :] + recv[rows, :]).astype(BF16)
        k = base + chunk
        first, second = ret(buf, me, chunk, 0, k, to_across), ret(buf, me, chunk, 1, k, to_mate)
        first.start()
        second.start()
        third = ret(buf, across, chunk, 2, k, to_mate)
        returns.extend((first, second, third))
        return first, second, third

    def pass_on(group):
        group[0].wait_recv()
        group[2].start()

    o_back = []
    for e in range(OWN):
        rows = slice(e * PAD, (e + 1) * PAD)
        d_gate, d_up = glu_grads(mm(us[rows, :], wd[e], NT), acts[rows, :], acts_up[rows, :])
        da[rows, :] = d_gate
        db[rows, :] = d_up
        part = slice(e * CAP, (e + 1) * CAP)
        d_send[part, :] = (mm(d_gate, wg[e, theirs, :], NT) + mm(d_up, wu[e, theirs, :], NT))[:CAP]
        d_keep[part, :] = (mm(d_gate, wg[e, mine, :], NT) + mm(d_up, wu[e, mine, :], NT))[:CAP]
        if e % 2:
            chunk = slice((e - 1) * CAP, (e + 1) * CAP)
            d_copies.append(twin(d_send.at[chunk], d_recv.at[chunk], 6 + e // 2))
            d_copies[-1].start()
        if e == 5:
            o_back.append(give_back(o_all, o_keep, o_recv, o_copies, 0, 0))

    saves = [pltpu.make_async_copy(src, dst, out_sem.at[k]) for k, (src, dst) in enumerate((
        (xs, xs_hbm), (us, us_hbm), (hid, h_hbm), (da, da_hbm), (db, db_hbm), (n_all, n_hbm), (dy_all, dy_all_hbm), (hid_s, sh_hbm), (da_s, sda_hbm), (db_s, sdb_hbm)))]
    for save in saves[:7]:
        save.start()
    act_gate = mm(n_all[...], sg[...])
    act_up = mm(n_all[...], su[...])
    hid_s[...] = (jax.nn.silu(act_gate) * act_up).astype(BF16)
    d_gate, d_up = glu_grads(mm(dy_all[...].reshape(total, DIM), sd[...], NT), act_gate, act_up)
    da_s[...] = d_gate
    db_s[...] = d_up
    for save in saves[7:]:
        save.start()

    o_back.append(give_back(o_all, o_keep, o_recv, o_copies, 1, 0))
    pass_on(o_back[0])
    x_half = x_all[me, :, mine].astype(F32)
    dy_half = dy_all[me, :, mine].astype(F32)
    gate_home = to_col(meta[2:3, home])
    flat_home = to_col(meta[1:2, home]).astype(jnp.int32)
    pick = (lax.broadcasted_iota(jnp.int32, (TOK, SHARDS * SLOTS), 1) == flat_home).astype(F32).astype(BF16)
    pass_on(o_back[1])
    for group in o_back:
        group[1].wait_recv()
        group[2].wait_recv()
    tok_out = mm(pick, o_all[...].reshape(SHARDS * SLOTS, HALF))
    dg_mine[...] = to_row(jnp.sum(dy_half * tok_out, axis=1, keepdims=True))
    place = side * SHARDS + me
    dg_copies = [pltpu.make_async_remote_copy(src_ref=dg_mine, dst_ref=dg_all.at[place], send_sem=g_send_sem.at[k], recv_sem=g_recv_sem.at[k], device_id=other, device_id_type=MESH) for k, other in enumerate(others)]
    for copy in dg_copies:
        copy.start()
    dg_all[place] = dg_mine[...]
    s_copy.wait_recv()
    y_half[...] = (x_half + (s_keep[...] + s_recv[...]) + gate_home * tok_out).astype(BF16)
    y_copy = twin(y_half, y_out.at[:, mine], 10)
    y_copy.start()
    y_out[:, mine] = y_half[...]

    d_back = [give_back(d_all, d_keep, d_recv, d_copies, 0, 2)]
    for copy in dg_copies:
        copy.wait_recv()
    dg = jnp.concatenate([dg_all[s, 0:1, :] + dg_all[SHARDS + s, 0:1, :] for s in range(SHARDS)], axis=1)
    one_assign = (lax.broadcasted_iota(jnp.int32, (EXPERTS, total), 0) == meta[0:1, :].astype(jnp.int32)).astype(F32)
    d_logits = (dg * meta[2:3, :] * (one_assign - probs[...])).astype(BF16)
    home_one = (lax.broadcasted_iota(jnp.int32, (EXPERTS, TOK), 0) == meta[0:1, home].astype(jnp.int32)).astype(F32)
    dg_home = dg_all[me, 0:1, :] + dg_all[SHARDS + me, 0:1, :]
    d_logits_home = (dg_home * meta[2:3, home] * (home_one - probs[:, home])).astype(BF16)
    n_copy.wait_recv()
    d_normed = n_keep[...] + n_recv[...] + mm(d_logits_home, wr[:, mine], TN)
    pass_on(d_back[0])
    d_back.append(give_back(d_all, d_keep, d_recv, d_copies, 1, 2))
    gr_out[...] = mm(d_logits, n_all[...])
    pass_on(d_back[1])
    for group in d_back:
        group[1].wait_recv()
        group[2].wait_recv()
    d_normed = d_normed + mm(pick, d_all[...].reshape(SHARDS * SLOTS, HALF))
    np_part = jnp.sum(d_normed * x_half, axis=1, keepdims=True)
    np_mine[...] = to_row(np_part)
    np_copy = twin(np_mine, np_recv, 11)
    np_copy.start()
    np_copy.wait_recv()
    norm_proj = (np_part + to_col(np_recv[0:1, :])) / DIM
    dx_half[...] = (dy_half + inv_rms * d_normed - x_half * inv_rms**3 * norm_proj).astype(BF16)
    dx_copy = twin(dx_half, dx_out.at[:, mine], 12)
    dx_copy.start()
    dx_out[:, mine] = dx_half[...]
    for save in saves:
        save.wait()
    y_copy.wait_recv()
    dx_copy.wait_recv()
    for copy in out_across + out_mate + forwards + [n_copy, s_copy] + o_copies + d_copies + returns + dg_copies + [y_copy, np_copy, dx_copy]:
        copy.wait_send()


def layer_call(x_in, y_grad, prim, alt, wr_t, exp_gate, exp_up, exp_down, sh_gate, sh_up, sh_down):
    width = sh_gate.shape[1]
    total = SHARDS * TOK
    rows = OWN * PAD
    shape = jax.ShapeDtypeStruct
    dma = pltpu.SemaphoreType.DMA
    half_f32 = pltpu.VMEM((TOK, HALF), F32)
    slots_f32 = pltpu.VMEM((SLOTS, HALF), F32)
    return pl.pallas_call(
        layer_kernel,
        out_shape=(
            shape((TOK, DIM), BF16), shape((TOK, DIM), BF16), shape((EXPERTS, DIM), F32),
            shape((rows, DIM), BF16), shape((rows, DIM), BF16), shape((rows, width), BF16), shape((rows, width), BF16), shape((rows, width), BF16),
            shape((total, DIM), BF16), shape((SHARDS, TOK, DIM), BF16), shape((total, width), BF16), shape((total, width), BF16), shape((total, width), BF16),
        ),
        in_specs=[ANY] * 11,
        out_specs=(VMEM,) * 3 + (ANY,) * 10,
        scratch_shapes=[
            pltpu.VMEM((SHARDS, TOK, DIM), BF16), pltpu.VMEM((SHARDS, TOK, DIM), BF16), pltpu.VMEM((SHARDS, 8, TOK), jnp.int32), pltpu.VMEM((EXPERTS, DIM), BF16),
            pltpu.VMEM((OWN, DIM, width), BF16), pltpu.VMEM((OWN, DIM, width), BF16), pltpu.VMEM((OWN, width, DIM), BF16),
            pltpu.VMEM((DIM, width), BF16), pltpu.VMEM((DIM, width), BF16), pltpu.VMEM((width, DIM), BF16),
            pltpu.VMEM((total, DIM), BF16), pltpu.VMEM((rows, DIM), BF16), pltpu.VMEM((rows, DIM), BF16),
            pltpu.VMEM((rows, width), F32), pltpu.VMEM((rows, width), F32), pltpu.VMEM((rows, width), BF16), pltpu.VMEM((rows, width), BF16), pltpu.VMEM((rows, width), BF16),
            pltpu.VMEM((total, width), BF16), pltpu.VMEM((total, width), BF16), pltpu.VMEM((total, width), BF16),
            pltpu.VMEM((EXPERTS, total), F32), pltpu.VMEM((8, total), F32),
            half_f32, half_f32, half_f32, half_f32, half_f32, half_f32,
            slots_f32, slots_f32, slots_f32, slots_f32, slots_f32, slots_f32,
            pltpu.VMEM((SHARDS, SLOTS, HALF), BF16), pltpu.VMEM((SHARDS, SLOTS, HALF), BF16),
            pltpu.VMEM((8, TOK), F32), pltpu.VMEM((2 * SHARDS, 8, TOK), F32), pltpu.VMEM((8, TOK), F32), pltpu.VMEM((8, TOK), F32),
            pltpu.VMEM((TOK, HALF), BF16), pltpu.VMEM((TOK, HALF), BF16),
            dma((8,)), dma((3, OWN)), dma((10,)), dma((3, 5)), dma((3, 5)), dma((3, 4)), dma((3, 4)), dma((13,)), dma((13,)), dma((7,)), dma((7,)),
        ],
        compiler_params=pltpu.CompilerParams(collective_id=0, has_side_effects=True, vmem_limit_bytes=60 << 20),
        name="moe_layer",
    )(x_in, y_grad, prim, alt, wr_t, exp_gate, exp_up, exp_down, sh_gate, sh_up, sh_down)


def grads_kernel(xs, us, h_in, da_in, db_in, n_ref, dy_ref, hid_s, da_s, db_s, y_in, dx_in, gr_in, g_gate, g_up, g_down, gs_gate, gs_up, gs_down, y_out, dx_out, gr_out, sem):
    step = pl.program_id(0)
    moves = [pltpu.make_async_copy(src, dst, sem.at[k]) for k, (src, dst) in enumerate(((y_in, y_out), (dx_in, dx_out), (gr_in, gr_out)))]

    @pl.when(step == 0)
    def begin():
        for move in moves:
            move.start()

    g_down[0] = mm(h_in[...], us[...], TN)
    g_gate[0] = mm(xs[...], da_in[...], TN)
    g_up[0] = mm(xs[...], db_in[...], TN)
    gs_gate[...] = mm(n_ref[...], da_s[...], TN)
    gs_up[...] = mm(n_ref[...], db_s[...], TN)
    gs_down[...] = mm(hid_s[...], dy_ref[...], TN)

    @pl.when(step == pl.num_programs(0) - 1)
    def end():
        for move in moves:
            move.wait()


def grads_call(xs, us, hid, da, db, n_all, dy_all, hid_s, da_s, db_s, y_out, dx_out, gr_out):
    width = hid.shape[1]
    total = SHARDS * TOK
    block = DIM // OWN
    shape = jax.ShapeDtypeStruct
    whole = lambda *dims: pl.BlockSpec(dims, lambda i: (0,) * len(dims))
    one = lambda *dims: pl.BlockSpec((1,) + dims, lambda i: (i, 0, 0))
    slots = lambda cols: pl.BlockSpec((PAD, cols), lambda i: (i, 0))
    cols = lambda height: pl.BlockSpec((height, block), lambda i: (0, i))
    return pl.pallas_call(
        grads_kernel,
        grid=(OWN,),
        out_shape=(
            shape((OWN, DIM, width), F32), shape((OWN, DIM, width), F32), shape((OWN, width, DIM), F32),
            shape((DIM, width), F32), shape((DIM, width), F32), shape((width, DIM), F32),
            shape((TOK, DIM), BF16), shape((TOK, DIM), BF16), shape((EXPERTS, DIM), F32),
        ),
        in_specs=[slots(DIM), slots(DIM), slots(width), slots(width), slots(width), cols(total), cols(total), whole(total, width), whole(total, width), whole(total, width), VMEM, VMEM, VMEM],
        out_specs=(one(DIM, width), one(DIM, width), one(width, DIM), pl.BlockSpec((block, width), lambda i: (i, 0)), pl.BlockSpec((block, width), lambda i: (i, 0)), cols(width), ANY, ANY, ANY),
        scratch_shapes=[pltpu.SemaphoreType.DMA((3,))],
        compiler_params=pltpu.CompilerParams(dimension_semantics=("arbitrary",), vmem_limit_bytes=63 << 20),
        cost_estimate=pl.CostEstimate(flops=8 << 30, bytes_accessed=32 << 20, transcendentals=0),
        name="weight_grads",
    )(xs, us, hid, da, db, n_all, dy_all.reshape(total, DIM), hid_s, da_s, db_s, y_out, dx_out, gr_out)


def solution(mesh):
    tok_spec = P(("dp", "ep"), None)
    id_spec = P(("dp", "ep"))
    in_specs = (tok_spec, tok_spec, id_spec, id_spec, P(None, None), P("ep", None, "etp"), P("ep", None, "etp"), P("ep", "etp", None), P(None, "etp"), P(None, "etp"), P("etp", None))
    out_specs = (tok_spec, tok_spec, P(("dp", "ep"), None, "etp"), P(("dp", "ep"), None, "etp"), P(("dp", "ep"), "etp", None), P("dp", "etp"), P("dp", "etp"), P(("dp", "etp"), None), P("dp", None))

    def local_step(x_in, y_grad, prim_exp, alt_exp, w_router, exp_gate, exp_up, exp_down, sh_gate, sh_up, sh_down):
        y, dx, gr, *saved = layer_call(x_in, y_grad, prim_exp.reshape(1, TOK), alt_exp.reshape(1, TOK), w_router.T, exp_gate, exp_up, exp_down, sh_gate, sh_up, sh_down)
        g_gate, g_up, g_down, gs_gate, gs_up, gs_down, y_out, x_grad, g_router = grads_call(*saved, y, dx, gr)
        return (y_out, x_grad, g_gate, g_up, g_down, gs_gate, gs_up, gs_down, g_router.T)

    return jax.shard_map(local_step, mesh=mesh, in_specs=in_specs, out_specs=out_specs, check_vma=False)
```

```python
import functools

import jax
import jax.numpy as jnp
from jax import lax
from jax.experimental import pallas as pl
from jax.experimental.pallas import tpu as pltpu
from jax.sharding import PartitionSpec as P

EPS = 1e-5
F32 = jnp.float32
BF16 = jnp.bfloat16
MESH = pl.DeviceIdType.MESH
ANY = pl.BlockSpec(memory_space=pl.ANY)
VMEM = pl.BlockSpec(memory_space=pltpu.VMEM)
NN = (((1,), (0,)), ((), ()))
NT = (((1,), (1,)), ((), ()))
TN = (((0,), (0,)), ((), ()))

SHARDS = 4
TOK = 128
DIM = 1024
HALF = 512
EXPERTS = 32
OWN = 8
WIDTH = 256
CAP = 20
PAD = 32
SLOTS = OWN * CAP


def mm(a, b, dims=NN):
    return lax.dot_general(a, b, dims, preferred_element_type=F32)


def inv_rms_of(x_wide):
    return lax.rsqrt(jnp.mean(x_wide * x_wide, axis=1, keepdims=True) + EPS)


def glu_grads(d_hidden, act_gate, act_up):
    sig_gate = jax.nn.sigmoid(act_gate)
    d_gate = (d_hidden * act_up * sig_gate * (1.0 + act_gate * (1.0 - sig_gate))).astype(BF16)
    d_up = (d_hidden * act_gate * sig_gate).astype(BF16)
    return d_gate, d_up


def to_row(col):
    return jnp.transpose(jnp.broadcast_to(col, (TOK, TOK)))[:8]


def to_col(row):
    return jnp.transpose(jnp.broadcast_to(row, (TOK, TOK)))[:, :1]


def barrier(peers):
    sem = pltpu.get_barrier_semaphore()
    for peer in peers:
        pl.semaphore_signal(sem, inc=1, device_id=peer, device_id_type=MESH)
    pl.semaphore_wait(sem, len(peers))


def layer_kernel(x_hbm, dy_hbm, prim_hbm, alt_hbm, wr_hbm, wg_hbm, wu_hbm, wd_hbm, sg_hbm, su_hbm, sd_hbm,
                 y_hbm, dn_hbm, gr_hbm, xs_hbm, us_hbm, h_hbm, dab_hbm, n_hbm, dy_all_hbm, sh_hbm, sdab_hbm,
                 x_all, dy_all, ids_all, wr, wg, wu, wd, sg, su, sd, n_all, xs, us, pick_own, acts, acts_up, hid, dab, hid_s, dab_s,
                 probs, meta, s_send, s_recv, s_keep, n_send, n_recv, n_keep, o_send, o_recv, o_keep, d_send, d_recv, d_keep,
                 o_all, d_all, dg_mine, dg_all, y_half, dn_half, gr_buf,
                 in_sem, w_sem, out_sem, send_sem, recv_sem, r_send_sem, r_recv_sem, y_send_sem, y_recv_sem, g_send_sem, g_recv_sem):
    me = lax.axis_index("ep")
    side = lax.axis_index("etp")
    total = SHARDS * TOK
    mate = jnp.bitwise_xor(me, 1)
    across = jnp.bitwise_xor(me, 2)
    to_mate, to_across, to_twin = {"ep": mate}, {"ep": across}, {"etp": 1 - side}
    others = [{"etp": jnp.bitwise_xor(side, k // SHARDS), "ep": jnp.bitwise_xor(me, k % SHARDS)} for k in range(1, 2 * SHARDS)]
    theirs = pl.ds(pl.multiple_of((1 - side) * HALF, HALF), HALF)
    mine = pl.ds(pl.multiple_of(side * HALF, HALF), HALF)
    home = pl.ds(pl.multiple_of(me * TOK, TOK), TOK)

    loads = [pltpu.make_async_copy(src, dst, in_sem.at[k]) for k, (src, dst) in enumerate((
        (x_hbm, x_all.at[me]), (prim_hbm, ids_all.at[me, 0:1]), (alt_hbm, ids_all.at[me, 1:2]), (dy_hbm, dy_all.at[me]),
        (sg_hbm, sg), (su_hbm, su), (sd_hbm, sd), (wr_hbm, wr)))]
    for load in loads:
        load.start()
    w_loads = [[pltpu.make_async_copy(src.at[e], dst.at[e], w_sem.at[k, e]) for k, (src, dst) in enumerate(((wg_hbm, wg), (wu_hbm, wu), (wd_hbm, wd)))] for e in range(OWN)]
    barrier(others)

    def remote(view, lane, k, target):
        return pltpu.make_async_remote_copy(src_ref=view, dst_ref=view, send_sem=send_sem.at[lane, k], recv_sem=recv_sem.at[lane, k], device_id=target, device_id_type=MESH)

    CHUNKS = (((0, 80), (80, 160)), ((0, 80), (80, 112), (112, 160)))
    READY = ((2, 4), (2, 3, 4))
    DIRECT = ((True, False), (False, True, True))
    returns = []

    def give_back(lane, chunk):
        buf, keep, recv, copies = ((o_all, o_keep, o_recv, o_copies), (d_all, d_keep, d_recv, d_copies))[lane]
        for copy in copies[READY[lane][chunk - 1] if chunk else 0 : READY[lane][chunk]]:
            copy.wait_recv()
        rows = slice(*CHUNKS[lane][chunk])
        buf[me, rows] = (keep[rows, :] + recv[rows, :]).astype(BF16)

        def send(owner, k, j):
            view = buf.at[owner, rows]
            return pltpu.make_async_remote_copy(src_ref=view, dst_ref=view, send_sem=r_send_sem.at[lane, chunk, j], recv_sem=r_recv_sem.at[lane, chunk, j], device_id={"ep": jnp.bitwise_xor(me, k)}, device_id_type=MESH)

        group = [send(me, 2, 0), send(me, 1, 1), send(me, 3, 2) if DIRECT[lane][chunk] else send(across, 1, 2)]
        for copy in group if DIRECT[lane][chunk] else group[:2]:
            copy.start()
        returns.append(group)
        return group

    def pass_on(group):
        group[0].wait_recv()
        group[2].start()

    def arrived(group, forwarded):
        for copy in group[1:] if forwarded else group:
            copy.wait_recv()

    def twin(src, dst, k):
        return pltpu.make_async_remote_copy(src_ref=src, dst_ref=dst, send_sem=y_send_sem.at[k], recv_sem=y_recv_sem.at[k], device_id=to_twin, device_id_type=MESH)

    def pieces(shard):
        rows = TOK // 2
        return [ids_all.at[shard], x_all.at[shard, :rows], x_all.at[shard, rows:], dy_all.at[shard, :rows], dy_all.at[shard, rows:]]

    out_across = [remote(view, 0, k, to_across) for k, view in enumerate(pieces(me))]
    out_mate = [remote(view, 1, k, to_mate) for k, view in enumerate(pieces(me))]
    forwards = [remote(view, 2, k, to_mate) for k, view in enumerate(pieces(across))]
    for load in loads[:3]:
        load.wait()
    for k in range(3):
        out_across[k].start()
        out_mate[k].start()
    loads[3].wait()
    for k in range(3, 5):
        out_across[k].start()
        out_mate[k].start()
    for group in w_loads:
        for load in group:
            load.start()

    x_wide = x_all[me].astype(F32)
    normed = (x_wide * inv_rms_of(x_wide)).astype(BF16)
    for load in loads[4:7]:
        load.wait()
    act_gate = mm(normed, sg[...])
    act_up = mm(normed, su[...])
    hidden = (jax.nn.silu(act_gate) * act_up).astype(BF16)
    d_gate, d_up = glu_grads(mm(dy_all[me], sd[...], NT), act_gate, act_up)
    n_send[...] = mm(d_gate, sg[theirs, :], NT) + mm(d_up, su[theirs, :], NT)
    n_copy = twin(n_send, n_recv, 0)
    n_copy.start()
    s_send[...] = mm(hidden, sd[:, theirs])
    s_copies = [twin(s_send.at[k * (TOK // 2) : (k + 1) * (TOK // 2)], s_recv.at[k * (TOK // 2) : (k + 1) * (TOK // 2)], 12 + k) for k in range(2)]
    s_copies[0].start()
    n_keep[...] = mm(d_gate, sg[mine, :], NT) + mm(d_up, su[mine, :], NT)
    s_keep[...] = mm(hidden, sd[:, mine])

    def norm(shard):
        rows = x_all[shard].astype(F32)
        n_all[pl.ds(pl.multiple_of(shard * TOK, TOK), TOK), :] = (rows * inv_rms_of(rows)).astype(BF16)

    n_all[home, :] = normed
    out_across[0].wait_recv()
    forwards[0].start()
    for copy in (out_mate[0], forwards[0]):
        copy.wait_recv()
    prim = jnp.concatenate([ids_all[s, 0:1, :] for s in range(SHARDS)], axis=1)
    alt = jnp.concatenate([ids_all[s, 1:2, :] for s in range(SHARDS)], axis=1)
    expert = lax.broadcasted_iota(jnp.int32, (EXPERTS, total), 0)
    before = (lax.broadcasted_iota(jnp.int32, (total, total), 0) < lax.broadcasted_iota(jnp.int32, (total, total), 1)).astype(F32).astype(BF16)
    one_prim = (expert == prim).astype(F32)
    rank_prim = jnp.sum(one_prim * mm(one_prim.astype(BF16), before), axis=0, keepdims=True)
    keep_prim = rank_prim < CAP
    kept = jnp.minimum(jnp.sum(one_prim, axis=1, keepdims=True), float(CAP))
    one_alt = jnp.where(keep_prim, 0.0, (expert == alt).astype(F32))
    slot_alt = jnp.sum(one_alt * (mm(one_alt.astype(BF16), before) + kept), axis=0, keepdims=True)
    keep_alt = jnp.logical_and(jnp.logical_not(keep_prim), slot_alt < CAP)
    assign = jnp.where(keep_prim, prim, jnp.where(keep_alt, alt, -1))
    slot = jnp.where(keep_prim, rank_prim, slot_alt).astype(jnp.int32)
    meta[0:1] = assign.astype(F32)
    meta[1:2] = jnp.where(assign >= 0, assign * CAP + slot, -1).astype(F32)
    local = assign - me * OWN
    owned = jnp.logical_and(local >= 0, local < OWN)
    target = jnp.where(owned, local * PAD + slot, -1)
    pick_own[...] = (lax.broadcasted_iota(jnp.int32, (OWN * PAD, total), 0) == target).astype(F32).astype(BF16)

    for k in range(1, 3):
        out_mate[k].wait_recv()
    norm(mate)
    for k in range(1, 3):
        out_across[k].wait_recv()
        forwards[k].start()
    norm(across)
    for k in range(1, 3):
        forwards[k].wait_recv()
    norm(jnp.bitwise_xor(me, 3))
    xs[...] = mm(pick_own[...], n_all[...]).astype(BF16)

    o_copies, d_copies = [], []
    for e in range(OWN):
        for load in w_loads[e]:
            load.wait()
        rows = slice(e * PAD, (e + 1) * PAD)
        act_gate = mm(xs[rows, :], wg[e])
        act_up = mm(xs[rows, :], wu[e])
        hidden = (jax.nn.silu(act_gate) * act_up).astype(BF16)
        acts[rows, :] = act_gate
        acts_up[rows, :] = act_up
        hid[rows, :] = hidden
        part = slice(e * CAP, (e + 1) * CAP)
        o_send[part, :] = mm(hidden, wd[e, :, theirs])[:CAP]
        o_keep[part, :] = mm(hidden, wd[e, :, mine])[:CAP]
        if e % 2:
            chunk = slice((e - 1) * CAP, (e + 1) * CAP)
            o_copies.append(twin(o_send.at[chunk], o_recv.at[chunk], 2 + e // 2))
            o_copies[-1].start()
        if e in (1, 4):
            k = 3 if e == 1 else 4
            out_across[k].wait_recv()
            forwards[k].start()
    loads[7].wait()
    logits = mm(n_all[...], wr[...], NT)
    top = jnp.max(logits, axis=1, keepdims=True)
    expo = jnp.exp(logits - top)
    share = expo / jnp.sum(expo, axis=1, keepdims=True)
    wide = jnp.concatenate([share, jnp.zeros((total, TOK - EXPERTS), F32)], axis=1)
    probs_t = jnp.concatenate([jnp.transpose(wide[s * TOK : (s + 1) * TOK])[:EXPERTS] for s in range(SHARDS)], axis=1)
    probs[...] = probs_t
    one_assign = lax.broadcasted_iota(jnp.int32, (EXPERTS, total), 0) == meta[0:1, :].astype(jnp.int32)
    gate = jnp.sum(jnp.where(one_assign, probs_t, 0.0), axis=0, keepdims=True)
    meta[2:3] = gate
    gate_slot = jnp.sum(pick_own[...].astype(F32) * gate, axis=1, keepdims=True)
    for k in range(3, 5):
        out_mate[k].wait_recv()
        forwards[k].wait_recv()
    us[...] = (gate_slot * mm(pick_own[...], dy_all[...].reshape(total, DIM))).astype(BF16)

    for e in range(OWN):
        rows = slice(e * PAD, (e + 1) * PAD)
        d_gate, d_up = glu_grads(mm(us[rows, :], wd[e], NT), acts[rows, :], acts_up[rows, :])
        dab[rows, :WIDTH] = d_gate
        dab[rows, WIDTH:] = d_up
        part = slice(e * CAP, (e + 1) * CAP)
        d_send[part, :] = (mm(d_gate, wg[e, theirs, :], NT) + mm(d_up, wu[e, theirs, :], NT))[:CAP]
        d_keep[part, :] = (mm(d_gate, wg[e, mine, :], NT) + mm(d_up, wu[e, mine, :], NT))[:CAP]
        if e % 2:
            chunk = slice((e - 1) * CAP, (e + 1) * CAP)
            d_copies.append(twin(d_send.at[chunk], d_recv.at[chunk], 6 + e // 2))
            d_copies[-1].start()
        if e == 3:
            o_first = give_back(0, 0)

    s_copies[1].start()
    o_second = give_back(0, 1)

    saves = [pltpu.make_async_copy(src, dst, out_sem.at[k]) for k, (src, dst) in enumerate((
        (xs, xs_hbm), (us, us_hbm), (hid, h_hbm), (dab, dab_hbm), (n_all, n_hbm), (dy_all, dy_all_hbm), (hid_s, sh_hbm), (dab_s, sdab_hbm), (y_half, y_hbm), (gr_buf, gr_hbm), (dn_half, dn_hbm)))]
    save_y, save_gr, save_dn = saves[8:]
    saves = saves[:8]
    for save in saves[:6]:
        save.start()
    act_gate = mm(n_all[...], sg[...])
    act_up = mm(n_all[...], su[...])
    hid_s[...] = (jax.nn.silu(act_gate) * act_up).astype(BF16)
    d_gate, d_up = glu_grads(mm(dy_all[...].reshape(total, DIM), sd[...], NT), act_gate, act_up)
    dab_s[:, :WIDTH] = d_gate
    dab_s[:, WIDTH:] = d_up
    for save in saves[6:]:
        save.start()

    x_half = x_all[me, :, mine].astype(F32)
    dy_half = dy_all[me, :, mine].astype(F32)
    gate_home = to_col(meta[2:3, home])
    flat_home = to_col(meta[1:2, home]).astype(jnp.int32)
    pick = (lax.broadcasted_iota(jnp.int32, (TOK, SHARDS * SLOTS), 1) == flat_home).astype(F32).astype(BF16)
    d_first = give_back(1, 0)
    pass_on(o_second)
    arrived(o_first, False)
    d_second = give_back(1, 1)
    arrived(o_second, True)
    tok_out = mm(pick, o_all[...].reshape(SHARDS * SLOTS, HALF))
    dg_mine[...] = to_row(jnp.sum(dy_half * tok_out, axis=1, keepdims=True))
    place = side * SHARDS + me
    dg_copies = [pltpu.make_async_remote_copy(src_ref=dg_mine, dst_ref=dg_all.at[place], send_sem=g_send_sem.at[k], recv_sem=g_recv_sem.at[k], device_id=other, device_id_type=MESH) for k, other in enumerate(others)]
    for copy in dg_copies:
        copy.start()
    dg_all[place] = dg_mine[...]
    d_third = give_back(1, 2)
    pass_on(d_first)
    for copy in s_copies:
        copy.wait_recv()
    y_half[...] = (x_half + (s_keep[...] + s_recv[...]) + gate_home * tok_out).astype(BF16)
    save_y.start()
    for copy in dg_copies:
        copy.wait_recv()
    dg = jnp.concatenate([dg_all[s, 0:1, :] + dg_all[SHARDS + s, 0:1, :] for s in range(SHARDS)], axis=1)
    one_assign = (lax.broadcasted_iota(jnp.int32, (EXPERTS, total), 0) == meta[0:1, :].astype(jnp.int32)).astype(F32)
    d_logits = (dg * meta[2:3, :] * (one_assign - probs[...])).astype(BF16)
    home_one = (lax.broadcasted_iota(jnp.int32, (EXPERTS, TOK), 0) == meta[0:1, home].astype(jnp.int32)).astype(F32)
    dg_home = dg_all[me, 0:1, :] + dg_all[SHARDS + me, 0:1, :]
    d_logits_home = (dg_home * meta[2:3, home] * (home_one - probs[:, home])).astype(BF16)
    n_copy.wait_recv()
    d_normed = n_keep[...] + n_recv[...] + mm(d_logits_home, wr[:, mine], TN)
    gr_buf[...] = mm(d_logits, n_all[...])
    save_gr.start()
    arrived(d_second, False)
    arrived(d_first, True)
    arrived(d_third, False)
    dn_half[...] = d_normed + mm(pick, d_all[...].reshape(SHARDS * SLOTS, HALF))
    save_dn.start()
    for copy in out_across + out_mate + forwards + [n_copy] + s_copies + o_copies + d_copies + sum(returns, []) + dg_copies:
        copy.wait_send()
    for save in saves + [save_y, save_gr, save_dn]:
        save.wait()


def layer_call(x_in, y_grad, prim, alt, wr_t, exp_gate, exp_up, exp_down, sh_gate, sh_up, sh_down):
    width = sh_gate.shape[1]
    total = SHARDS * TOK
    rows = OWN * PAD
    shape = jax.ShapeDtypeStruct
    dma = pltpu.SemaphoreType.DMA
    half_f32 = pltpu.VMEM((TOK, HALF), F32)
    slots_f32 = pltpu.VMEM((SLOTS, HALF), F32)
    return pl.pallas_call(
        layer_kernel,
        out_shape=(
            shape((TOK, HALF), BF16), shape((TOK, HALF), F32), shape((EXPERTS, DIM), F32),
            shape((rows, DIM), BF16), shape((rows, DIM), BF16), shape((rows, width), BF16), shape((rows, 2 * width), BF16),
            shape((total, DIM), BF16), shape((SHARDS, TOK, DIM), BF16), shape((total, width), BF16), shape((total, 2 * width), BF16),
        ),
        in_specs=[ANY] * 11,
        out_specs=(ANY,) * 11,
        scratch_shapes=[
            pltpu.VMEM((SHARDS, TOK, DIM), BF16), pltpu.VMEM((SHARDS, TOK, DIM), BF16), pltpu.VMEM((SHARDS, 8, TOK), jnp.int32), pltpu.VMEM((EXPERTS, DIM), BF16),
            pltpu.VMEM((OWN, DIM, width), BF16), pltpu.VMEM((OWN, DIM, width), BF16), pltpu.VMEM((OWN, width, DIM), BF16),
            pltpu.VMEM((DIM, width), BF16), pltpu.VMEM((DIM, width), BF16), pltpu.VMEM((width, DIM), BF16),
            pltpu.VMEM((total, DIM), BF16), pltpu.VMEM((rows, DIM), BF16), pltpu.VMEM((rows, DIM), BF16), pltpu.VMEM((rows, total), BF16),
            pltpu.VMEM((rows, width), F32), pltpu.VMEM((rows, width), F32), pltpu.VMEM((rows, width), BF16), pltpu.VMEM((rows, 2 * width), BF16),
            pltpu.VMEM((total, width), BF16), pltpu.VMEM((total, 2 * width), BF16),
            pltpu.VMEM((EXPERTS, total), F32), pltpu.VMEM((8, total), F32),
            half_f32, half_f32, half_f32, half_f32, half_f32, half_f32,
            slots_f32, slots_f32, slots_f32, slots_f32, slots_f32, slots_f32,
            pltpu.VMEM((SHARDS, SLOTS, HALF), BF16), pltpu.VMEM((SHARDS, SLOTS, HALF), BF16),
            pltpu.VMEM((8, TOK), F32), pltpu.VMEM((2 * SHARDS, 8, TOK), F32), pltpu.VMEM((TOK, HALF), BF16), half_f32, pltpu.VMEM((EXPERTS, DIM), F32),
            dma((8,)), dma((3, OWN)), dma((11,)), dma((3, 5)), dma((3, 5)), dma((2, 3, 3)), dma((2, 3, 3)), dma((14,)), dma((14,)), dma((7,)), dma((7,)),
        ],
        compiler_params=pltpu.CompilerParams(collective_id=0, has_side_effects=True, vmem_limit_bytes=60 << 20),
        name="moe_layer",
    )(x_in, y_grad, prim, alt, wr_t, exp_gate, exp_up, exp_down, sh_gate, sh_up, sh_down)


def grads_kernel(xs_hbm, us_hbm, h_hbm, dab_hbm, n_hbm, dy_hbm, sh_hbm, sdab_hbm, gr_hbm, g_gate_hbm, g_up_hbm, g_down_hbm, gs_gate_hbm, gs_up_hbm, gs_down_hbm, g_router_hbm,
                 xs, us, hid, dab, n_all, dy_all, hid_s, dab_s, g_router, g_gate, g_up, g_down, gs_gate, gs_up, gs_down, in_sem, out_sem, sh_sem):
    loads = [pltpu.make_async_copy(src, dst, in_sem.at[k]) for k, (src, dst) in enumerate((
        (h_hbm, hid), (us_hbm, us), (xs_hbm, xs), (dab_hbm, dab), (n_hbm, n_all), (sdab_hbm, dab_s), (sh_hbm, hid_s), (dy_hbm, dy_all), (gr_hbm, g_router)))]
    for load in loads:
        load.start()
    writes = []

    def write(src, dst, sem):
        writes.append(pltpu.make_async_copy(src, dst, sem))
        writes[-1].start()

    for load in loads[:2]:
        load.wait()
    for e in range(OWN):
        rows = slice(e * PAD, (e + 1) * PAD)
        g_down[e] = mm(hid[rows, :], us[rows, :], TN)
        write(g_down.at[e], g_down_hbm.at[e], out_sem.at[0, e])
        if e == 0:
            for load in loads[2:4]:
                load.wait()
        both = mm(xs[rows, :], dab[rows, :], TN)
        g_gate[e] = both[:, :WIDTH]
        g_up[e] = both[:, WIDTH:]
        write(g_gate.at[e], g_gate_hbm.at[e], out_sem.at[1, e])
        write(g_up.at[e], g_up_hbm.at[e], out_sem.at[2, e])
    for load in loads[4:]:
        load.wait()
    both = mm(n_all[...], dab_s[...], TN)
    gs_gate[...] = both[:, :WIDTH]
    gs_up[...] = both[:, WIDTH:]
    write(gs_gate, gs_gate_hbm, sh_sem.at[0])
    write(gs_up, gs_up_hbm, sh_sem.at[1])
    gs_down[...] = mm(hid_s[...], dy_all[...], TN)
    write(gs_down, gs_down_hbm, sh_sem.at[2])
    write(g_router, g_router_hbm, sh_sem.at[3])
    for copy in writes:
        copy.wait()


def grads_call(*saved):
    shape = jax.ShapeDtypeStruct
    outs = ((OWN, DIM, WIDTH), (OWN, DIM, WIDTH), (OWN, WIDTH, DIM), (DIM, WIDTH), (DIM, WIDTH), (WIDTH, DIM), (EXPERTS, DIM))
    return pl.pallas_call(
        grads_kernel,
        out_shape=tuple(shape(dims, F32) for dims in outs),
        in_specs=[ANY] * 9,
        out_specs=(ANY,) * 7,
        scratch_shapes=[pltpu.VMEM(a.shape, a.dtype) for a in saved] + [pltpu.VMEM(dims, F32) for dims in outs[:-1]] + [pltpu.SemaphoreType.DMA((9,)), pltpu.SemaphoreType.DMA((3, OWN)), pltpu.SemaphoreType.DMA((4,))],
        compiler_params=pltpu.CompilerParams(vmem_limit_bytes=63 << 20),
        cost_estimate=pl.CostEstimate(flops=8 << 30, bytes_accessed=32 << 20, transcendentals=0),
        name="weight_grads",
    )(*saved)


def finish_kernel(x_ref, dy_ref, y_mine, y_recv, dn_mine, dn_recv, y_out, dx_out):
    side = lax.axis_index("etp")
    theirs = pl.ds(pl.multiple_of((1 - side) * HALF, HALF), HALF)
    mine = pl.ds(pl.multiple_of(side * HALF, HALF), HALF)
    y_out[:, mine] = y_mine[...]
    y_out[:, theirs] = y_recv[...]
    x_wide = x_ref[...].astype(F32)
    inv_rms = inv_rms_of(x_wide)
    halves = ((mine, dn_mine), (theirs, dn_recv))
    norm_proj = sum(jnp.sum(dn[...] * x_ref[:, cols].astype(F32), axis=1, keepdims=True) for cols, dn in halves) / DIM
    for cols, dn in halves:
        dx_out[:, cols] = (dy_ref[:, cols].astype(F32) + inv_rms * dn[...] - x_ref[:, cols].astype(F32) * inv_rms**3 * norm_proj).astype(BF16)


def finish_call(*args):
    shape = jax.ShapeDtypeStruct
    return pl.pallas_call(
        finish_kernel,
        out_shape=(shape((TOK, DIM), BF16), shape((TOK, DIM), BF16)),
        in_specs=[VMEM] * 6,
        out_specs=(VMEM,) * 2,
        compiler_params=pltpu.CompilerParams(vmem_limit_bytes=8 << 20),
        name="finish_tokens",
    )(*args)


def solution(mesh):
    tok_spec = P(("dp", "ep"), None)
    id_spec = P(("dp", "ep"))
    in_specs = (tok_spec, tok_spec, id_spec, id_spec, P(None, None), P("ep", None, "etp"), P("ep", None, "etp"), P("ep", "etp", None), P(None, "etp"), P(None, "etp"), P("etp", None))
    out_specs = (tok_spec, tok_spec, P(("dp", "ep"), None, "etp"), P(("dp", "ep"), None, "etp"), P(("dp", "ep"), "etp", None), P("dp", "etp"), P("dp", "etp"), P(("dp", "etp"), None), P("dp", None))

    def local_step(x_in, y_grad, prim_exp, alt_exp, w_router, exp_gate, exp_up, exp_down, sh_gate, sh_up, sh_down):
        y_half, dn_half, gr, xs, us, hid, dab, n_all, dy_all, hid_s, dab_s = layer_call(x_in, y_grad, prim_exp.reshape(1, TOK), alt_exp.reshape(1, TOK), w_router.T, exp_gate, exp_up, exp_down, sh_gate, sh_up, sh_down)
        swap = [(0, 1), (1, 0)]
        dn_other = lax.ppermute(dn_half, "etp", swap)
        y_other = lax.ppermute(y_half, "etp", swap)
        g_gate, g_up, g_down, gs_gate, gs_up, gs_down, g_router = grads_call(xs, us, hid, dab, n_all, dy_all.reshape(SHARDS * TOK, DIM), hid_s, dab_s, gr)
        y_out, x_grad = finish_call(x_in, y_grad, y_half, y_other, dn_half, dn_other)
        return (y_out, x_grad, g_gate, g_up, g_down, gs_gate, gs_up, gs_down, g_router.T)

    return jax.shard_map(local_step, mesh=mesh, in_specs=in_specs, out_specs=out_specs, check_vma=False)
```

```python
import functools

import jax
import jax.numpy as jnp
from jax import lax
from jax.experimental import pallas as pl
from jax.experimental.pallas import tpu as pltpu
from jax.sharding import PartitionSpec as P

EPS = 1e-5
F32 = jnp.float32
BF16 = jnp.bfloat16
MESH = pl.DeviceIdType.MESH
ANY = pl.BlockSpec(memory_space=pl.ANY)
VMEM = pl.BlockSpec(memory_space=pltpu.VMEM)
NN = (((1,), (0,)), ((), ()))
NT = (((1,), (1,)), ((), ()))
TN = (((0,), (0,)), ((), ()))

SHARDS = 4
TOK = 128
DIM = 1024
HALF = 512
EXPERTS = 32
OWN = 8
WIDTH = 256
CAP = 20
PAD = 32
SLOTS = OWN * CAP


def mm(a, b, dims=NN):
    return lax.dot_general(a, b, dims, preferred_element_type=F32)


def inv_rms_of(x_wide):
    return lax.rsqrt(jnp.mean(x_wide * x_wide, axis=1, keepdims=True) + EPS)


def glu_grads(d_hidden, act_gate, act_up):
    sig_gate = jax.nn.sigmoid(act_gate)
    d_gate = (d_hidden * act_up * sig_gate * (1.0 + act_gate * (1.0 - sig_gate))).astype(BF16)
    d_up = (d_hidden * act_gate * sig_gate).astype(BF16)
    return d_gate, d_up


def to_row(col):
    return jnp.transpose(jnp.broadcast_to(col, (TOK, TOK)))[:8]


def to_col(row):
    return jnp.transpose(jnp.broadcast_to(row, (TOK, TOK)))[:, :1]


def barrier(peers):
    sem = pltpu.get_barrier_semaphore()
    for peer in peers:
        pl.semaphore_signal(sem, inc=1, device_id=peer, device_id_type=MESH)
    pl.semaphore_wait(sem, len(peers))


def layer_kernel(x_hbm, dy_hbm, prim_hbm, alt_hbm, wr_hbm, wg_hbm, wu_hbm, wd_hbm, sg_hbm, su_hbm, sd_hbm,
                 y_hbm, dn_hbm, gr_hbm, xs_hbm, us_hbm, h_hbm, dab_hbm, n_hbm, dy_all_hbm, sh_hbm, sdab_hbm,
                 x_all, dy_all, ids_all, wr, wg, wu, wd, sg, su, sd, n_all, xs, us, pick_own, acts, acts_up, hid, dab, hid_s, dab_s,
                 probs, meta, hid_own, hid_twin, sd_twin, s_keep, n_send, n_recv, n_keep, o_send, o_recv, o_keep, d_send, d_recv, d_keep,
                 o_all, d_all, dg_mine, dg_all, y_half, dn_half, gr_buf,
                 in_sem, w_sem, out_sem, send_sem, recv_sem, r_send_sem, r_recv_sem, y_send_sem, y_recv_sem, g_send_sem, g_recv_sem, q_send_sem, q_recv_sem):
    me = lax.axis_index("ep")
    side = lax.axis_index("etp")
    total = SHARDS * TOK
    mate = jnp.bitwise_xor(me, 1)
    across = jnp.bitwise_xor(me, 2)
    to_mate, to_across, to_twin = {"ep": mate}, {"ep": across}, {"etp": 1 - side}
    others = [{"etp": jnp.bitwise_xor(side, k // SHARDS), "ep": jnp.bitwise_xor(me, k % SHARDS)} for k in range(1, 2 * SHARDS)]
    theirs = pl.ds(pl.multiple_of((1 - side) * HALF, HALF), HALF)
    mine = pl.ds(pl.multiple_of(side * HALF, HALF), HALF)
    home = pl.ds(pl.multiple_of(me * TOK, TOK), TOK)

    loads = [pltpu.make_async_copy(src, dst, in_sem.at[k]) for k, (src, dst) in enumerate((
        (x_hbm, x_all.at[me]), (prim_hbm, ids_all.at[me, 0:1]), (alt_hbm, ids_all.at[me, 1:2]), (dy_hbm, dy_all.at[me]),
        (sg_hbm, sg), (su_hbm, su), (sd_hbm, sd), (wr_hbm, wr)))]
    for load in loads:
        load.start()
    w_loads = [pltpu.make_async_copy(src, dst, w_sem.at[k]) for k, (src, dst) in enumerate(((wg_hbm, wg), (wu_hbm, wu), (wd_hbm, wd)))]
    barrier(others)

    def remote(view, lane, k, target):
        return pltpu.make_async_remote_copy(src_ref=view, dst_ref=view, send_sem=send_sem.at[(k + 1) // 2], recv_sem=recv_sem.at[lane, k], device_id=target, device_id_type=MESH)

    def twin(src, dst, k, group):
        return pltpu.make_async_remote_copy(src_ref=src, dst_ref=dst, send_sem=y_send_sem.at[group], recv_sem=y_recv_sem.at[k], device_id=to_twin, device_id_type=MESH)

    def pieces(shard):
        rows = TOK // 2
        return [ids_all.at[shard], x_all.at[shard, :rows], x_all.at[shard, rows:], dy_all.at[shard, :rows], dy_all.at[shard, rows:]]

    out_across = [remote(view, 0, k, to_across) for k, view in enumerate(pieces(me))]
    out_mate = [remote(view, 1, k, to_mate) for k, view in enumerate(pieces(me))]
    forwards = [remote(view, 2, k, to_mate) for k, view in enumerate(pieces(across))]
    def quarter(shard):
        return pl.ds(pl.multiple_of(shard * (WIDTH // SHARDS), WIDTH // SHARDS), WIDTH // SHARDS)

    sd_copy = twin(sd_hbm.at[quarter(me), theirs], sd_twin.at[quarter(me)], 2, 2)
    sd_copy.start()
    for load in loads[:3]:
        load.wait()
    for k in range(3):
        out_across[k].start()
        out_mate[k].start()
    loads[3].wait()
    for k in range(3, 5):
        out_across[k].start()
        out_mate[k].start()
    for load in w_loads:
        load.start()

    x_wide = x_all[me].astype(F32)
    normed = (x_wide * inv_rms_of(x_wide)).astype(BF16)
    for load in loads[4:7]:
        load.wait()
    act_gate = mm(normed, sg[...])
    act_up = mm(normed, su[...])
    hidden = (jax.nn.silu(act_gate) * act_up).astype(BF16)
    d_gate, d_up = glu_grads(mm(dy_all[me], sd[...], NT), act_gate, act_up)
    n_send[...] = mm(d_gate, sg[theirs, :], NT) + mm(d_up, su[theirs, :], NT)
    n_copy = twin(n_send, n_recv, 0, 0)
    n_copy.start()
    hid_own[...] = hidden
    h_copy = twin(hid_own, hid_twin, 1, 1)
    h_copy.start()
    n_keep[...] = mm(d_gate, sg[mine, :], NT) + mm(d_up, su[mine, :], NT)
    s_keep[...] = mm(hidden, sd[:, mine])

    def norm(shard):
        rows = x_all[shard].astype(F32)
        n_all[pl.ds(pl.multiple_of(shard * TOK, TOK), TOK), :] = (rows * inv_rms_of(rows)).astype(BF16)

    n_all[home, :] = normed
    out_across[0].wait_recv()
    forwards[0].start()
    for copy in (out_mate[0], forwards[0]):
        copy.wait_recv()
    prim = jnp.concatenate([ids_all[s, 0:1, :] for s in range(SHARDS)], axis=1)
    alt = jnp.concatenate([ids_all[s, 1:2, :] for s in range(SHARDS)], axis=1)
    expert = lax.broadcasted_iota(jnp.int32, (EXPERTS, total), 0)
    before = (lax.broadcasted_iota(jnp.int32, (total, total), 0) < lax.broadcasted_iota(jnp.int32, (total, total), 1)).astype(F32).astype(BF16)
    one_prim = (expert == prim).astype(F32)
    rank_prim = jnp.sum(one_prim * mm(one_prim.astype(BF16), before), axis=0, keepdims=True)
    keep_prim = rank_prim < CAP
    kept = jnp.minimum(jnp.sum(one_prim, axis=1, keepdims=True), float(CAP))
    one_alt = jnp.where(keep_prim, 0.0, (expert == alt).astype(F32))
    slot_alt = jnp.sum(one_alt * (mm(one_alt.astype(BF16), before) + kept), axis=0, keepdims=True)
    keep_alt = jnp.logical_and(jnp.logical_not(keep_prim), slot_alt < CAP)
    assign = jnp.where(keep_prim, prim, jnp.where(keep_alt, alt, -1))
    slot = jnp.where(keep_prim, rank_prim, slot_alt).astype(jnp.int32)
    meta[0:1] = assign.astype(F32)
    meta[1:2] = jnp.where(assign >= 0, assign * CAP + slot, -1).astype(F32)
    local = assign - me * OWN
    owned = jnp.logical_and(local >= 0, local < OWN)
    target = jnp.where(owned, local * PAD + slot, -1)
    pick_own[...] = (lax.broadcasted_iota(jnp.int32, (OWN * PAD, total), 0) == target).astype(F32).astype(BF16)

    sd_copy.wait_recv()
    view = sd_twin.at[quarter(me)]
    sd_spread = [pltpu.make_async_remote_copy(src_ref=view, dst_ref=view, send_sem=q_send_sem.at[0], recv_sem=q_recv_sem.at[k - 1], device_id={"ep": jnp.bitwise_xor(me, k)}, device_id_type=MESH) for k in range(1, SHARDS)]
    for copy in sd_spread:
        copy.start()
    for k in range(1, 3):
        out_mate[k].wait_recv()
    norm(mate)
    for k in range(1, 3):
        out_across[k].wait_recv()
        forwards[k].start()
    norm(across)
    for k in range(1, 3):
        forwards[k].wait_recv()
    norm(jnp.bitwise_xor(me, 3))
    xs[...] = mm(pick_own[...], n_all[...]).astype(BF16)

    o_copies, d_copies = [], []
    for e in range(OWN):
        if e == 0:
            for load in w_loads:
                load.wait()
        rows = slice(e * PAD, (e + 1) * PAD)
        act_gate = mm(xs[rows, :], wg[e])
        act_up = mm(xs[rows, :], wu[e])
        hidden = (jax.nn.silu(act_gate) * act_up).astype(BF16)
        acts[rows, :] = act_gate
        acts_up[rows, :] = act_up
        hid[rows, :] = hidden
        part = slice(e * CAP, (e + 1) * CAP)
        o_send[part, :] = mm(hidden, wd[e, :, theirs])[:CAP]
        o_keep[part, :] = mm(hidden, wd[e, :, mine])[:CAP]
        if e % 2:
            chunk = slice((e - 1) * CAP, (e + 1) * CAP)
            o_copies.append(twin(o_send.at[chunk], o_recv.at[chunk], 3 + e // 2, 3))
            o_copies[-1].start()
        if e == 5:
            out_across[3].wait_recv()
            forwards[3].start()
    D_PIECES = {1: (0, 40), 3: (40, 80), 5: (80, 120), 6: (120, 136), 7: (136, 160)}
    CHUNKS = (((0, 80), (80, 160)), ((0, 80), (80, 128), (128, 160)))
    READY = ((2, 4), (2, 4, 5))
    DIRECT = ((True, False), (False, False, True))

    def give_back(lane, chunk):
        buf, keep, recv, copies = ((o_all, o_keep, o_recv, o_copies), (d_all, d_keep, d_recv, d_copies))[lane]
        for copy in copies[READY[lane][chunk - 1] if chunk else 0 : READY[lane][chunk]]:
            copy.wait_recv()
        rows = slice(*CHUNKS[lane][chunk])
        buf[me, rows] = (keep[rows, :] + recv[rows, :]).astype(BF16)

        def send(owner, k, j):
            view = buf.at[owner, rows]
            return pltpu.make_async_remote_copy(src_ref=view, dst_ref=view, send_sem=r_send_sem.at[lane], recv_sem=r_recv_sem.at[lane, chunk, j], device_id={"ep": jnp.bitwise_xor(me, k)}, device_id_type=MESH)

        group = [send(me, 2, 0), send(me, 1, 1), send(me, 3, 2) if DIRECT[lane][chunk] else send(across, 1, 2)]
        for copy in group if DIRECT[lane][chunk] else group[:2]:
            copy.start()
        return group

    def pass_on(group):
        group[0].wait_recv()
        group[2].start()

    def arrived(group, forwarded):
        for copy in group[1:] if forwarded else group:
            copy.wait_recv()

    @pl.when(me % 2 == 1)
    def forward_early():
        out_across[4].wait_recv()
        forwards[4].start()

    loads[7].wait()
    logits = mm(n_all[...], wr[...], NT)
    top = jnp.max(logits, axis=1, keepdims=True)
    expo = jnp.exp(logits - top)
    share = expo / jnp.sum(expo, axis=1, keepdims=True)
    wide = jnp.concatenate([share, jnp.zeros((total, TOK - EXPERTS), F32)], axis=1)
    probs_t = jnp.concatenate([jnp.transpose(wide[s * TOK : (s + 1) * TOK])[:EXPERTS] for s in range(SHARDS)], axis=1)
    probs[...] = probs_t
    one_assign = lax.broadcasted_iota(jnp.int32, (EXPERTS, total), 0) == meta[0:1, :].astype(jnp.int32)
    gate = jnp.sum(jnp.where(one_assign, probs_t, 0.0), axis=0, keepdims=True)
    meta[2:3] = gate
    gate_slot = jnp.sum(pick_own[...].astype(F32) * gate, axis=1, keepdims=True)
    @pl.when(me % 2 == 0)
    def forward_late():
        out_across[4].wait_recv()
        forwards[4].start()

    for k in range(3, 5):
        out_mate[k].wait_recv()
        forwards[k].wait_recv()
    us[...] = (gate_slot * mm(pick_own[...], dy_all[...].reshape(total, DIM))).astype(BF16)

    for e in range(OWN):
        rows = slice(e * PAD, (e + 1) * PAD)
        d_gate, d_up = glu_grads(mm(us[rows, :], wd[e], NT), acts[rows, :], acts_up[rows, :])
        dab[rows, :WIDTH] = d_gate
        dab[rows, WIDTH:] = d_up
        part = slice(e * CAP, (e + 1) * CAP)
        d_send[part, :] = (mm(d_gate, wg[e, theirs, :], NT) + mm(d_up, wu[e, theirs, :], NT))[:CAP]
        d_keep[part, :] = (mm(d_gate, wg[e, mine, :], NT) + mm(d_up, wu[e, mine, :], NT))[:CAP]
        if e in D_PIECES:
            chunk = slice(*D_PIECES[e])
            d_copies.append(twin(d_send.at[chunk], d_recv.at[chunk], 7 + len(d_copies), 4))
            d_copies[-1].start()
        if e == 1:
            o_first = give_back(0, 0)
        if e == 5:
            o_second = give_back(0, 1)


    saves = [pltpu.make_async_copy(src, dst, out_sem.at[k]) for k, (src, dst) in enumerate((
        (xs, xs_hbm), (us, us_hbm), (hid, h_hbm), (dab, dab_hbm), (n_all, n_hbm), (dy_all, dy_all_hbm), (hid_s, sh_hbm), (dab_s, sdab_hbm), (y_half, y_hbm.at[:, mine]), (gr_buf, gr_hbm), (dn_half, dn_hbm)))]
    save_y, save_gr, save_dn = saves[8:]
    saves = saves[:8]
    for save in saves[:6]:
        save.start()
    act_gate = mm(n_all[...], sg[...])
    act_up = mm(n_all[...], su[...])
    hid_s[...] = (jax.nn.silu(act_gate) * act_up).astype(BF16)
    d_gate, d_up = glu_grads(mm(dy_all[...].reshape(total, DIM), sd[...], NT), act_gate, act_up)
    dab_s[:, :WIDTH] = d_gate
    dab_s[:, WIDTH:] = d_up
    for save in saves[6:]:
        save.start()

    x_half = x_all[me, :, mine].astype(F32)
    dy_half = dy_all[me, :, mine].astype(F32)
    gate_home = to_col(meta[2:3, home])
    flat_home = to_col(meta[1:2, home]).astype(jnp.int32)
    pick = (lax.broadcasted_iota(jnp.int32, (TOK, SHARDS * SLOTS), 1) == flat_home).astype(F32).astype(BF16)
    pass_on(o_second)
    d_first = give_back(1, 0)
    arrived(o_first, False)
    arrived(o_second, True)
    tok_out = mm(pick, o_all[...].reshape(SHARDS * SLOTS, HALF))
    dg_mine[...] = to_row(jnp.sum(dy_half * tok_out, axis=1, keepdims=True))
    place = side * SHARDS + me
    dg_copies = [pltpu.make_async_remote_copy(src_ref=dg_mine, dst_ref=dg_all.at[place], send_sem=g_send_sem.at[0], recv_sem=g_recv_sem.at[0], device_id=other, device_id_type=MESH) for other in others]
    for copy in dg_copies:
        copy.start()
    dg_all[place] = dg_mine[...]
    h_copy.wait_recv()
    for copy in sd_spread:
        copy.wait_recv()
    y_half[...] = (x_half + (s_keep[...] + mm(hid_twin[...], sd_twin[...])) + gate_home * tok_out).astype(BF16)
    y_copy = twin(y_half, y_hbm.at[:, mine], 12, 5)
    y_copy.start()
    save_y.start()
    d_second = give_back(1, 1)
    d_third = give_back(1, 2)
    pass_on(d_first)
    pass_on(d_second)
    seven = pltpu.make_async_remote_copy(src_ref=dg_all.at[1:], dst_ref=dg_all.at[1:], send_sem=g_send_sem.at[0], recv_sem=g_recv_sem.at[0], device_id=to_twin, device_id_type=MESH)
    seven.wait_recv()
    dg = jnp.concatenate([dg_all[s, 0:1, :] + dg_all[SHARDS + s, 0:1, :] for s in range(SHARDS)], axis=1)
    one_assign = (lax.broadcasted_iota(jnp.int32, (EXPERTS, total), 0) == meta[0:1, :].astype(jnp.int32)).astype(F32)
    d_logits = (dg * meta[2:3, :] * (one_assign - probs[...])).astype(BF16)
    home_one = (lax.broadcasted_iota(jnp.int32, (EXPERTS, TOK), 0) == meta[0:1, home].astype(jnp.int32)).astype(F32)
    dg_home = dg_all[me, 0:1, :] + dg_all[SHARDS + me, 0:1, :]
    d_logits_home = (dg_home * meta[2:3, home] * (home_one - probs[:, home])).astype(BF16)
    n_copy.wait_recv()
    d_normed = n_keep[...] + n_recv[...] + mm(d_logits_home, wr[:, mine], TN)
    gr_buf[...] = mm(d_logits, n_all[...])
    save_gr.start()
    arrived(d_first, True)
    arrived(d_second, True)
    arrived(d_third, False)
    dn_half[...] = d_normed + mm(pick, d_all[...].reshape(SHARDS * SLOTS, HALF))
    save_dn.start()
    def sent(ref, sem):
        pltpu.make_async_remote_copy(src_ref=ref, dst_ref=ref, send_sem=sem, recv_sem=sem, device_id=to_twin, device_id_type=MESH).wait_send()

    for k, ref in enumerate((ids_all, x_all, dy_all)):
        sent(ref.at[1:], send_sem.at[k])
    for copy in (n_copy, h_copy, sd_copy, y_copy):
        copy.wait_send()
    sent(o_send, y_send_sem.at[3])
    sent(d_send, y_send_sem.at[4])
    sent(sd_twin.at[: 3 * (WIDTH // SHARDS)], q_send_sem.at[0])
    sent(o_all.at[1:], r_send_sem.at[0])
    sent(d_all.at[1:], r_send_sem.at[1])
    seven.wait_send()
    y_copy.wait_recv()
    for save in saves + [save_y, save_gr, save_dn]:
        save.wait()


def layer_call(x_in, y_grad, prim, alt, wr_t, exp_gate, exp_up, exp_down, sh_gate, sh_up, sh_down):
    width = sh_gate.shape[1]
    total = SHARDS * TOK
    rows = OWN * PAD
    shape = jax.ShapeDtypeStruct
    dma = pltpu.SemaphoreType.DMA
    half_f32 = pltpu.VMEM((TOK, HALF), F32)
    slots_f32 = pltpu.VMEM((SLOTS, HALF), F32)
    return pl.pallas_call(
        layer_kernel,
        out_shape=(
            shape((TOK, DIM), BF16), shape((TOK, HALF), F32), shape((EXPERTS, DIM), F32),
            shape((rows, DIM), BF16), shape((rows, DIM), BF16), shape((rows, width), BF16), shape((rows, 2 * width), BF16),
            shape((total, DIM), BF16), shape((SHARDS, TOK, DIM), BF16), shape((total, width), BF16), shape((total, 2 * width), BF16),
        ),
        in_specs=[ANY] * 11,
        out_specs=(ANY,) * 11,
        scratch_shapes=[
            pltpu.VMEM((SHARDS, TOK, DIM), BF16), pltpu.VMEM((SHARDS, TOK, DIM), BF16), pltpu.VMEM((SHARDS, 8, TOK), jnp.int32), pltpu.VMEM((EXPERTS, DIM), BF16),
            pltpu.VMEM((OWN, DIM, width), BF16), pltpu.VMEM((OWN, DIM, width), BF16), pltpu.VMEM((OWN, width, DIM), BF16),
            pltpu.VMEM((DIM, width), BF16), pltpu.VMEM((DIM, width), BF16), pltpu.VMEM((width, DIM), BF16),
            pltpu.VMEM((total, DIM), BF16), pltpu.VMEM((rows, DIM), BF16), pltpu.VMEM((rows, DIM), BF16), pltpu.VMEM((rows, total), BF16),
            pltpu.VMEM((rows, width), F32), pltpu.VMEM((rows, width), F32), pltpu.VMEM((rows, width), BF16), pltpu.VMEM((rows, 2 * width), BF16),
            pltpu.VMEM((total, width), BF16), pltpu.VMEM((total, 2 * width), BF16),
            pltpu.VMEM((EXPERTS, total), F32), pltpu.VMEM((8, total), F32),
            pltpu.VMEM((TOK, width), BF16), pltpu.VMEM((TOK, width), BF16), pltpu.VMEM((width, HALF), BF16), half_f32, half_f32, half_f32, half_f32,
            slots_f32, slots_f32, slots_f32, slots_f32, slots_f32, slots_f32,
            pltpu.VMEM((SHARDS, SLOTS, HALF), BF16), pltpu.VMEM((SHARDS, SLOTS, HALF), BF16),
            pltpu.VMEM((8, TOK), F32), pltpu.VMEM((2 * SHARDS, 8, TOK), F32), pltpu.VMEM((TOK, HALF), BF16), half_f32, pltpu.VMEM((EXPERTS, DIM), F32),
            dma((8,)), dma((3,)), dma((11,)), dma((3,)), dma((3, 5)), dma((2,)), dma((2, 3, 3)), dma((6,)), dma((13,)), dma((1,)), dma((1,)), dma((1,)), dma((3,)),
        ],
        compiler_params=pltpu.CompilerParams(collective_id=0, has_side_effects=True, vmem_limit_bytes=60 << 20),
        name="moe_layer",
    )(x_in, y_grad, prim, alt, wr_t, exp_gate, exp_up, exp_down, sh_gate, sh_up, sh_down)


def grads_kernel(xs_hbm, us_hbm, h_hbm, dab_hbm, n_hbm, dy_hbm, sh_hbm, sdab_hbm, gr_hbm, y_hbm, g_gate_hbm, g_up_hbm, g_down_hbm, gs_gate_hbm, gs_up_hbm, gs_down_hbm, g_router_hbm, y_out_hbm,
                 xs, us, hid, dab, n_all, dy_all, hid_s, dab_s, g_router, y_out, g_gate, g_up, g_down, gs_gate, gs_up, gs_down, in_sem, out_sem, sh_sem):
    loads = [pltpu.make_async_copy(src, dst, in_sem.at[k]) for k, (src, dst) in enumerate((
        (h_hbm, hid), (us_hbm, us), (xs_hbm, xs), (dab_hbm, dab), (n_hbm, n_all), (sdab_hbm, dab_s), (sh_hbm, hid_s), (dy_hbm, dy_all), (gr_hbm, g_router), (y_hbm, y_out)))]
    for load in loads:
        load.start()

    def write(src, dst, sem):
        copy = pltpu.make_async_copy(src, dst, sem)
        copy.start()
        return copy

    for load in loads[:2]:
        load.wait()
    for e in range(OWN):
        rows = slice(e * PAD, (e + 1) * PAD)
        g_down[e] = mm(hid[rows, :], us[rows, :], TN)
        write(g_down.at[e], g_down_hbm.at[e], out_sem.at[0])
        if e == 0:
            for load in loads[2:4]:
                load.wait()
        both = mm(xs[rows, :], dab[rows, :], TN)
        g_gate[e] = both[:, :WIDTH]
        g_up[e] = both[:, WIDTH:]
        write(g_gate.at[e], g_gate_hbm.at[e], out_sem.at[1])
        write(g_up.at[e], g_up_hbm.at[e], out_sem.at[2])
    for load in loads[4:]:
        load.wait()
    both = mm(n_all[...], dab_s[...], TN)
    gs_gate[...] = both[:, :WIDTH]
    gs_up[...] = both[:, WIDTH:]
    writes = [write(gs_gate, gs_gate_hbm, sh_sem.at[0]), write(gs_up, gs_up_hbm, sh_sem.at[1])]
    gs_down[...] = mm(hid_s[...], dy_all[...], TN)
    writes += [write(gs_down, gs_down_hbm, sh_sem.at[2]), write(g_router, g_router_hbm, sh_sem.at[3]), write(y_out, y_out_hbm, sh_sem.at[4])]
    for copy in writes:
        copy.wait()
    for k, (src, dst) in enumerate(((g_down, g_down_hbm), (g_gate, g_gate_hbm), (g_up, g_up_hbm))):
        pltpu.make_async_copy(src, dst, out_sem.at[k]).wait()


def grads_call(*saved):
    shape = jax.ShapeDtypeStruct
    outs = ((OWN, DIM, WIDTH), (OWN, DIM, WIDTH), (OWN, WIDTH, DIM), (DIM, WIDTH), (DIM, WIDTH), (WIDTH, DIM), (EXPERTS, DIM))
    return pl.pallas_call(
        grads_kernel,
        out_shape=tuple(shape(dims, F32) for dims in outs) + (shape((TOK, DIM), BF16),),
        in_specs=[ANY] * 10,
        out_specs=(ANY,) * 8,
        scratch_shapes=[pltpu.VMEM(a.shape, a.dtype) for a in saved] + [pltpu.VMEM(dims, F32) for dims in outs[:-1]] + [pltpu.SemaphoreType.DMA((10,)), pltpu.SemaphoreType.DMA((3,)), pltpu.SemaphoreType.DMA((5,))],
        compiler_params=pltpu.CompilerParams(vmem_limit_bytes=63 << 20),
        cost_estimate=pl.CostEstimate(flops=8 << 30, bytes_accessed=32 << 20, transcendentals=0),
        name="weight_grads",
    )(*saved)


def finish_kernel(x_ref, dy_ref, dn_mine, dn_recv, dx_out):
    side = lax.axis_index("etp")
    theirs = pl.ds(pl.multiple_of((1 - side) * HALF, HALF), HALF)
    mine = pl.ds(pl.multiple_of(side * HALF, HALF), HALF)
    x_wide = x_ref[...].astype(F32)
    inv_rms = inv_rms_of(x_wide)
    halves = ((mine, dn_mine), (theirs, dn_recv))
    norm_proj = sum(jnp.sum(dn[...] * x_ref[:, cols].astype(F32), axis=1, keepdims=True) for cols, dn in halves) / DIM
    for cols, dn in halves:
        dx_out[:, cols] = (dy_ref[:, cols].astype(F32) + inv_rms * dn[...] - x_ref[:, cols].astype(F32) * inv_rms**3 * norm_proj).astype(BF16)


def finish_call(*args):
    return pl.pallas_call(
        finish_kernel,
        out_shape=jax.ShapeDtypeStruct((TOK, DIM), BF16),
        in_specs=[VMEM] * 4,
        out_specs=VMEM,
        compiler_params=pltpu.CompilerParams(vmem_limit_bytes=8 << 20),
        name="finish_tokens",
    )(*args)


def solution(mesh):
    tok_spec = P(("dp", "ep"), None)
    id_spec = P(("dp", "ep"))
    in_specs = (tok_spec, tok_spec, id_spec, id_spec, P(None, None), P("ep", None, "etp"), P("ep", None, "etp"), P("ep", "etp", None), P(None, "etp"), P(None, "etp"), P("etp", None))
    out_specs = (tok_spec, tok_spec, P(("dp", "ep"), None, "etp"), P(("dp", "ep"), None, "etp"), P(("dp", "ep"), "etp", None), P("dp", "etp"), P("dp", "etp"), P(("dp", "etp"), None), P("dp", None))

    def local_step(x_in, y_grad, prim_exp, alt_exp, w_router, exp_gate, exp_up, exp_down, sh_gate, sh_up, sh_down):
        y_full, dn_half, gr, xs, us, hid, dab, n_all, dy_all, hid_s, dab_s = layer_call(x_in, y_grad, prim_exp.reshape(1, TOK), alt_exp.reshape(1, TOK), w_router.T, exp_gate, exp_up, exp_down, sh_gate, sh_up, sh_down)
        dn_other = lax.ppermute(dn_half, "etp", [(0, 1), (1, 0)])
        g_gate, g_up, g_down, gs_gate, gs_up, gs_down, g_router, y_out = grads_call(xs, us, hid, dab, n_all, dy_all.reshape(SHARDS * TOK, DIM), hid_s, dab_s, gr, y_full)
        x_grad = finish_call(x_in, y_grad, dn_half, dn_other)
        return (y_out, x_grad, g_gate, g_up, g_down, gs_gate, gs_up, gs_down, g_router.T)

    return jax.shard_map(local_step, mesh=mesh, in_specs=in_specs, out_specs=out_specs, check_vma=False)
```

```python
import functools

import jax
import jax.numpy as jnp
from jax import lax
from jax.experimental import pallas as pl
from jax.experimental.pallas import tpu as pltpu
from jax.sharding import PartitionSpec as P

EPS = 1e-5
F32 = jnp.float32
BF16 = jnp.bfloat16
MESH = pl.DeviceIdType.MESH
ANY = pl.BlockSpec(memory_space=pl.ANY)
VMEM = pl.BlockSpec(memory_space=pltpu.VMEM)
NN = (((1,), (0,)), ((), ()))
NT = (((1,), (1,)), ((), ()))
TN = (((0,), (0,)), ((), ()))

SHARDS = 4
TOK = 128
DIM = 1024
HALF = 512
EXPERTS = 32
OWN = 8
WIDTH = 256
CAP = 20
PAD = 32
SLOTS = OWN * CAP


def mm(a, b, dims=NN):
    return lax.dot_general(a, b, dims, preferred_element_type=F32)


def inv_rms_of(x_wide):
    return lax.rsqrt(jnp.mean(x_wide * x_wide, axis=1, keepdims=True) + EPS)


def glu_grads(d_hidden, act_gate, act_up):
    sig_gate = jax.nn.sigmoid(act_gate)
    d_gate = (d_hidden * act_up * sig_gate * (1.0 + act_gate * (1.0 - sig_gate))).astype(BF16)
    d_up = (d_hidden * act_gate * sig_gate).astype(BF16)
    return d_gate, d_up


def to_row(col):
    return jnp.transpose(jnp.broadcast_to(col, (TOK, TOK)))[:8]


def to_col(row):
    return jnp.transpose(jnp.broadcast_to(row, (TOK, TOK)))[:, :1]


def barrier(peers):
    sem = pltpu.get_barrier_semaphore()
    for peer in peers:
        pl.semaphore_signal(sem, inc=1, device_id=peer, device_id_type=MESH)
    pl.semaphore_wait(sem, len(peers))


def layer_kernel(x_hbm, dy_hbm, prim_hbm, alt_hbm, wr_hbm, wg_hbm, wu_hbm, wd_hbm, sg_hbm, su_hbm, sd_hbm,
                 y_out, dn_half, gr_out, xs, us, hid, dab, n_all, dy_all, hid_s, dab_s,
                 x_all, ids_all, wr, wg, wu, wd, sg, su, sd, pick_own, acts, acts_up,
                 probs, meta, hid_own, hid_twin, sd_twin, s_keep, n_send, n_recv, n_keep, o_send, o_recv, o_keep, d_send, d_recv, d_keep,
                 o_all, d_all, dg_mine, dg_all,
                 in_sem, w_sem, send_sem, recv_sem, r_send_sem, r_recv_sem, y_send_sem, y_recv_sem, g_send_sem, g_recv_sem, q_send_sem, q_recv_sem):
    me = lax.axis_index("ep")
    side = lax.axis_index("etp")
    total = SHARDS * TOK
    mate = jnp.bitwise_xor(me, 1)
    across = jnp.bitwise_xor(me, 2)
    to_mate, to_across, to_twin = {"ep": mate}, {"ep": across}, {"etp": 1 - side}
    others = [{"etp": jnp.bitwise_xor(side, k // SHARDS), "ep": jnp.bitwise_xor(me, k % SHARDS)} for k in range(1, 2 * SHARDS)]
    theirs = pl.ds(pl.multiple_of((1 - side) * HALF, HALF), HALF)
    mine = pl.ds(pl.multiple_of(side * HALF, HALF), HALF)
    home = pl.ds(pl.multiple_of(me * TOK, TOK), TOK)

    loads = [pltpu.make_async_copy(src, dst, in_sem.at[k]) for k, (src, dst) in enumerate((
        (x_hbm, x_all.at[me]), (prim_hbm, ids_all.at[me, 0:1]), (alt_hbm, ids_all.at[me, 1:2]), (dy_hbm, dy_all.at[me]),
        (sg_hbm, sg), (su_hbm, su), (sd_hbm, sd), (wr_hbm, wr)))]
    for load in loads:
        load.start()
    w_loads = [pltpu.make_async_copy(src, dst, w_sem.at[k]) for k, (src, dst) in enumerate(((wg_hbm, wg), (wu_hbm, wu), (wd_hbm, wd)))]
    barrier(others)

    def remote(view, lane, k, target):
        return pltpu.make_async_remote_copy(src_ref=view, dst_ref=view, send_sem=send_sem.at[(k + 1) // 2], recv_sem=recv_sem.at[lane, k], device_id=target, device_id_type=MESH)

    def twin(src, dst, k, group):
        return pltpu.make_async_remote_copy(src_ref=src, dst_ref=dst, send_sem=y_send_sem.at[group], recv_sem=y_recv_sem.at[k], device_id=to_twin, device_id_type=MESH)

    def pieces(shard):
        rows = TOK // 2
        return [ids_all.at[shard], x_all.at[shard, :rows], x_all.at[shard, rows:], dy_all.at[shard, :rows], dy_all.at[shard, rows:]]

    out_across = [remote(view, 0, k, to_across) for k, view in enumerate(pieces(me))]
    out_mate = [remote(view, 1, k, to_mate) for k, view in enumerate(pieces(me))]
    forwards = [remote(view, 2, k, to_mate) for k, view in enumerate(pieces(across))]
    def quarter(shard):
        return pl.ds(pl.multiple_of(shard * (WIDTH // SHARDS), WIDTH // SHARDS), WIDTH // SHARDS)

    sd_copy = twin(sd_hbm.at[quarter(me), theirs], sd_twin.at[quarter(me)], 2, 2)
    sd_copy.start()
    for load in loads[:3]:
        load.wait()
    for k in range(3):
        out_across[k].start()
        out_mate[k].start()
    loads[3].wait()
    for k in range(3, 5):
        out_across[k].start()
        out_mate[k].start()
    for load in w_loads:
        load.start()

    x_wide = x_all[me].astype(F32)
    normed = (x_wide * inv_rms_of(x_wide)).astype(BF16)
    for load in loads[4:7]:
        load.wait()
    act_gate = mm(normed, sg[...])
    act_up = mm(normed, su[...])
    hidden = (jax.nn.silu(act_gate) * act_up).astype(BF16)
    d_gate, d_up = glu_grads(mm(dy_all[me], sd[...], NT), act_gate, act_up)
    n_send[...] = mm(d_gate, sg[theirs, :], NT) + mm(d_up, su[theirs, :], NT)
    n_copy = twin(n_send, n_recv, 0, 0)
    n_copy.start()
    hid_own[...] = hidden
    h_copy = twin(hid_own, hid_twin, 1, 1)
    h_copy.start()
    n_keep[...] = mm(d_gate, sg[mine, :], NT) + mm(d_up, su[mine, :], NT)
    s_keep[...] = mm(hidden, sd[:, mine])

    def norm(shard):
        rows = x_all[shard].astype(F32)
        n_all[pl.ds(pl.multiple_of(shard * TOK, TOK), TOK), :] = (rows * inv_rms_of(rows)).astype(BF16)

    n_all[home, :] = normed
    out_across[0].wait_recv()
    forwards[0].start()
    for copy in (out_mate[0], forwards[0]):
        copy.wait_recv()
    prim = jnp.concatenate([ids_all[s, 0:1, :] for s in range(SHARDS)], axis=1)
    alt = jnp.concatenate([ids_all[s, 1:2, :] for s in range(SHARDS)], axis=1)
    expert = lax.broadcasted_iota(jnp.int32, (EXPERTS, total), 0)
    before = (lax.broadcasted_iota(jnp.int32, (total, total), 0) < lax.broadcasted_iota(jnp.int32, (total, total), 1)).astype(F32).astype(BF16)
    one_prim = (expert == prim).astype(F32)
    rank_prim = jnp.sum(one_prim * mm(one_prim.astype(BF16), before), axis=0, keepdims=True)
    keep_prim = rank_prim < CAP
    kept = jnp.minimum(jnp.sum(one_prim, axis=1, keepdims=True), float(CAP))
    one_alt = jnp.where(keep_prim, 0.0, (expert == alt).astype(F32))
    slot_alt = jnp.sum(one_alt * (mm(one_alt.astype(BF16), before) + kept), axis=0, keepdims=True)
    keep_alt = jnp.logical_and(jnp.logical_not(keep_prim), slot_alt < CAP)
    assign = jnp.where(keep_prim, prim, jnp.where(keep_alt, alt, -1))
    slot = jnp.where(keep_prim, rank_prim, slot_alt).astype(jnp.int32)
    meta[0:1] = assign.astype(F32)
    meta[1:2] = jnp.where(assign >= 0, assign * CAP + slot, -1).astype(F32)
    local = assign - me * OWN
    owned = jnp.logical_and(local >= 0, local < OWN)
    target = jnp.where(owned, local * PAD + slot, -1)
    pick_own[...] = (lax.broadcasted_iota(jnp.int32, (OWN * PAD, total), 0) == target).astype(F32).astype(BF16)

    sd_copy.wait_recv()
    view = sd_twin.at[quarter(me)]
    sd_spread = [pltpu.make_async_remote_copy(src_ref=view, dst_ref=view, send_sem=q_send_sem.at[0], recv_sem=q_recv_sem.at[k - 1], device_id={"ep": jnp.bitwise_xor(me, k)}, device_id_type=MESH) for k in range(1, SHARDS)]
    for copy in sd_spread:
        copy.start()
    for k in range(1, 3):
        out_mate[k].wait_recv()
    norm(mate)
    for k in range(1, 3):
        out_across[k].wait_recv()
        forwards[k].start()
    norm(across)
    for k in range(1, 3):
        forwards[k].wait_recv()
    norm(jnp.bitwise_xor(me, 3))
    xs[...] = mm(pick_own[...], n_all[...]).astype(BF16)

    O_PIECES = {0: (0, 16), 1: (16, 40), 3: (40, 80), 5: (80, 120), 7: (120, 160)}
    o_copies, d_copies = [], []
    for e in range(OWN):
        if e == 0:
            for load in w_loads:
                load.wait()
        rows = slice(e * PAD, (e + 1) * PAD)
        act_gate = mm(xs[rows, :], wg[e])
        act_up = mm(xs[rows, :], wu[e])
        hidden = (jax.nn.silu(act_gate) * act_up).astype(BF16)
        acts[rows, :] = act_gate
        acts_up[rows, :] = act_up
        hid[rows, :] = hidden
        part = slice(e * CAP, (e + 1) * CAP)
        o_send[part, :] = mm(hidden, wd[e, :, theirs])[:CAP]
        o_keep[part, :] = mm(hidden, wd[e, :, mine])[:CAP]
        if e in O_PIECES:
            chunk = slice(*O_PIECES[e])
            o_copies.append(twin(o_send.at[chunk], o_recv.at[chunk], 13 if e == 0 else 3 + e // 2, 3))
            o_copies[-1].start()
        if e == 5:
            out_across[3].wait_recv()
            forwards[3].start()
    D_PIECES = {1: (0, 40), 3: (40, 80), 5: (80, 120), 6: (120, 136), 7: (136, 160)}
    CHUNKS = (((0, 80), (80, 160)), ((0, 80), (80, 128), (128, 160)))
    READY = ((3, 5), (2, 4, 5))
    DIRECT = ((False, False), (False, False, True))

    def give_back(lane, chunk):
        buf, keep, recv, copies = ((o_all, o_keep, o_recv, o_copies), (d_all, d_keep, d_recv, d_copies))[lane]
        for copy in copies[READY[lane][chunk - 1] if chunk else 0 : READY[lane][chunk]]:
            copy.wait_recv()
        rows = slice(*CHUNKS[lane][chunk])
        buf[me, rows] = (keep[rows, :] + recv[rows, :]).astype(BF16)

        def send(owner, k, j):
            view = buf.at[owner, rows]
            return pltpu.make_async_remote_copy(src_ref=view, dst_ref=view, send_sem=r_send_sem.at[lane], recv_sem=r_recv_sem.at[lane, chunk, j], device_id={"ep": jnp.bitwise_xor(me, k)}, device_id_type=MESH)

        group = [send(me, 2, 0), send(me, 1, 1), send(me, 3, 2) if DIRECT[lane][chunk] else send(across, 1, 2)]
        for copy in group if DIRECT[lane][chunk] else group[:2]:
            copy.start()
        return group

    def pass_on(group):
        group[0].wait_recv()
        group[2].start()

    def arrived(group, forwarded):
        for copy in group[1:] if forwarded else group:
            copy.wait_recv()

    @pl.when(me % 2 == 1)
    def forward_early():
        out_across[4].wait_recv()
        forwards[4].start()

    loads[7].wait()
    logits = mm(n_all[...], wr[...], NT)
    top = jnp.max(logits, axis=1, keepdims=True)
    expo = jnp.exp(logits - top)
    share = expo / jnp.sum(expo, axis=1, keepdims=True)
    wide = jnp.concatenate([share, jnp.zeros((total, TOK - EXPERTS), F32)], axis=1)
    probs_t = jnp.concatenate([jnp.transpose(wide[s * TOK : (s + 1) * TOK])[:EXPERTS] for s in range(SHARDS)], axis=1)
    probs[...] = probs_t
    one_assign = lax.broadcasted_iota(jnp.int32, (EXPERTS, total), 0) == meta[0:1, :].astype(jnp.int32)
    gate = jnp.sum(jnp.where(one_assign, probs_t, 0.0), axis=0, keepdims=True)
    meta[2:3] = gate
    gate_slot = jnp.sum(pick_own[...].astype(F32) * gate, axis=1, keepdims=True)
    @pl.when(me % 2 == 0)
    def forward_late():
        out_across[4].wait_recv()
        forwards[4].start()

    for k in range(3, 5):
        out_mate[k].wait_recv()
        forwards[k].wait_recv()
    us[...] = (gate_slot * mm(pick_own[...], dy_all[...].reshape(total, DIM))).astype(BF16)

    for e in range(OWN):
        rows = slice(e * PAD, (e + 1) * PAD)
        d_gate, d_up = glu_grads(mm(us[rows, :], wd[e], NT), acts[rows, :], acts_up[rows, :])
        dab[rows, :WIDTH] = d_gate
        dab[rows, WIDTH:] = d_up
        part = slice(e * CAP, (e + 1) * CAP)
        d_send[part, :] = (mm(d_gate, wg[e, theirs, :], NT) + mm(d_up, wu[e, theirs, :], NT))[:CAP]
        d_keep[part, :] = (mm(d_gate, wg[e, mine, :], NT) + mm(d_up, wu[e, mine, :], NT))[:CAP]
        if e in D_PIECES:
            chunk = slice(*D_PIECES[e])
            d_copies.append(twin(d_send.at[chunk], d_recv.at[chunk], 7 + len(d_copies), 4))
            d_copies[-1].start()
        if e == 1:
            o_first = give_back(0, 0)
        if e == 5:
            o_second = give_back(0, 1)


    pass_on(o_first)
    act_gate = mm(n_all[...], sg[...])
    act_up = mm(n_all[...], su[...])
    hid_s[...] = (jax.nn.silu(act_gate) * act_up).astype(BF16)
    d_gate, d_up = glu_grads(mm(dy_all[...].reshape(total, DIM), sd[...], NT), act_gate, act_up)
    dab_s[:, :WIDTH] = d_gate
    dab_s[:, WIDTH:] = d_up

    x_half = x_all[me, :, mine].astype(F32)
    dy_half = dy_all[me, :, mine].astype(F32)
    gate_home = to_col(meta[2:3, home])
    flat_home = to_col(meta[1:2, home]).astype(jnp.int32)
    pick = (lax.broadcasted_iota(jnp.int32, (TOK, SHARDS * SLOTS), 1) == flat_home).astype(F32).astype(BF16)
    d_first = give_back(1, 0)
    pass_on(o_second)
    arrived(o_first, True)
    arrived(o_second, True)
    tok_out = mm(pick, o_all[...].reshape(SHARDS * SLOTS, HALF))
    dg_mine[...] = to_row(jnp.sum(dy_half * tok_out, axis=1, keepdims=True))
    place = side * SHARDS + me
    dg_copies = [pltpu.make_async_remote_copy(src_ref=dg_mine, dst_ref=dg_all.at[place], send_sem=g_send_sem.at[0], recv_sem=g_recv_sem.at[0], device_id=other, device_id_type=MESH) for other in others]
    for copy in dg_copies:
        copy.start()
    dg_all[place] = dg_mine[...]
    h_copy.wait_recv()
    for copy in sd_spread:
        copy.wait_recv()
    y_out[:, mine] = (x_half + (s_keep[...] + mm(hid_twin[...], sd_twin[...])) + gate_home * tok_out).astype(BF16)
    y_copy = twin(y_out.at[:, mine], y_out.at[:, mine], 12, 5)
    y_copy.start()
    d_second = give_back(1, 1)
    d_third = give_back(1, 2)
    pass_on(d_first)
    pass_on(d_second)
    seven = pltpu.make_async_remote_copy(src_ref=dg_all.at[1:], dst_ref=dg_all.at[1:], send_sem=g_send_sem.at[0], recv_sem=g_recv_sem.at[0], device_id=to_twin, device_id_type=MESH)
    seven.wait_recv()
    dg = jnp.concatenate([dg_all[s, 0:1, :] + dg_all[SHARDS + s, 0:1, :] for s in range(SHARDS)], axis=1)
    one_assign = (lax.broadcasted_iota(jnp.int32, (EXPERTS, total), 0) == meta[0:1, :].astype(jnp.int32)).astype(F32)
    d_logits = (dg * meta[2:3, :] * (one_assign - probs[...])).astype(BF16)
    home_one = (lax.broadcasted_iota(jnp.int32, (EXPERTS, TOK), 0) == meta[0:1, home].astype(jnp.int32)).astype(F32)
    dg_home = dg_all[me, 0:1, :] + dg_all[SHARDS + me, 0:1, :]
    d_logits_home = (dg_home * meta[2:3, home] * (home_one - probs[:, home])).astype(BF16)
    n_copy.wait_recv()
    d_normed = n_keep[...] + n_recv[...] + mm(d_logits_home, wr[:, mine], TN)
    gr_out[...] = mm(d_logits, n_all[...])
    arrived(d_first, True)
    arrived(d_second, True)
    arrived(d_third, False)
    dn_half[...] = d_normed + mm(pick, d_all[...].reshape(SHARDS * SLOTS, HALF))
    def sent(ref, sem):
        pltpu.make_async_remote_copy(src_ref=ref, dst_ref=ref, send_sem=sem, recv_sem=sem, device_id=to_twin, device_id_type=MESH).wait_send()

    for k, ref in enumerate((ids_all, x_all, dy_all)):
        sent(ref.at[1:], send_sem.at[k])
    for copy in (n_copy, h_copy, sd_copy, y_copy):
        copy.wait_send()
    sent(o_send, y_send_sem.at[3])
    sent(d_send, y_send_sem.at[4])
    sent(sd_twin.at[: 3 * (WIDTH // SHARDS)], q_send_sem.at[0])
    sent(o_all.at[1:], r_send_sem.at[0])
    sent(d_all.at[1:], r_send_sem.at[1])
    seven.wait_send()
    y_copy.wait_recv()


def layer_call(x_in, y_grad, prim, alt, wr_t, exp_gate, exp_up, exp_down, sh_gate, sh_up, sh_down):
    width = sh_gate.shape[1]
    total = SHARDS * TOK
    rows = OWN * PAD
    shape = jax.ShapeDtypeStruct
    dma = pltpu.SemaphoreType.DMA
    half_f32 = pltpu.VMEM((TOK, HALF), F32)
    slots_f32 = pltpu.VMEM((SLOTS, HALF), F32)
    return pl.pallas_call(
        layer_kernel,
        out_shape=(
            shape((TOK, DIM), BF16), shape((TOK, HALF), F32), shape((EXPERTS, DIM), F32),
            shape((rows, DIM), BF16), shape((rows, DIM), BF16), shape((rows, width), BF16), shape((rows, 2 * width), BF16),
            shape((total, DIM), BF16), shape((SHARDS, TOK, DIM), BF16), shape((total, width), BF16), shape((total, 2 * width), BF16),
        ),
        in_specs=[ANY] * 11,
        out_specs=(VMEM,) * 11,
        scratch_shapes=[
            pltpu.VMEM((SHARDS, TOK, DIM), BF16), pltpu.VMEM((SHARDS, 8, TOK), jnp.int32), pltpu.VMEM((EXPERTS, DIM), BF16),
            pltpu.VMEM((OWN, DIM, width), BF16), pltpu.VMEM((OWN, DIM, width), BF16), pltpu.VMEM((OWN, width, DIM), BF16),
            pltpu.VMEM((DIM, width), BF16), pltpu.VMEM((DIM, width), BF16), pltpu.VMEM((width, DIM), BF16),
            pltpu.VMEM((rows, total), BF16),
            pltpu.VMEM((rows, width), F32), pltpu.VMEM((rows, width), F32),
            pltpu.VMEM((EXPERTS, total), F32), pltpu.VMEM((8, total), F32),
            pltpu.VMEM((TOK, width), BF16), pltpu.VMEM((TOK, width), BF16), pltpu.VMEM((width, HALF), BF16), half_f32, half_f32, half_f32, half_f32,
            slots_f32, slots_f32, slots_f32, slots_f32, slots_f32, slots_f32,
            pltpu.VMEM((SHARDS, SLOTS, HALF), BF16), pltpu.VMEM((SHARDS, SLOTS, HALF), BF16),
            pltpu.VMEM((8, TOK), F32), pltpu.VMEM((2 * SHARDS, 8, TOK), F32),
            dma((8,)), dma((3,)), dma((3,)), dma((3, 5)), dma((2,)), dma((2, 3, 3)), dma((6,)), dma((14,)), dma((1,)), dma((1,)), dma((1,)), dma((3,)),
        ],
        compiler_params=pltpu.CompilerParams(collective_id=0, has_side_effects=True, vmem_limit_bytes=40 << 20),
        name="moe_layer",
    )(x_in, y_grad, prim, alt, wr_t, exp_gate, exp_up, exp_down, sh_gate, sh_up, sh_down)


def grads_kernel(xs, us, hid, dab, n_all, dy_all, hid_s, dab_s, g_router, y_out, g_gate_hbm, g_up_hbm, g_down_hbm, gs_gate_hbm, gs_up_hbm, gs_down_hbm, g_router_hbm, y_out_hbm,
                 g_gate, g_up, g_down, gs_gate, gs_up, gs_down, out_sem, sh_sem):
    def write(src, dst, sem):
        copy = pltpu.make_async_copy(src, dst, sem)
        copy.start()
        return copy

    for e in range(OWN):
        rows = slice(e * PAD, (e + 1) * PAD)
        g_down[e] = mm(hid[rows, :], us[rows, :], TN)
        write(g_down.at[e], g_down_hbm.at[e], out_sem.at[0])
        both = mm(xs[rows, :], dab[rows, :], TN)
        g_gate[e] = both[:, :WIDTH]
        g_up[e] = both[:, WIDTH:]
        write(g_gate.at[e], g_gate_hbm.at[e], out_sem.at[1])
        write(g_up.at[e], g_up_hbm.at[e], out_sem.at[2])
    both = mm(n_all[...], dab_s[...], TN)
    gs_gate[...] = both[:, :WIDTH]
    gs_up[...] = both[:, WIDTH:]
    writes = [write(gs_gate, gs_gate_hbm, sh_sem.at[0]), write(gs_up, gs_up_hbm, sh_sem.at[1])]
    gs_down[...] = mm(hid_s[...], dy_all[...], TN)
    writes += [write(gs_down, gs_down_hbm, sh_sem.at[2]), write(g_router, g_router_hbm, sh_sem.at[3]), write(y_out, y_out_hbm, sh_sem.at[4])]
    for copy in writes:
        copy.wait()
    for k, (src, dst) in enumerate(((g_down, g_down_hbm), (g_gate, g_gate_hbm), (g_up, g_up_hbm))):
        pltpu.make_async_copy(src, dst, out_sem.at[k]).wait()


def grads_call(*saved):
    shape = jax.ShapeDtypeStruct
    outs = ((OWN, DIM, WIDTH), (OWN, DIM, WIDTH), (OWN, WIDTH, DIM), (DIM, WIDTH), (DIM, WIDTH), (WIDTH, DIM), (EXPERTS, DIM))
    return pl.pallas_call(
        grads_kernel,
        out_shape=tuple(shape(dims, F32) for dims in outs) + (shape((TOK, DIM), BF16),),
        in_specs=[VMEM] * 10,
        out_specs=(ANY,) * 8,
        scratch_shapes=[pltpu.VMEM(dims, F32) for dims in outs[:-1]] + [pltpu.SemaphoreType.DMA((3,)), pltpu.SemaphoreType.DMA((5,))],
        compiler_params=pltpu.CompilerParams(vmem_limit_bytes=44 << 20),
        cost_estimate=pl.CostEstimate(flops=8 << 30, bytes_accessed=32 << 20, transcendentals=0),
        name="weight_grads",
    )(*saved)


def finish_kernel(x_ref, dy_ref, dn_mine, dn_recv, dx_out):
    side = lax.axis_index("etp")
    theirs = pl.ds(pl.multiple_of((1 - side) * HALF, HALF), HALF)
    mine = pl.ds(pl.multiple_of(side * HALF, HALF), HALF)
    x_wide = x_ref[...].astype(F32)
    inv_rms = inv_rms_of(x_wide)
    halves = ((mine, dn_mine), (theirs, dn_recv))
    norm_proj = sum(jnp.sum(dn[...] * x_ref[:, cols].astype(F32), axis=1, keepdims=True) for cols, dn in halves) / DIM
    for cols, dn in halves:
        dx_out[:, cols] = (dy_ref[:, cols].astype(F32) + inv_rms * dn[...] - x_ref[:, cols].astype(F32) * inv_rms**3 * norm_proj).astype(BF16)


def finish_call(*args):
    return pl.pallas_call(
        finish_kernel,
        out_shape=jax.ShapeDtypeStruct((TOK, DIM), BF16),
        in_specs=[VMEM] * 4,
        out_specs=VMEM,
        compiler_params=pltpu.CompilerParams(vmem_limit_bytes=8 << 20),
        name="finish_tokens",
    )(*args)


def solution(mesh):
    tok_spec = P(("dp", "ep"), None)
    id_spec = P(("dp", "ep"))
    in_specs = (tok_spec, tok_spec, id_spec, id_spec, P(None, None), P("ep", None, "etp"), P("ep", None, "etp"), P("ep", "etp", None), P(None, "etp"), P(None, "etp"), P("etp", None))
    out_specs = (tok_spec, tok_spec, P(("dp", "ep"), None, "etp"), P(("dp", "ep"), None, "etp"), P(("dp", "ep"), "etp", None), P("dp", "etp"), P("dp", "etp"), P(("dp", "etp"), None), P("dp", None))

    def local_step(x_in, y_grad, prim_exp, alt_exp, w_router, exp_gate, exp_up, exp_down, sh_gate, sh_up, sh_down):
        y_full, dn_half, gr, xs, us, hid, dab, n_all, dy_all, hid_s, dab_s = layer_call(*[pltpu.with_memory_space_constraint(a, pltpu.HBM) for a in (x_in, y_grad, prim_exp.reshape(1, TOK), alt_exp.reshape(1, TOK), w_router.T, exp_gate, exp_up, exp_down, sh_gate, sh_up, sh_down)])
        dn_other = lax.ppermute(dn_half, "etp", [(0, 1), (1, 0)])
        g_gate, g_up, g_down, gs_gate, gs_up, gs_down, g_router, y_out = grads_call(xs, us, hid, dab, n_all, dy_all.reshape(SHARDS * TOK, DIM), hid_s, dab_s, gr, y_full)
        x_grad = finish_call(x_in, y_grad, dn_half, dn_other)
        return (y_out, x_grad, g_gate, g_up, g_down, gs_gate, gs_up, gs_down, g_router.T)

    return jax.shard_map(local_step, mesh=mesh, in_specs=in_specs, out_specs=out_specs, check_vma=False)
```

```python
import functools

import jax
import jax.numpy as jnp
from jax import lax
from jax.experimental import pallas as pl
from jax.experimental.pallas import tpu as pltpu
from jax.sharding import PartitionSpec as P

EPS = 1e-5
F32 = jnp.float32
BF16 = jnp.bfloat16
MESH = pl.DeviceIdType.MESH
ANY = pl.BlockSpec(memory_space=pl.ANY)
VMEM = pl.BlockSpec(memory_space=pltpu.VMEM)
NN = (((1,), (0,)), ((), ()))
NT = (((1,), (1,)), ((), ()))
TN = (((0,), (0,)), ((), ()))

SHARDS = 4
TOK = 128
DIM = 1024
HALF = 512
EXPERTS = 32
OWN = 8
WIDTH = 256
CAP = 20
PAD = 32
SLOTS = OWN * CAP


def mm(a, b, dims=NN):
    return lax.dot_general(a, b, dims, preferred_element_type=F32)


def inv_rms_of(x_wide):
    return lax.rsqrt(jnp.mean(x_wide * x_wide, axis=1, keepdims=True) + EPS)


def glu_grads(d_hidden, act_gate, act_up):
    sig_gate = jax.nn.sigmoid(act_gate)
    d_gate = (d_hidden * act_up * sig_gate * (1.0 + act_gate * (1.0 - sig_gate))).astype(BF16)
    d_up = (d_hidden * act_gate * sig_gate).astype(BF16)
    return d_gate, d_up


def to_row(col):
    return jnp.transpose(jnp.broadcast_to(col, (TOK, TOK)))[:8]


def to_col(row):
    return jnp.transpose(jnp.broadcast_to(row, (TOK, TOK)))[:, :1]


def barrier(peers):
    sem = pltpu.get_barrier_semaphore()
    for peer in peers:
        pl.semaphore_signal(sem, inc=1, device_id=peer, device_id_type=MESH)
    pl.semaphore_wait(sem, len(peers))


def layer_kernel(x_hbm, dy_hbm, prim_hbm, alt_hbm, wr_hbm, wg_hbm, wu_hbm, wd_hbm, sg_hbm, su_hbm, sd_hbm,
                 y_out, dn_half, gr_out, xs, us, hid, dab, n_all, dy_all, hid_s, dab_s,
                 x_all, ids_all, wr, wg, wu, wd, sg, su, sd, pick_own, xs_sum, acts, acts_up,
                 probs, meta, hid_own, hid_twin, sd_twin, s_keep, n_send, n_recv, n_keep, o_send, o_recv, o_keep, d_send, d_recv, d_keep,
                 o_all, d_all, dg_mine, dg_all,
                 in_sem, w_sem, send_sem, recv_sem, r_send_sem, r_recv_sem, y_send_sem, y_recv_sem, g_send_sem, g_recv_sem, q_send_sem, q_recv_sem):
    me = lax.axis_index("ep")
    side = lax.axis_index("etp")
    total = SHARDS * TOK
    mate = jnp.bitwise_xor(me, 1)
    across = jnp.bitwise_xor(me, 2)
    to_mate, to_across, to_twin = {"ep": mate}, {"ep": across}, {"etp": 1 - side}
    others = [{"etp": jnp.bitwise_xor(side, k // SHARDS), "ep": jnp.bitwise_xor(me, k % SHARDS)} for k in range(1, 2 * SHARDS)]
    theirs = pl.ds(pl.multiple_of((1 - side) * HALF, HALF), HALF)
    mine = pl.ds(pl.multiple_of(side * HALF, HALF), HALF)
    home = pl.ds(pl.multiple_of(me * TOK, TOK), TOK)

    loads = [pltpu.make_async_copy(src, dst, in_sem.at[k]) for k, (src, dst) in enumerate((
        (x_hbm, x_all.at[me]), (prim_hbm, ids_all.at[me, 0:1]), (alt_hbm, ids_all.at[me, 1:2]), (dy_hbm, dy_all.at[me]),
        (sg_hbm, sg), (su_hbm, su), (sd_hbm, sd), (wr_hbm, wr)))]
    for load in loads:
        load.start()
    w_loads = [pltpu.make_async_copy(src, dst, w_sem.at[k]) for k, (src, dst) in enumerate(((wg_hbm, wg), (wu_hbm, wu), (wd_hbm, wd)))]
    barrier(others)

    def remote(view, lane, k, target):
        return pltpu.make_async_remote_copy(src_ref=view, dst_ref=view, send_sem=send_sem.at[(k + 1) // 2], recv_sem=recv_sem.at[k if lane == 0 else (4 + lane, 6 + lane, 9)[(k + 1) // 2]], device_id=target, device_id_type=MESH)

    def twin(src, dst, k, group):
        return pltpu.make_async_remote_copy(src_ref=src, dst_ref=dst, send_sem=y_send_sem.at[group], recv_sem=y_recv_sem.at[k], device_id=to_twin, device_id_type=MESH)

    def pieces(shard):
        rows = TOK // 2
        return [ids_all.at[shard], x_all.at[shard, :rows], x_all.at[shard, rows:], dy_all.at[shard, :rows], dy_all.at[shard, rows:]]

    out_across = [remote(view, 0, k, to_across) for k, view in enumerate(pieces(me))]
    out_mate = [remote(view, 1, k, to_mate) for k, view in enumerate(pieces(me))]
    forwards = [remote(view, 2, k, to_mate) for k, view in enumerate(pieces(across))]
    def quarter(shard):
        return pl.ds(pl.multiple_of(shard * (WIDTH // SHARDS), WIDTH // SHARDS), WIDTH // SHARDS)

    sd_copy = twin(sd_hbm.at[quarter(me), theirs], sd_twin.at[quarter(me)], 2, 2)
    sd_copy.start()
    for load in loads[:3]:
        load.wait()
    for k in range(3):
        out_across[k].start()
        out_mate[k].start()
    loads[3].wait()
    for k in range(3, 5):
        out_across[k].start()
        out_mate[k].start()
    for load in w_loads:
        load.start()

    def landed(ref, sem):
        pltpu.make_async_remote_copy(src_ref=ref, dst_ref=ref, send_sem=sem, recv_sem=sem, device_id=to_twin, device_id_type=MESH).wait_recv()

    x_wide = x_all[me].astype(F32)
    normed = (x_wide * inv_rms_of(x_wide)).astype(BF16)
    for load in loads[4:7]:
        load.wait()
    act_gate = mm(normed, sg[...])
    act_up = mm(normed, su[...])
    hidden = (jax.nn.silu(act_gate) * act_up).astype(BF16)
    d_gate, d_up = glu_grads(mm(dy_all[me], sd[...], NT), act_gate, act_up)
    n_send[...] = mm(d_gate, sg[theirs, :], NT) + mm(d_up, su[theirs, :], NT)
    n_copy = twin(n_send, n_recv, 0, 0)
    n_copy.start()
    hid_own[...] = hidden
    h_copy = twin(hid_own, hid_twin, 1, 1)
    h_copy.start()
    n_keep[...] = mm(d_gate, sg[mine, :], NT) + mm(d_up, su[mine, :], NT)
    s_keep[...] = mm(hidden, sd[:, mine])

    def norm(shard):
        rows = x_all[shard].astype(F32)
        n_all[pl.ds(pl.multiple_of(shard * TOK, TOK), TOK), :] = (rows * inv_rms_of(rows)).astype(BF16)

    n_all[home, :] = normed
    out_across[0].wait_recv()
    forwards[0].start()
    for copy in (out_mate[0], forwards[0]):
        copy.wait_recv()
    prim = jnp.concatenate([ids_all[s, 0:1, :] for s in range(SHARDS)], axis=1)
    alt = jnp.concatenate([ids_all[s, 1:2, :] for s in range(SHARDS)], axis=1)
    expert = lax.broadcasted_iota(jnp.int32, (EXPERTS, total), 0)
    before = (lax.broadcasted_iota(jnp.int32, (total, total), 0) < lax.broadcasted_iota(jnp.int32, (total, total), 1)).astype(F32).astype(BF16)
    one_prim = (expert == prim).astype(F32)
    rank_prim = jnp.sum(one_prim * mm(one_prim.astype(BF16), before), axis=0, keepdims=True)
    keep_prim = rank_prim < CAP
    kept = jnp.minimum(jnp.sum(one_prim, axis=1, keepdims=True), float(CAP))
    one_alt = jnp.where(keep_prim, 0.0, (expert == alt).astype(F32))
    slot_alt = jnp.sum(one_alt * (mm(one_alt.astype(BF16), before) + kept), axis=0, keepdims=True)
    keep_alt = jnp.logical_and(jnp.logical_not(keep_prim), slot_alt < CAP)
    assign = jnp.where(keep_prim, prim, jnp.where(keep_alt, alt, -1))
    slot = jnp.where(keep_prim, rank_prim, slot_alt).astype(jnp.int32)
    meta[0:1] = assign.astype(F32)
    meta[1:2] = jnp.where(assign >= 0, assign * CAP + slot, -1).astype(F32)
    local = assign - me * OWN
    owned = jnp.logical_and(local >= 0, local < OWN)
    target = jnp.where(owned, local * PAD + slot, -1)
    pick_own[...] = (lax.broadcasted_iota(jnp.int32, (OWN * PAD, total), 0) == target).astype(F32).astype(BF16)

    sd_copy.wait_recv()
    view = sd_twin.at[quarter(me)]
    sd_spread = [pltpu.make_async_remote_copy(src_ref=view, dst_ref=view, send_sem=q_send_sem.at[0], recv_sem=q_recv_sem.at[0], device_id={"ep": jnp.bitwise_xor(me, k)}, device_id_type=MESH) for k in range(1, SHARDS)]
    for copy in sd_spread:
        copy.start()
    def picked(shard):
        rows = pl.ds(pl.multiple_of(shard * TOK, TOK), TOK)
        return mm(pick_own[:, rows], n_all[rows, :])

    landed(x_all.at[0], recv_sem.at[7])
    norm(mate)
    xs_sum[...] = picked(me) + picked(mate)
    for k in range(1, 3):
        out_across[k].wait_recv()
        forwards[k].start()
    norm(across)
    xs_sum[...] += picked(across)
    landed(x_all.at[0], recv_sem.at[8])
    norm(jnp.bitwise_xor(me, 3))
    xs[...] = (xs_sum[...] + picked(jnp.bitwise_xor(me, 3))).astype(BF16)

    O_PIECES = {0: (0, 16, 0), 1: (16, 40, 0), 3: (40, 80, 0), 5: (80, 120, 1), 6: (120, 136, 1), 7: (136, 160, 2)}
    D_PIECES = {1: (0, 40, 0), 3: (40, 80, 0), 5: (80, 120, 1), 6: (120, 136, 1), 7: (136, 160, 2)}
    LANDED = ((0, 80), (80, 136), (136, 160))
    CHUNKS = ((0, 80), (80, 128), (128, 160))
    for e in range(OWN):
        if e == 0:
            for load in w_loads:
                load.wait()
        rows = slice(e * PAD, (e + 1) * PAD)
        act_gate = mm(xs[rows, :], wg[e])
        act_up = mm(xs[rows, :], wu[e])
        hidden = (jax.nn.silu(act_gate) * act_up).astype(BF16)
        acts[rows, :] = act_gate
        acts_up[rows, :] = act_up
        hid[rows, :] = hidden
        part = slice(e * CAP, (e + 1) * CAP)
        o_send[part, :] = mm(hidden, wd[e, :, theirs])[:CAP]
        o_keep[part, :] = mm(hidden, wd[e, :, mine])[:CAP]
        if e in O_PIECES:
            first, last, group = O_PIECES[e]
            twin(o_send.at[first:last], o_recv.at[first:last], 3 + group, 3).start()
        if e == 5:
            out_across[3].wait_recv()
            forwards[3].start()
    def give_back(lane, chunk):
        buf, keep, recv = ((o_all, o_keep, o_recv), (d_all, d_keep, d_recv))[lane]
        landed(recv.at[slice(*LANDED[chunk])], y_recv_sem.at[3 + 3 * lane + chunk])
        rows = slice(*CHUNKS[chunk])
        buf[me, rows] = (keep[rows, :] + recv[rows, :]).astype(BF16)
        direct = chunk == 2

        def send(owner, k, j):
            view = buf.at[owner, rows]
            return pltpu.make_async_remote_copy(src_ref=view, dst_ref=view, send_sem=r_send_sem.at[lane], recv_sem=r_recv_sem.at[lane, chunk, j], device_id={"ep": jnp.bitwise_xor(me, k)}, device_id_type=MESH)

        group = [send(me, 2, 1 if direct else 0), send(me, 1, 1), send(me, 3, 1) if direct else send(across, 1, 1)]
        for copy in group if direct else group[:2]:
            copy.start()
        return group

    def pass_on(group):
        group[0].wait_recv()
        group[2].start()

    def arrived(lane):
        buf = (o_all, d_all)[lane]
        for chunk, (first, last) in enumerate(CHUNKS):
            landed(buf.at[: 3 if chunk == 2 else 2, first:last], r_recv_sem.at[lane, chunk, 1])

    @pl.when(me % 2 == 1)
    def forward_early():
        out_across[4].wait_recv()
        forwards[4].start()

    loads[7].wait()
    logits = mm(n_all[...], wr[...], NT)
    top = jnp.max(logits, axis=1, keepdims=True)
    expo = jnp.exp(logits - top)
    share = expo / jnp.sum(expo, axis=1, keepdims=True)
    wide = jnp.concatenate([share, jnp.zeros((total, TOK - EXPERTS), F32)], axis=1)
    probs_t = jnp.concatenate([jnp.transpose(wide[s * TOK : (s + 1) * TOK])[:EXPERTS] for s in range(SHARDS)], axis=1)
    probs[...] = probs_t
    one_assign = lax.broadcasted_iota(jnp.int32, (EXPERTS, total), 0) == meta[0:1, :].astype(jnp.int32)
    gate = jnp.sum(jnp.where(one_assign, probs_t, 0.0), axis=0, keepdims=True)
    meta[2:3] = gate
    gate_slot = jnp.sum(pick_own[...].astype(F32) * gate, axis=1, keepdims=True)
    @pl.when(me % 2 == 0)
    def forward_late():
        out_across[4].wait_recv()
        forwards[4].start()

    landed(dy_all.at[:2], recv_sem.at[9])
    us[...] = (gate_slot * mm(pick_own[...], dy_all[...].reshape(total, DIM))).astype(BF16)

    for e in range(OWN):
        rows = slice(e * PAD, (e + 1) * PAD)
        d_gate, d_up = glu_grads(mm(us[rows, :], wd[e], NT), acts[rows, :], acts_up[rows, :])
        dab[rows, :WIDTH] = d_gate
        dab[rows, WIDTH:] = d_up
        part = slice(e * CAP, (e + 1) * CAP)
        d_send[part, :] = (mm(d_gate, wg[e, theirs, :], NT) + mm(d_up, wu[e, theirs, :], NT))[:CAP]
        d_keep[part, :] = (mm(d_gate, wg[e, mine, :], NT) + mm(d_up, wu[e, mine, :], NT))[:CAP]
        if e in D_PIECES:
            first, last, group = D_PIECES[e]
            twin(d_send.at[first:last], d_recv.at[first:last], 6 + group, 4).start()
        if e == 1:
            o_first = give_back(0, 0)
        if e == 4:
            o_second = give_back(0, 1)
        if e == 5:
            give_back(0, 2)


    pass_on(o_first)
    act_gate = mm(n_all[...], sg[...])
    act_up = mm(n_all[...], su[...])
    hid_s[...] = (jax.nn.silu(act_gate) * act_up).astype(BF16)
    d_gate, d_up = glu_grads(mm(dy_all[...].reshape(total, DIM), sd[...], NT), act_gate, act_up)
    dab_s[:, :WIDTH] = d_gate
    dab_s[:, WIDTH:] = d_up

    h_copy.wait_recv()
    landed(sd_twin.at[: 3 * (WIDTH // SHARDS)], q_recv_sem.at[0])
    s_keep[...] += mm(hid_twin[...], sd_twin[...])
    x_half = x_all[me, :, mine].astype(F32)
    dy_half = dy_all[me, :, mine].astype(F32)
    gate_home = to_col(meta[2:3, home])
    flat_home = to_col(meta[1:2, home]).astype(jnp.int32)
    pick = (lax.broadcasted_iota(jnp.int32, (TOK, SHARDS * SLOTS), 1) == flat_home).astype(F32).astype(BF16)
    d_first = give_back(1, 0)
    pass_on(o_second)
    arrived(0)
    tok_out = mm(pick, o_all[...].reshape(SHARDS * SLOTS, HALF))
    dg_mine[...] = to_row(jnp.sum(dy_half * tok_out, axis=1, keepdims=True))
    place = side * SHARDS + me
    dg_copies = [pltpu.make_async_remote_copy(src_ref=dg_mine, dst_ref=dg_all.at[place], send_sem=g_send_sem.at[0], recv_sem=g_recv_sem.at[0], device_id=other, device_id_type=MESH) for other in others]
    for copy in dg_copies:
        copy.start()
    dg_all[place] = dg_mine[...]
    y_out[:, mine] = (x_half + s_keep[...] + gate_home * tok_out).astype(BF16)
    y_copy = twin(y_out.at[:, mine], y_out.at[:, mine], 9, 5)
    y_copy.start()
    d_second = give_back(1, 1)
    give_back(1, 2)
    pass_on(d_first)
    pass_on(d_second)
    seven = pltpu.make_async_remote_copy(src_ref=dg_all.at[1:], dst_ref=dg_all.at[1:], send_sem=g_send_sem.at[0], recv_sem=g_recv_sem.at[0], device_id=to_twin, device_id_type=MESH)
    seven.wait_recv()
    dg = jnp.concatenate([dg_all[s, 0:1, :] + dg_all[SHARDS + s, 0:1, :] for s in range(SHARDS)], axis=1)
    one_assign = (lax.broadcasted_iota(jnp.int32, (EXPERTS, total), 0) == meta[0:1, :].astype(jnp.int32)).astype(F32)
    d_logits = (dg * meta[2:3, :] * (one_assign - probs[...])).astype(BF16)
    home_one = (lax.broadcasted_iota(jnp.int32, (EXPERTS, TOK), 0) == meta[0:1, home].astype(jnp.int32)).astype(F32)
    dg_home = dg_all[me, 0:1, :] + dg_all[SHARDS + me, 0:1, :]
    d_logits_home = (dg_home * meta[2:3, home] * (home_one - probs[:, home])).astype(BF16)
    n_copy.wait_recv()
    d_normed = n_keep[...] + n_recv[...] + mm(d_logits_home, wr[:, mine], TN)
    gr_out[...] = mm(d_logits, n_all[...])
    arrived(1)
    dn_half[...] = d_normed + mm(pick, d_all[...].reshape(SHARDS * SLOTS, HALF))
    def sent(ref, sem):
        pltpu.make_async_remote_copy(src_ref=ref, dst_ref=ref, send_sem=sem, recv_sem=sem, device_id=to_twin, device_id_type=MESH).wait_send()

    for k, ref in enumerate((ids_all, x_all, dy_all)):
        sent(ref.at[1:], send_sem.at[k])
    for copy in (n_copy, h_copy, sd_copy, y_copy):
        copy.wait_send()
    sent(o_send, y_send_sem.at[3])
    sent(d_send, y_send_sem.at[4])
    sent(sd_twin.at[: 3 * (WIDTH // SHARDS)], q_send_sem.at[0])
    sent(o_all.at[1:], r_send_sem.at[0])
    sent(d_all.at[1:], r_send_sem.at[1])
    seven.wait_send()
    y_copy.wait_recv()


def layer_call(x_in, y_grad, prim, alt, wr_t, exp_gate, exp_up, exp_down, sh_gate, sh_up, sh_down):
    width = sh_gate.shape[1]
    total = SHARDS * TOK
    rows = OWN * PAD
    shape = jax.ShapeDtypeStruct
    dma = pltpu.SemaphoreType.DMA
    half_f32 = pltpu.VMEM((TOK, HALF), F32)
    slots_f32 = pltpu.VMEM((SLOTS, HALF), F32)
    return pl.pallas_call(
        layer_kernel,
        out_shape=(
            shape((TOK, DIM), BF16), shape((TOK, HALF), F32), shape((EXPERTS, DIM), F32),
            shape((rows, DIM), BF16), shape((rows, DIM), BF16), shape((rows, width), BF16), shape((rows, 2 * width), BF16),
            shape((total, DIM), BF16), shape((SHARDS, TOK, DIM), BF16), shape((total, width), BF16), shape((total, 2 * width), BF16),
        ),
        in_specs=[ANY] * 11,
        out_specs=(VMEM,) * 11,
        scratch_shapes=[
            pltpu.VMEM((SHARDS, TOK, DIM), BF16), pltpu.VMEM((SHARDS, 8, TOK), jnp.int32), pltpu.VMEM((EXPERTS, DIM), BF16),
            pltpu.VMEM((OWN, DIM, width), BF16), pltpu.VMEM((OWN, DIM, width), BF16), pltpu.VMEM((OWN, width, DIM), BF16),
            pltpu.VMEM((DIM, width), BF16), pltpu.VMEM((DIM, width), BF16), pltpu.VMEM((width, DIM), BF16),
            pltpu.VMEM((rows, total), BF16), pltpu.VMEM((rows, DIM), F32),
            pltpu.VMEM((rows, width), F32), pltpu.VMEM((rows, width), F32),
            pltpu.VMEM((EXPERTS, total), F32), pltpu.VMEM((8, total), F32),
            pltpu.VMEM((TOK, width), BF16), pltpu.VMEM((TOK, width), BF16), pltpu.VMEM((width, HALF), BF16), half_f32, half_f32, half_f32, half_f32,
            slots_f32, slots_f32, slots_f32, slots_f32, slots_f32, slots_f32,
            pltpu.VMEM((SHARDS, SLOTS, HALF), BF16), pltpu.VMEM((SHARDS, SLOTS, HALF), BF16),
            pltpu.VMEM((8, TOK), F32), pltpu.VMEM((2 * SHARDS, 8, TOK), F32),
            dma((8,)), dma((3,)), dma((3,)), dma((10,)), dma((2,)), dma((2, 3, 2)), dma((6,)), dma((10,)), dma((1,)), dma((1,)), dma((1,)), dma((1,)),
        ],
        compiler_params=pltpu.CompilerParams(collective_id=0, has_side_effects=True, vmem_limit_bytes=40 << 20),
        name="moe_layer",
    )(x_in, y_grad, prim, alt, wr_t, exp_gate, exp_up, exp_down, sh_gate, sh_up, sh_down)


def grads_kernel(xs, us, hid, dab, n_all, dy_all, hid_s, dab_s, g_router, y_out, g_gate_hbm, g_up_hbm, g_down_hbm, gs_gate_hbm, gs_up_hbm, gs_down_hbm, g_router_hbm, y_out_hbm,
                 g_gate, g_up, g_down, gs_gate, gs_up, gs_down, out_sem, sh_sem):
    def write(src, dst, sem):
        copy = pltpu.make_async_copy(src, dst, sem)
        copy.start()
        return copy

    for e in range(OWN):
        rows = slice(e * PAD, (e + 1) * PAD)
        g_down[e] = mm(hid[rows, :], us[rows, :], TN)
        write(g_down.at[e], g_down_hbm.at[e], out_sem.at[0])
        both = mm(xs[rows, :], dab[rows, :], TN)
        g_gate[e] = both[:, :WIDTH]
        g_up[e] = both[:, WIDTH:]
        write(g_gate.at[e], g_gate_hbm.at[e], out_sem.at[1])
        write(g_up.at[e], g_up_hbm.at[e], out_sem.at[2])
    both = mm(n_all[...], dab_s[...], TN)
    gs_gate[...] = both[:, :WIDTH]
    gs_up[...] = both[:, WIDTH:]
    writes = [write(gs_gate, gs_gate_hbm, sh_sem.at[0]), write(gs_up, gs_up_hbm, sh_sem.at[1])]
    gs_down[...] = mm(hid_s[...], dy_all[...], TN)
    writes += [write(gs_down, gs_down_hbm, sh_sem.at[2]), write(g_router, g_router_hbm, sh_sem.at[3]), write(y_out, y_out_hbm, sh_sem.at[4])]
    for copy in writes:
        copy.wait()
    for k, (src, dst) in enumerate(((g_down, g_down_hbm), (g_gate, g_gate_hbm), (g_up, g_up_hbm))):
        pltpu.make_async_copy(src, dst, out_sem.at[k]).wait()


def grads_call(*saved):
    shape = jax.ShapeDtypeStruct
    outs = ((OWN, DIM, WIDTH), (OWN, DIM, WIDTH), (OWN, WIDTH, DIM), (DIM, WIDTH), (DIM, WIDTH), (WIDTH, DIM), (EXPERTS, DIM))
    return pl.pallas_call(
        grads_kernel,
        out_shape=tuple(shape(dims, F32) for dims in outs) + (shape((TOK, DIM), BF16),),
        in_specs=[VMEM] * 10,
        out_specs=(ANY,) * 8,
        scratch_shapes=[pltpu.VMEM(dims, F32) for dims in outs[:-1]] + [pltpu.SemaphoreType.DMA((3,)), pltpu.SemaphoreType.DMA((5,))],
        compiler_params=pltpu.CompilerParams(vmem_limit_bytes=44 << 20),
        cost_estimate=pl.CostEstimate(flops=8 << 30, bytes_accessed=32 << 20, transcendentals=0),
        name="weight_grads",
    )(*saved)


def finish_kernel(x_ref, dy_ref, dn_mine, dn_recv, dx_out):
    side = lax.axis_index("etp")
    theirs = pl.ds(pl.multiple_of((1 - side) * HALF, HALF), HALF)
    mine = pl.ds(pl.multiple_of(side * HALF, HALF), HALF)
    x_wide = x_ref[...].astype(F32)
    inv_rms = inv_rms_of(x_wide)
    halves = ((mine, dn_mine), (theirs, dn_recv))
    norm_proj = sum(jnp.sum(dn[...] * x_ref[:, cols].astype(F32), axis=1, keepdims=True) for cols, dn in halves) / DIM
    for cols, dn in halves:
        dx_out[:, cols] = (dy_ref[:, cols].astype(F32) + inv_rms * dn[...] - x_ref[:, cols].astype(F32) * inv_rms**3 * norm_proj).astype(BF16)


def finish_call(*args):
    return pl.pallas_call(
        finish_kernel,
        out_shape=jax.ShapeDtypeStruct((TOK, DIM), BF16),
        in_specs=[VMEM] * 4,
        out_specs=VMEM,
        compiler_params=pltpu.CompilerParams(vmem_limit_bytes=8 << 20),
        name="finish_tokens",
    )(*args)


def solution(mesh):
    tok_spec = P(("dp", "ep"), None)
    id_spec = P(("dp", "ep"))
    in_specs = (tok_spec, tok_spec, id_spec, id_spec, P(None, None), P("ep", None, "etp"), P("ep", None, "etp"), P("ep", "etp", None), P(None, "etp"), P(None, "etp"), P("etp", None))
    out_specs = (tok_spec, tok_spec, P(("dp", "ep"), None, "etp"), P(("dp", "ep"), None, "etp"), P(("dp", "ep"), "etp", None), P("dp", "etp"), P("dp", "etp"), P(("dp", "etp"), None), P("dp", None))

    def local_step(x_in, y_grad, prim_exp, alt_exp, w_router, exp_gate, exp_up, exp_down, sh_gate, sh_up, sh_down):
        y_full, dn_half, gr, xs, us, hid, dab, n_all, dy_all, hid_s, dab_s = layer_call(*[pltpu.with_memory_space_constraint(a, pltpu.HBM) for a in (x_in, y_grad, prim_exp.reshape(1, TOK), alt_exp.reshape(1, TOK), w_router.T, exp_gate, exp_up, exp_down, sh_gate, sh_up, sh_down)])
        dn_other = lax.ppermute(dn_half, "etp", [(0, 1), (1, 0)])
        g_gate, g_up, g_down, gs_gate, gs_up, gs_down, g_router, y_out = grads_call(xs, us, hid, dab, n_all, dy_all.reshape(SHARDS * TOK, DIM), hid_s, dab_s, gr, y_full)
        x_grad = finish_call(x_in, y_grad, dn_half, dn_other)
        return (y_out, x_grad, g_gate, g_up, g_down, gs_gate, gs_up, gs_down, g_router.T)

    return jax.shard_map(local_step, mesh=mesh, in_specs=in_specs, out_specs=out_specs, check_vma=False)
```

```python
import functools

import jax
import jax.numpy as jnp
from jax import lax
from jax.experimental import pallas as pl
from jax.experimental.pallas import tpu as pltpu
from jax.sharding import PartitionSpec as P

EPS = 1e-5
F32 = jnp.float32
BF16 = jnp.bfloat16
MESH = pl.DeviceIdType.MESH
ANY = pl.BlockSpec(memory_space=pl.ANY)
VMEM = pl.BlockSpec(memory_space=pltpu.VMEM)
NN = (((1,), (0,)), ((), ()))
NT = (((1,), (1,)), ((), ()))
TN = (((0,), (0,)), ((), ()))

SHARDS = 4
TOK = 128
DIM = 1024
HALF = 512
EXPERTS = 32
OWN = 8
WIDTH = 256
CAP = 20
PAD = 32
SLOTS = OWN * CAP


def mm(a, b, dims=NN):
    return lax.dot_general(a, b, dims, preferred_element_type=F32)


def inv_rms_of(x_wide):
    return lax.rsqrt(jnp.mean(x_wide * x_wide, axis=1, keepdims=True) + EPS)


def glu_grads(d_hidden, act_gate, act_up):
    sig_gate = jax.nn.sigmoid(act_gate)
    d_gate = (d_hidden * act_up * sig_gate * (1.0 + act_gate * (1.0 - sig_gate))).astype(BF16)
    d_up = (d_hidden * act_gate * sig_gate).astype(BF16)
    return d_gate, d_up


def to_row(col):
    return jnp.transpose(jnp.broadcast_to(col, (TOK, TOK)))[:8]


def to_col(row):
    return jnp.transpose(jnp.broadcast_to(row, (TOK, TOK)))[:, :1]


def barrier(peers):
    sem = pltpu.get_barrier_semaphore()
    for peer in peers:
        pl.semaphore_signal(sem, inc=1, device_id=peer, device_id_type=MESH)
    pl.semaphore_wait(sem, len(peers))


def layer_kernel(x_hbm, dy_hbm, prim_hbm, alt_hbm, wr_hbm, wg_hbm, wu_hbm, wd_hbm, sg_hbm, su_hbm, sd_hbm,
                 y_out, dn_half, gr_out, xs, us, hid, dab, n_all, dy_all, hid_s, dab_s,
                 x_all, ids_all, wr, wg, wu, wd, sg, su, sd, pick_own, xs_sum, acts, acts_up,
                 probs, meta, hid_own, hid_twin, sd_twin, s_keep, n_send, n_recv, n_keep, o_send, o_recv, o_keep, d_send, d_recv, d_keep,
                 o_all, d_all, dg_mine, dg_all,
                 in_sem, w_sem, send_sem, recv_sem, r_send_sem, r_recv_sem, y_send_sem, y_recv_sem, g_send_sem, g_recv_sem, q_send_sem, q_recv_sem, step_sem):
    me = lax.axis_index("ep")
    side = lax.axis_index("etp")
    total = SHARDS * TOK
    mate = jnp.bitwise_xor(me, 1)
    across = jnp.bitwise_xor(me, 2)
    to_mate, to_across, to_twin = {"ep": mate}, {"ep": across}, {"etp": 1 - side}
    others = [{"etp": jnp.bitwise_xor(side, k // SHARDS), "ep": jnp.bitwise_xor(me, k % SHARDS)} for k in range(1, 2 * SHARDS)]
    theirs = pl.ds(pl.multiple_of((1 - side) * HALF, HALF), HALF)
    mine = pl.ds(pl.multiple_of(side * HALF, HALF), HALF)
    home = pl.ds(pl.multiple_of(me * TOK, TOK), TOK)

    loads = [pltpu.make_async_copy(src, dst, in_sem.at[k]) for k, (src, dst) in enumerate((
        (x_hbm, x_all.at[me]), (prim_hbm, ids_all.at[me, 0:1]), (alt_hbm, ids_all.at[me, 1:2]), (dy_hbm, dy_all.at[me]),
        (sg_hbm, sg), (su_hbm, su), (sd_hbm, sd), (wr_hbm, wr)))]
    for load in loads:
        load.start()
    w_loads = [pltpu.make_async_copy(src, dst, w_sem.at[k]) for k, (src, dst) in enumerate(((wg_hbm, wg), (wu_hbm, wu), (wd_hbm, wd)))]
    near = (to_mate, to_across, to_twin)
    barrier(near)

    def relay(k):
        for peer in near:
            pl.semaphore_signal(step_sem.at[k], inc=1, device_id=peer, device_id_type=MESH)

    relay(0)

    def remote(view, lane, k, target):
        return pltpu.make_async_remote_copy(src_ref=view, dst_ref=view, send_sem=send_sem.at[(k + 1) // 2], recv_sem=recv_sem.at[k if lane == 0 else (4 + lane, 6 + lane, 9)[(k + 1) // 2]], device_id=target, device_id_type=MESH)

    def twin(src, dst, k, group):
        return pltpu.make_async_remote_copy(src_ref=src, dst_ref=dst, send_sem=y_send_sem.at[group], recv_sem=y_recv_sem.at[k], device_id=to_twin, device_id_type=MESH)

    def pieces(shard):
        rows = TOK // 2
        return [ids_all.at[shard], x_all.at[shard, :rows], x_all.at[shard, rows:], dy_all.at[shard, :rows], dy_all.at[shard, rows:]]

    out_across = [remote(view, 0, k, to_across) for k, view in enumerate(pieces(me))]
    out_mate = [remote(view, 1, k, to_mate) for k, view in enumerate(pieces(me))]
    forwards = [remote(view, 2, k, to_mate) for k, view in enumerate(pieces(across))]
    def quarter(shard):
        return pl.ds(pl.multiple_of(shard * (WIDTH // SHARDS), WIDTH // SHARDS), WIDTH // SHARDS)

    sd_copy = twin(sd_hbm.at[quarter(me), theirs], sd_twin.at[quarter(me)], 2, 2)
    sd_copy.start()
    for load in loads[:3]:
        load.wait()
    for k in range(3):
        out_across[k].start()
        out_mate[k].start()
    loads[3].wait()
    for k in range(3, 5):
        out_across[k].start()
        out_mate[k].start()
    for load in w_loads:
        load.start()

    def landed(ref, sem):
        pltpu.make_async_remote_copy(src_ref=ref, dst_ref=ref, send_sem=sem, recv_sem=sem, device_id=to_twin, device_id_type=MESH).wait_recv()

    x_wide = x_all[me].astype(F32)
    normed = (x_wide * inv_rms_of(x_wide)).astype(BF16)
    for load in loads[4:7]:
        load.wait()
    act_gate = mm(normed, sg[...])
    act_up = mm(normed, su[...])
    hidden = (jax.nn.silu(act_gate) * act_up).astype(BF16)
    d_gate, d_up = glu_grads(mm(dy_all[me], sd[...], NT), act_gate, act_up)
    n_send[...] = mm(d_gate, sg[theirs, :], NT) + mm(d_up, su[theirs, :], NT)
    n_copy = twin(n_send, n_recv, 0, 0)
    n_copy.start()
    hid_own[...] = hidden
    h_copy = twin(hid_own, hid_twin, 1, 1)
    h_copy.start()
    n_keep[...] = mm(d_gate, sg[mine, :], NT) + mm(d_up, su[mine, :], NT)
    s_keep[...] = mm(hidden, sd[:, mine])

    def norm(shard):
        rows = x_all[shard].astype(F32)
        n_all[pl.ds(pl.multiple_of(shard * TOK, TOK), TOK), :] = (rows * inv_rms_of(rows)).astype(BF16)

    n_all[home, :] = normed
    out_across[0].wait_recv()
    forwards[0].start()
    for copy in (out_mate[0], forwards[0]):
        copy.wait_recv()
    prim = jnp.concatenate([ids_all[s, 0:1, :] for s in range(SHARDS)], axis=1)
    alt = jnp.concatenate([ids_all[s, 1:2, :] for s in range(SHARDS)], axis=1)
    expert = lax.broadcasted_iota(jnp.int32, (EXPERTS, total), 0)
    before = (lax.broadcasted_iota(jnp.int32, (total, total), 0) < lax.broadcasted_iota(jnp.int32, (total, total), 1)).astype(F32).astype(BF16)
    one_prim = (expert == prim).astype(F32)
    rank_prim = jnp.sum(one_prim * mm(one_prim.astype(BF16), before), axis=0, keepdims=True)
    keep_prim = rank_prim < CAP
    kept = jnp.minimum(jnp.sum(one_prim, axis=1, keepdims=True), float(CAP))
    one_alt = jnp.where(keep_prim, 0.0, (expert == alt).astype(F32))
    slot_alt = jnp.sum(one_alt * (mm(one_alt.astype(BF16), before) + kept), axis=0, keepdims=True)
    keep_alt = jnp.logical_and(jnp.logical_not(keep_prim), slot_alt < CAP)
    assign = jnp.where(keep_prim, prim, jnp.where(keep_alt, alt, -1))
    slot = jnp.where(keep_prim, rank_prim, slot_alt).astype(jnp.int32)
    meta[0:1] = assign.astype(F32)
    meta[1:2] = jnp.where(assign >= 0, assign * CAP + slot, -1).astype(F32)
    local = assign - me * OWN
    owned = jnp.logical_and(local >= 0, local < OWN)
    target = jnp.where(owned, local * PAD + slot, -1)
    pick_own[...] = (lax.broadcasted_iota(jnp.int32, (OWN * PAD, total), 0) == target).astype(F32).astype(BF16)

    pl.semaphore_wait(step_sem.at[0], 3)
    relay(1)
    sd_copy.wait_recv()
    view = sd_twin.at[quarter(me)]
    sd_spread = [pltpu.make_async_remote_copy(src_ref=view, dst_ref=view, send_sem=q_send_sem.at[0], recv_sem=q_recv_sem.at[0], device_id={"ep": jnp.bitwise_xor(me, k)}, device_id_type=MESH) for k in range(1, SHARDS)]
    for copy in sd_spread:
        copy.start()
    def picked(shard):
        rows = pl.ds(pl.multiple_of(shard * TOK, TOK), TOK)
        return mm(pick_own[:, rows], n_all[rows, :])

    landed(x_all.at[0], recv_sem.at[7])
    norm(mate)
    xs_sum[...] = picked(me) + picked(mate)
    for k in range(1, 3):
        out_across[k].wait_recv()
        forwards[k].start()
    norm(across)
    xs_sum[...] += picked(across)
    landed(x_all.at[0], recv_sem.at[8])
    norm(jnp.bitwise_xor(me, 3))
    xs[...] = (xs_sum[...] + picked(jnp.bitwise_xor(me, 3))).astype(BF16)

    O_PIECES = {0: (0, 16, 0), 1: (16, 40, 0), 3: (40, 80, 0), 5: (80, 120, 1), 6: (120, 136, 1), 7: (136, 160, 2)}
    D_PIECES = {1: (0, 40, 0), 3: (40, 80, 0), 5: (80, 120, 1), 6: (120, 136, 1), 7: (136, 160, 2)}
    LANDED = ((0, 80), (80, 136), (136, 160))
    CHUNKS = ((0, 80), (80, 128), (128, 160))
    for e in range(OWN):
        if e == 0:
            for load in w_loads:
                load.wait()
        rows = slice(e * PAD, (e + 1) * PAD)
        act_gate = mm(xs[rows, :], wg[e])
        act_up = mm(xs[rows, :], wu[e])
        hidden = (jax.nn.silu(act_gate) * act_up).astype(BF16)
        acts[rows, :] = act_gate
        acts_up[rows, :] = act_up
        hid[rows, :] = hidden
        part = slice(e * CAP, (e + 1) * CAP)
        o_send[part, :] = mm(hidden, wd[e, :, theirs])[:CAP]
        o_keep[part, :] = mm(hidden, wd[e, :, mine])[:CAP]
        if e in O_PIECES:
            first, last, group = O_PIECES[e]
            twin(o_send.at[first:last], o_recv.at[first:last], 3 + group, 3).start()
        if e == 5:
            out_across[3].wait_recv()
            forwards[3].start()
    def give_back(lane, chunk):
        buf, keep, recv = ((o_all, o_keep, o_recv), (d_all, d_keep, d_recv))[lane]
        landed(recv.at[slice(*LANDED[chunk])], y_recv_sem.at[3 + 3 * lane + chunk])
        rows = slice(*CHUNKS[chunk])
        buf[me, rows] = (keep[rows, :] + recv[rows, :]).astype(BF16)
        direct = chunk == 2

        def send(owner, k, j):
            view = buf.at[owner, rows]
            return pltpu.make_async_remote_copy(src_ref=view, dst_ref=view, send_sem=r_send_sem.at[lane], recv_sem=r_recv_sem.at[lane, chunk, j], device_id={"ep": jnp.bitwise_xor(me, k)}, device_id_type=MESH)

        group = [send(me, 2, 1 if direct else 0), send(me, 1, 1), send(me, 3, 1) if direct else send(across, 1, 1)]
        for copy in group if direct else group[:2]:
            copy.start()
        return group

    def pass_on(group):
        group[0].wait_recv()
        group[2].start()

    def arrived(lane):
        buf = (o_all, d_all)[lane]
        for chunk, (first, last) in enumerate(CHUNKS):
            landed(buf.at[: 3 if chunk == 2 else 2, first:last], r_recv_sem.at[lane, chunk, 1])

    @pl.when(me % 2 == 1)
    def forward_early():
        out_across[4].wait_recv()
        forwards[4].start()

    loads[7].wait()
    logits = mm(n_all[...], wr[...], NT)
    top = jnp.max(logits, axis=1, keepdims=True)
    expo = jnp.exp(logits - top)
    share = expo / jnp.sum(expo, axis=1, keepdims=True)
    wide = jnp.concatenate([share, jnp.zeros((total, TOK - EXPERTS), F32)], axis=1)
    probs_t = jnp.concatenate([jnp.transpose(wide[s * TOK : (s + 1) * TOK])[:EXPERTS] for s in range(SHARDS)], axis=1)
    probs[...] = probs_t
    one_assign = lax.broadcasted_iota(jnp.int32, (EXPERTS, total), 0) == meta[0:1, :].astype(jnp.int32)
    gate = jnp.sum(jnp.where(one_assign, probs_t, 0.0), axis=0, keepdims=True)
    meta[2:3] = gate
    gate_slot = jnp.sum(pick_own[...].astype(F32) * gate, axis=1, keepdims=True)
    @pl.when(me % 2 == 0)
    def forward_late():
        out_across[4].wait_recv()
        forwards[4].start()

    landed(dy_all.at[:2], recv_sem.at[9])
    us[...] = (gate_slot * mm(pick_own[...], dy_all[...].reshape(total, DIM))).astype(BF16)

    for e in range(OWN):
        rows = slice(e * PAD, (e + 1) * PAD)
        d_gate, d_up = glu_grads(mm(us[rows, :], wd[e], NT), acts[rows, :], acts_up[rows, :])
        dab[rows, :WIDTH] = d_gate
        dab[rows, WIDTH:] = d_up
        part = slice(e * CAP, (e + 1) * CAP)
        d_send[part, :] = (mm(d_gate, wg[e, theirs, :], NT) + mm(d_up, wu[e, theirs, :], NT))[:CAP]
        d_keep[part, :] = (mm(d_gate, wg[e, mine, :], NT) + mm(d_up, wu[e, mine, :], NT))[:CAP]
        if e in D_PIECES:
            first, last, group = D_PIECES[e]
            twin(d_send.at[first:last], d_recv.at[first:last], 6 + group, 4).start()
        if e == 1:
            o_first = give_back(0, 0)
        if e == 4:
            o_second = give_back(0, 1)
        if e == 5:
            give_back(0, 2)


    pass_on(o_first)
    act_gate = mm(n_all[...], sg[...])
    act_up = mm(n_all[...], su[...])
    hid_s[...] = (jax.nn.silu(act_gate) * act_up).astype(BF16)
    d_gate, d_up = glu_grads(mm(dy_all[...].reshape(total, DIM), sd[...], NT), act_gate, act_up)
    dab_s[:, :WIDTH] = d_gate
    dab_s[:, WIDTH:] = d_up

    h_copy.wait_recv()
    landed(sd_twin.at[: 3 * (WIDTH // SHARDS)], q_recv_sem.at[0])
    s_keep[...] += mm(hid_twin[...], sd_twin[...])
    x_half = x_all[me, :, mine].astype(F32)
    dy_half = dy_all[me, :, mine].astype(F32)
    gate_home = to_col(meta[2:3, home])
    flat_home = to_col(meta[1:2, home]).astype(jnp.int32)
    pick = (lax.broadcasted_iota(jnp.int32, (TOK, SHARDS * SLOTS), 1) == flat_home).astype(F32).astype(BF16)
    d_first = give_back(1, 0)
    pass_on(o_second)
    arrived(0)
    tok_out = mm(pick, o_all[...].reshape(SHARDS * SLOTS, HALF))
    dg_mine[...] = to_row(jnp.sum(dy_half * tok_out, axis=1, keepdims=True))
    place = side * SHARDS + me
    pl.semaphore_wait(step_sem.at[1], 3)
    dg_copies = [pltpu.make_async_remote_copy(src_ref=dg_mine, dst_ref=dg_all.at[place], send_sem=g_send_sem.at[0], recv_sem=g_recv_sem.at[0], device_id=other, device_id_type=MESH) for other in others]
    for copy in dg_copies:
        copy.start()
    dg_all[place] = dg_mine[...]
    y_out[:, mine] = (x_half + s_keep[...] + gate_home * tok_out).astype(BF16)
    y_copy = twin(y_out.at[:, mine], y_out.at[:, mine], 9, 5)
    y_copy.start()
    d_second = give_back(1, 1)
    give_back(1, 2)
    pass_on(d_first)
    pass_on(d_second)
    seven = pltpu.make_async_remote_copy(src_ref=dg_all.at[1:], dst_ref=dg_all.at[1:], send_sem=g_send_sem.at[0], recv_sem=g_recv_sem.at[0], device_id=to_twin, device_id_type=MESH)
    seven.wait_recv()
    dg = jnp.concatenate([dg_all[s, 0:1, :] + dg_all[SHARDS + s, 0:1, :] for s in range(SHARDS)], axis=1)
    one_assign = (lax.broadcasted_iota(jnp.int32, (EXPERTS, total), 0) == meta[0:1, :].astype(jnp.int32)).astype(F32)
    d_logits = (dg * meta[2:3, :] * (one_assign - probs[...])).astype(BF16)
    home_one = (lax.broadcasted_iota(jnp.int32, (EXPERTS, TOK), 0) == meta[0:1, home].astype(jnp.int32)).astype(F32)
    dg_home = dg_all[me, 0:1, :] + dg_all[SHARDS + me, 0:1, :]
    d_logits_home = (dg_home * meta[2:3, home] * (home_one - probs[:, home])).astype(BF16)
    n_copy.wait_recv()
    d_normed = n_keep[...] + n_recv[...] + mm(d_logits_home, wr[:, mine], TN)
    gr_out[...] = mm(d_logits, n_all[...])
    arrived(1)
    dn_half[...] = d_normed + mm(pick, d_all[...].reshape(SHARDS * SLOTS, HALF))
    def sent(ref, sem):
        pltpu.make_async_remote_copy(src_ref=ref, dst_ref=ref, send_sem=sem, recv_sem=sem, device_id=to_twin, device_id_type=MESH).wait_send()

    for k, ref in enumerate((ids_all, x_all, dy_all)):
        sent(ref.at[1:], send_sem.at[k])
    for copy in (n_copy, h_copy, sd_copy, y_copy):
        copy.wait_send()
    sent(o_send, y_send_sem.at[3])
    sent(d_send, y_send_sem.at[4])
    sent(sd_twin.at[: 3 * (WIDTH // SHARDS)], q_send_sem.at[0])
    sent(o_all.at[1:], r_send_sem.at[0])
    sent(d_all.at[1:], r_send_sem.at[1])
    seven.wait_send()
    y_copy.wait_recv()


def layer_call(x_in, y_grad, prim, alt, wr_t, exp_gate, exp_up, exp_down, sh_gate, sh_up, sh_down):
    width = sh_gate.shape[1]
    total = SHARDS * TOK
    rows = OWN * PAD
    shape = jax.ShapeDtypeStruct
    dma = pltpu.SemaphoreType.DMA
    half_f32 = pltpu.VMEM((TOK, HALF), F32)
    slots_f32 = pltpu.VMEM((SLOTS, HALF), F32)
    return pl.pallas_call(
        layer_kernel,
        out_shape=(
            shape((TOK, DIM), BF16), shape((TOK, HALF), F32), shape((EXPERTS, DIM), F32),
            shape((rows, DIM), BF16), shape((rows, DIM), BF16), shape((rows, width), BF16), shape((rows, 2 * width), BF16),
            shape((total, DIM), BF16), shape((SHARDS, TOK, DIM), BF16), shape((total, width), BF16), shape((total, 2 * width), BF16),
        ),
        in_specs=[ANY] * 11,
        out_specs=(VMEM,) * 11,
        scratch_shapes=[
            pltpu.VMEM((SHARDS, TOK, DIM), BF16), pltpu.VMEM((SHARDS, 8, TOK), jnp.int32), pltpu.VMEM((EXPERTS, DIM), BF16),
            pltpu.VMEM((OWN, DIM, width), BF16), pltpu.VMEM((OWN, DIM, width), BF16), pltpu.VMEM((OWN, width, DIM), BF16),
            pltpu.VMEM((DIM, width), BF16), pltpu.VMEM((DIM, width), BF16), pltpu.VMEM((width, DIM), BF16),
            pltpu.VMEM((rows, total), BF16), pltpu.VMEM((rows, DIM), F32),
            pltpu.VMEM((rows, width), F32), pltpu.VMEM((rows, width), F32),
            pltpu.VMEM((EXPERTS, total), F32), pltpu.VMEM((8, total), F32),
            pltpu.VMEM((TOK, width), BF16), pltpu.VMEM((TOK, width), BF16), pltpu.VMEM((width, HALF), BF16), half_f32, half_f32, half_f32, half_f32,
            slots_f32, slots_f32, slots_f32, slots_f32, slots_f32, slots_f32,
            pltpu.VMEM((SHARDS, SLOTS, HALF), BF16), pltpu.VMEM((SHARDS, SLOTS, HALF), BF16),
            pltpu.VMEM((8, TOK), F32), pltpu.VMEM((2 * SHARDS, 8, TOK), F32),
            dma((8,)), dma((3,)), dma((3,)), dma((10,)), dma((2,)), dma((2, 3, 2)), dma((6,)), dma((10,)), dma((1,)), dma((1,)), dma((1,)), dma((1,)), pltpu.SemaphoreType.REGULAR((2,)),
        ],
        compiler_params=pltpu.CompilerParams(collective_id=0, has_side_effects=True, vmem_limit_bytes=40 << 20),
        name="moe_layer",
    )(x_in, y_grad, prim, alt, wr_t, exp_gate, exp_up, exp_down, sh_gate, sh_up, sh_down)


def grads_kernel(xs, us, hid, dab, n_all, dy_all, hid_s, dab_s, g_router, y_out, g_gate_hbm, g_up_hbm, g_down_hbm, gs_gate_hbm, gs_up_hbm, gs_down_hbm, g_router_hbm, y_out_hbm,
                 g_gate, g_up, g_down, gs_gate, gs_up, gs_down, out_sem, sh_sem):
    def write(src, dst, sem):
        copy = pltpu.make_async_copy(src, dst, sem)
        copy.start()
        return copy

    for e in range(OWN):
        rows = slice(e * PAD, (e + 1) * PAD)
        g_down[e] = mm(hid[rows, :], us[rows, :], TN)
        write(g_down.at[e], g_down_hbm.at[e], out_sem.at[0])
        both = mm(xs[rows, :], dab[rows, :], TN)
        g_gate[e] = both[:, :WIDTH]
        g_up[e] = both[:, WIDTH:]
        write(g_gate.at[e], g_gate_hbm.at[e], out_sem.at[1])
        write(g_up.at[e], g_up_hbm.at[e], out_sem.at[2])
    both = mm(n_all[...], dab_s[...], TN)
    gs_gate[...] = both[:, :WIDTH]
    gs_up[...] = both[:, WIDTH:]
    writes = [write(gs_gate, gs_gate_hbm, sh_sem.at[0]), write(gs_up, gs_up_hbm, sh_sem.at[1])]
    gs_down[...] = mm(hid_s[...], dy_all[...], TN)
    writes += [write(gs_down, gs_down_hbm, sh_sem.at[2]), write(g_router, g_router_hbm, sh_sem.at[3]), write(y_out, y_out_hbm, sh_sem.at[4])]
    for copy in writes:
        copy.wait()
    for k, (src, dst) in enumerate(((g_down, g_down_hbm), (g_gate, g_gate_hbm), (g_up, g_up_hbm))):
        pltpu.make_async_copy(src, dst, out_sem.at[k]).wait()


def grads_call(*saved):
    shape = jax.ShapeDtypeStruct
    outs = ((OWN, DIM, WIDTH), (OWN, DIM, WIDTH), (OWN, WIDTH, DIM), (DIM, WIDTH), (DIM, WIDTH), (WIDTH, DIM), (EXPERTS, DIM))
    return pl.pallas_call(
        grads_kernel,
        out_shape=tuple(shape(dims, F32) for dims in outs) + (shape((TOK, DIM), BF16),),
        in_specs=[VMEM] * 10,
        out_specs=(ANY,) * 8,
        scratch_shapes=[pltpu.VMEM(dims, F32) for dims in outs[:-1]] + [pltpu.SemaphoreType.DMA((3,)), pltpu.SemaphoreType.DMA((5,))],
        compiler_params=pltpu.CompilerParams(vmem_limit_bytes=44 << 20),
        cost_estimate=pl.CostEstimate(flops=8 << 30, bytes_accessed=32 << 20, transcendentals=0),
        name="weight_grads",
    )(*saved)


def finish_kernel(x_ref, dy_ref, dn_mine, dn_recv, dx_out):
    side = lax.axis_index("etp")
    theirs = pl.ds(pl.multiple_of((1 - side) * HALF, HALF), HALF)
    mine = pl.ds(pl.multiple_of(side * HALF, HALF), HALF)
    x_wide = x_ref[...].astype(F32)
    inv_rms = inv_rms_of(x_wide)
    halves = ((mine, dn_mine), (theirs, dn_recv))
    norm_proj = sum(jnp.sum(dn[...] * x_ref[:, cols].astype(F32), axis=1, keepdims=True) for cols, dn in halves) / DIM
    for cols, dn in halves:
        dx_out[:, cols] = (dy_ref[:, cols].astype(F32) + inv_rms * dn[...] - x_ref[:, cols].astype(F32) * inv_rms**3 * norm_proj).astype(BF16)


def finish_call(*args):
    return pl.pallas_call(
        finish_kernel,
        out_shape=jax.ShapeDtypeStruct((TOK, DIM), BF16),
        in_specs=[VMEM] * 4,
        out_specs=VMEM,
        compiler_params=pltpu.CompilerParams(vmem_limit_bytes=8 << 20),
        name="finish_tokens",
    )(*args)


def solution(mesh):
    tok_spec = P(("dp", "ep"), None)
    id_spec = P(("dp", "ep"))
    in_specs = (tok_spec, tok_spec, id_spec, id_spec, P(None, None), P("ep", None, "etp"), P("ep", None, "etp"), P("ep", "etp", None), P(None, "etp"), P(None, "etp"), P("etp", None))
    out_specs = (tok_spec, tok_spec, P(("dp", "ep"), None, "etp"), P(("dp", "ep"), None, "etp"), P(("dp", "ep"), "etp", None), P("dp", "etp"), P("dp", "etp"), P(("dp", "etp"), None), P("dp", None))

    def local_step(x_in, y_grad, prim_exp, alt_exp, w_router, exp_gate, exp_up, exp_down, sh_gate, sh_up, sh_down):
        y_full, dn_half, gr, xs, us, hid, dab, n_all, dy_all, hid_s, dab_s = layer_call(*[pltpu.with_memory_space_constraint(a, pltpu.HBM) for a in (x_in, y_grad, prim_exp.reshape(1, TOK), alt_exp.reshape(1, TOK), w_router.T, exp_gate, exp_up, exp_down, sh_gate, sh_up, sh_down)])
        dn_other = lax.ppermute(dn_half, "etp", [(0, 1), (1, 0)])
        g_gate, g_up, g_down, gs_gate, gs_up, gs_down, g_router, y_out = grads_call(xs, us, hid, dab, n_all, dy_all.reshape(SHARDS * TOK, DIM), hid_s, dab_s, gr, y_full)
        x_grad = finish_call(x_in, y_grad, dn_half, dn_other)
        return (y_out, x_grad, g_gate, g_up, g_down, gs_gate, gs_up, gs_down, g_router.T)

    return jax.shard_map(local_step, mesh=mesh, in_specs=in_specs, out_specs=out_specs, check_vma=False)
```
